256 devices in a mesh: row: 32 (over z, y), feat: 8 (over x, core).
Axes of the slice: x: 4, y: 4, z: 8, core: 2. Of those that a mesh axis runs over, the one named last changes fastest.
Arguments:
- design: bfloat16 [4096, 65536], P('row', 'feat'), may hold values from -0.0234375 to 0.0234375
- targets: bfloat16 [4096, 48], P('row'), may hold values from -6 to 6
- factor: float32 [65536, 256], P(('feat', 'row')), may hold values from -0.09375 to 0.09375
- weights: float32 [256], replicated, may hold values from 0.3 to 3
- penalty: float32 [48], replicated, may hold values from 0.05 to 0.5
Outputs:
- solution: float32 [65536, 48], P(('feat', 'row'))
- residual: float32 [65536, 48], P(('feat', 'row'))
The draws below stay inside these ranges and needn't reach their ends.
All inputs are finite; a program needn't handle non-finite values.
Results may differ from the reference program's by a relative error of at most 0.024.
Values may be sent and summed in bfloat16 or wider, within the bound.
No kernel may reach another device: no remote copies, remote signals or barrier semaphores. Data moves between devices by JAX's collectives and lax.ppermute only.
A program may use at most 64 MiB of HBM per device.

```python
import math
import jax
import jax.numpy as jnp
from jax import lax

FEATURES = 65536
RANK = 256
TARGETS = 48
ROW_DEV = 128
ITERS = 3
ROWS = 4096
N_ROW = 32


def shard_levels(own_key, shape, shards, least, high):
    gain = 1.0
    for axis_at, blocks in shards:
        heights = jax.random.uniform(jax.random.fold_in(jax.random.fold_in(own_key, 6), axis_at), (blocks,), jnp.float32, least / len(shards), high / len(shards))
        gain = gain * jnp.repeat(jnp.exp(heights), shape[axis_at] // blocks).reshape((-1,) + (1,) * (len(shape) - 1 - axis_at))
    return gain


def centred(rng, extent, deviation, reach, cuts=(), held_as=jnp.bfloat16):
    gain = shard_levels(rng, extent, cuts, -0.22, 0.18) if cuts else 1.0
    entries = jax.random.normal(rng, extent, jnp.float32) * deviation * gain
    return jnp.minimum(jnp.maximum(entries, -reach), reach).astype(held_as)


def setup_inputs(seed: int = 0) -> dict:
    streams_of = jax.random.split(jax.random.key(seed), 6)
    return {
        "design": centred(streams_of[0], (ROWS, FEATURES), FEATURES ** -0.5, 0.0234375, ((0, 32), (1, 8))),
        "targets": centred(streams_of[1], (ROWS, TARGETS), 1.0, 6.0, ((0, 32),)),
        "factor": centred(streams_of[2], (FEATURES, RANK), (16 * RANK) ** -0.5, 0.09375, ((0, 256),), jnp.float32),
        "weights": jnp.clip(jnp.exp(jax.random.uniform(streams_of[3], (RANK,), jnp.float32, math.log(0.3), math.log(3.0))), 0.3, 3.0),
        "penalty": jnp.clip(jnp.exp(jax.random.uniform(streams_of[4], (TARGETS,), jnp.float32, math.log(0.05), math.log(0.5))), 0.05, 0.5),
    }


def row_blocks(design):
    return design.reshape(N_ROW, ROW_DEV, FEATURES)


def times_vector(design, vector_low):
    parts = lax.map(lambda segment: jnp.dot(segment, vector_low, preferred_element_type=jnp.float32), row_blocks(design))
    return parts.reshape(ROW_DEV * N_ROW, vector_low.shape[1])


def transpose_times(design, rows_low):
    blocks = row_blocks(design)
    pieces = rows_low.reshape(N_ROW, ROW_DEV, rows_low.shape[1])

    def accumulate(running, items):
        segment, values = items
        return running + lax.dot_general(segment, values, (((0,), (0,)), ((), ())), preferred_element_type=jnp.float32), None

    running = jnp.zeros((FEATURES, rows_low.shape[1]), jnp.float32)
    running, unused = lax.scan(accumulate, running, (blocks, pieces))
    return running


def precondition(factor, weights, vector):
    projected = jnp.dot(factor.T, vector, precision=lax.Precision.HIGHEST)
    return vector + jnp.dot(factor, weights[:, None] * projected, precision=lax.Precision.HIGHEST)


def reference(design, targets, factor, weights, penalty):
    residual = transpose_times(design, targets)
    solution = jnp.zeros_like(residual)
    search = precondition(factor, weights, residual)
    inner = jnp.sum(residual * search, axis=0)
    direction = search
    for step_index in range(ITERS):
        dir_low = direction.astype(jnp.bfloat16)
        row_values = times_vector(design, dir_low)
        row_low = row_values.astype(jnp.bfloat16)
        hessian_dir = transpose_times(design, row_low) + penalty[None, :] * direction
        curvature = jnp.sum(direction * hessian_dir, axis=0)
        step_size = inner / curvature
        solution = solution + step_size[None, :] * direction
        residual = residual - step_size[None, :] * hessian_dir
        if step_index + 1 < ITERS:
            search = precondition(factor, weights, residual)
            inner_next = jnp.sum(residual * search, axis=0)
            direction = search + (inner_next / inner)[None, :] * direction
            inner = inner_next
    return solution, residual
```

```python
import jax
import jax.numpy as jnp
from jax import lax
from jax.sharding import Mesh
from jax.sharding import PartitionSpec as P

ITERS = 3
ROW = ("zh", "zl", "y")
FEAT = ("x", "c")
OWN = ("zl", "y")
MANY = ("zl", "y", "x", "c")
N_OWN, N_MANY, N_ZH = 8, 64, 4
BF = jnp.bfloat16
F32 = jnp.float32


def exchange(pieces, axes):
    return lax.all_to_all(pieces, axes, 0, 0, tiled=True)


def spread(shard, axes, count):
    return exchange(jnp.broadcast_to(shard[None], (count, *shard.shape)), axes)


def high_low(value):
    high = lax.reduce_precision(value, 8, 7)
    return high, value - high


def to_tiles(array):
    rows, lanes = array.shape
    tiled = array.reshape(rows // 8, 8, lanes // 128, 128).transpose(0, 2, 1, 3)
    return tiled.reshape(rows * lanes // 1024, 8, 128)


def from_tiles(tiles, rows, lanes):
    tiled = tiles.reshape(rows // 8, lanes // 128, 8, 128).transpose(0, 2, 1, 3)
    return tiled.reshape(rows, lanes)


def mm(a, b):
    return jnp.dot(a.astype(BF), b.astype(BF), preferred_element_type=F32)


def mm_t(a, b):
    return lax.dot_general(
        a.astype(BF), b.astype(BF), (((1,), (1,)), ((), ())), preferred_element_type=F32
    )


def scalar_tile(first, second):
    rows = []
    for value in (first, second):
        rows.extend(high_low(value))
    block = jnp.stack(rows)
    return jnp.pad(block, ((0, 4), (0, 80)))[None]


def split_again(tile):
    total = tile[0::2] + tile[1::2]
    high, low = high_low(total)
    return jnp.stack([high, low], axis=1).reshape(8, 128)


def shards(design, targets, factor, weights, penalty):
    blocks = design.reshape(128, 4, 8, 256).transpose(2, 0, 1, 3).reshape(8, 128, 1024)
    goal = targets.T.reshape(6, 1024)
    goal = jnp.broadcast_to(jnp.pad(goal, ((0, 2), (0, 0)))[None], (8, 8, 1024))
    moved = exchange(jnp.concatenate([blocks, goal], axis=1), OWN)
    mat = moved[:, :128].reshape(1024, 1024)
    goal = moved[:, 128:134].reshape(8, 48, 128).transpose(1, 0, 2).reshape(48, 1024)
    fac = spread(factor.astype(BF), "zh", N_ZH).reshape(1024, 256)

    zh = lax.axis_index("zh")
    me = lax.axis_index(MANY)
    w = weights[None, :]

    def over_zh(rows, square):
        part = mm(rows, mat).astype(BF)
        high, low = high_low(square)
        extra = jnp.pad(jnp.stack([high, low], axis=1), ((0, 0), (0, 126))).astype(BF)
        arrived = spread(jnp.concatenate([part, extra], axis=1), "zh", N_ZH)
        total = arrived.astype(F32).sum(axis=0)
        return total[:, :1024], total[:, 1024] + total[:, 1025]

    def over_many(tiles, scalar_at):
        per = tiles.shape[0] // N_MANY
        pieces = tiles.reshape(N_MANY, per * 8, 128)
        total = exchange(pieces.astype(BF), MANY).astype(F32).sum(axis=0)
        head = jnp.where(me == scalar_at // per, split_again(total[:8]), total[:8])
        total = jnp.concatenate([head, total[8:]]) if per > 1 else head
        return spread(total.astype(BF), MANY, N_MANY).reshape(N_MANY * per, 8, 128).astype(F32)

    residual, unused = over_zh(goal, jnp.zeros((48,), F32))
    answer = jnp.zeros_like(residual)
    direction = residual
    for step_index in range(ITERS):
        first = step_index == 0
        image = mm_t(residual, mat)
        projected = mm(residual, fac)
        scal = scalar_tile(
            jnp.sum(residual * residual, axis=1), jnp.sum(residual * direction, axis=1)
        )
        tiles = jnp.concatenate([to_tiles(image), to_tiles(projected), jnp.zeros((3, 8, 128), F32)])
        if first:
            fac_t = fac.T
            cross = to_tiles(mm_t(fac_t, mat))
            gram = to_tiles(mm(fac_t, fac))
            everything = jnp.concatenate([scal, jnp.zeros((5, 8, 128), F32), tiles[:60], cross, gram[:62]])
            everything = lax.dynamic_update_slice(everything, gram[62:], (1, 0, 0))
            back = over_many(everything, 0)
            scal = back[0]
            image_p = back[6:66]
            cross = from_tiles(back[66:322], 256, 1024)
            gram = from_tiles(jnp.concatenate([back[322:384], back[1:3]]), 256, 256)
        else:
            back = over_many(jnp.concatenate([scal, tiles]), 0)
            scal = back[0]
            image_p = back[1:61]
        image = from_tiles(image_p[:48], 48, 1024)
        projected = from_tiles(image_p[48:60], 48, 256)
        rr = (scal[0] + scal[1])[:48]
        rd = (scal[2] + scal[3])[:48]

        scaled = w * projected
        inner_next = rr + jnp.sum(scaled * projected, axis=1)
        through = mm(scaled, gram)
        ss = rr + 2.0 * jnp.sum(scaled * projected, axis=1) + jnp.sum(scaled * through, axis=1)
        search = residual + mm_t(scaled, fac)
        row_search = image + mm(scaled, cross)
        if first:
            direction, row_values = search, row_search
            dd = ss
            seen = projected + through
        else:
            beta = inner_next / inner
            sd = rd + jnp.sum(scaled * seen, axis=1)
            dd = ss + 2.0 * beta * sd + beta * beta * dd
            seen = projected + through + beta[:, None] * seen
            direction = search + beta[:, None] * direction
            row_values = row_search + beta[:, None] * row_values
        inner = inner_next
        row_low = row_values.astype(BF)
        square = jnp.sum(row_values * row_low.astype(F32), axis=1)
        if step_index + 1 < ITERS:
            hess, curvature = over_zh(row_low, square)
            step = (inner / (curvature + penalty * dd))[:, None]
            answer = answer + step * direction
            residual = residual - step * (hess + penalty[:, None] * direction)
        else:
            part = mm(row_low, mat).astype(BF).reshape(48, 4, 256).transpose(1, 0, 2)
            high, low = high_low(square)
            extra = jnp.pad(jnp.stack([high, low], axis=1), ((0, 0), (0, 126))).astype(BF)
            extra = jnp.broadcast_to(extra[None], (4, 48, 128))
            total = exchange(jnp.concatenate([part, extra], axis=2), "zh").astype(F32).sum(axis=0)
            curvature = total[:, 256] + total[:, 257]
            step = (inner / (curvature + penalty * dd))[:, None]

            def own(array):
                return lax.dynamic_slice(array, (0, zh * 256), (48, 256))

            mine = own(direction)
            answer = own(answer) + step * mine
            residual = own(residual) - step * (total[:, :256] + penalty[:, None] * mine)
    return answer.T, residual.T


def solution(mesh):
    finer = Mesh(mesh.devices.reshape(4, 2, 4, 4, 2), ("zh", "zl", "y", "x", "c"))
    spec = P((*FEAT, *ROW), None)
    in_specs = (P(ROW, FEAT), P(ROW, None), spec, P(), P())
    return jax.shard_map(
        shards, mesh=finer, in_specs=in_specs, out_specs=(spec, spec), check_vma=False
    )
```

```python
import jax
import jax.numpy as jnp
from jax import lax
from jax.experimental import pallas as pl
from jax.experimental.pallas import tpu as pltpu
from jax.sharding import Mesh
from jax.sharding import PartitionSpec as P

ITERS = 3
ROW = ("zh", "zl", "y")
FEAT = ("x", "c")
OWN = ("zl", "y")
MANY = ("zl", "y", "x", "c")
N_OWN, N_MANY, N_ZH = 8, 64, 4
T, RANK, BLOCK = 48, 256, 1024
SCAL = 480
HEAD = 512
BF = jnp.bfloat16
F32 = jnp.float32


def exchange(pieces, axes):
    return lax.all_to_all(pieces, axes, 0, 0, tiled=True)


def spread(shard, axes, count):
    return exchange(jnp.broadcast_to(shard[None], (count, *shard.shape)), axes)


def high_low(value):
    high = lax.reduce_precision(value, 8, 7)
    return high, value - high


def dot(a, b):
    return jnp.dot(a, b, preferred_element_type=F32)


def dot_t(a, b):
    return lax.dot_general(a, b, (((1,), (1,)), ((), ())), preferred_element_type=F32)


def call(body, out, **kw):
    return pl.pallas_call(body, out_shape=out, **kw)


def shape(*dims, dtype=F32):
    return jax.ShapeDtypeStruct(dims, dtype)


def columns(parts):
    lane = lax.broadcasted_iota(jnp.int32, (T, 128), 1)
    block = jnp.zeros((T, 128), F32)
    for index, part in enumerate(parts):
        block = jnp.where(lane == index, part, block)
    return block


def split16(value):
    high = value.astype(BF).astype(F32)
    return high, value - high


def total_of(array):
    return jnp.sum(array, axis=1, keepdims=True)


def pack_kernel(a0, a1, a2, a3, goal, out):
    for index, block in enumerate((a0, a1, a2, a3)):
        out[0, :128, index * 256 : (index + 1) * 256] = block[...]
    for index in range(6):
        out[0, 128:136, index * 128 : (index + 1) * 128] = goal[index * 8 : index * 8 + 8, :]
    out[0, 128:136, 768:] = jnp.zeros((8, 256), BF)


def pack(design, goal):
    def part(index):
        return pl.BlockSpec((128, 256), lambda s, index=index: (0, index * 8 + s))

    return pl.pallas_call(
        pack_kernel,
        grid=(8,),
        in_specs=[part(0), part(1), part(2), part(3), pl.BlockSpec((T, 128), lambda s: (0, 0))],
        out_specs=pl.BlockSpec((1, 136, BLOCK), lambda s: (s, 0, 0)),
        out_shape=shape(8, 136, BLOCK, dtype=BF),
    )(design, design, design, design, goal)


def start_kernel(mat, out):
    part = jnp.zeros((T, BLOCK), F32)
    for src in range(8):
        goal = jnp.concatenate(
            [mat[src, 128:136, t * 128 : (t + 1) * 128].astype(F32) for t in range(6)], axis=0
        ).astype(BF)
        part = part + dot(goal, mat[src, :128, :])
    high, low = split16(part)
    high, low = high.astype(BF), low.astype(BF)
    for to in range(N_ZH):
        out[to, :, :BLOCK] = high
        out[to, :, BLOCK:] = low[:, to * 256 : (to + 1) * 256]


def cross_kernel(mat, fac, gram, out):
    factor = fac[...]
    for src in range(8):
        block = dot(mat[src, :128, :], factor).astype(BF)
        out[src * 256 : src * 256 + 128, :] = block[:, :128]
        out[src * 256 + 128 : src * 256 + 256, :] = block[:, 128:]
    both = gram[...].astype(BF)
    out[2048:2304, :] = both[:, :128]
    out[2304:2560, :] = both[:, 128:]


def write_head(residual, direction, mat, fac, out):
    low = residual.astype(BF)
    for src in range(8):
        out[src * T : (src + 1) * T, :] = dot_t(low, mat[src, :128, :]).astype(BF)
    seen = dot(low, fac[...]).astype(BF)
    out[384:432, :] = seen[:, :128]
    out[432:480, :] = seen[:, 128:]
    rr = split16(total_of(residual * residual))
    rd = split16(total_of(residual * direction))
    block = jnp.concatenate([columns([*rr, *rd]), jnp.zeros((80, 128), F32)], axis=0)
    tile = block.T[:32, :]
    out[SCAL:HEAD, :] = tile.astype(BF)


def first_kernel(arrived, mat, fac, rest, out, residual_out, fix_out):
    residual = jnp.zeros((T, BLOCK), F32)
    fix = jnp.zeros((T, 256), F32)
    for source in range(N_ZH):
        residual = residual + arrived[source, :, :BLOCK].astype(F32)
        fix = fix + arrived[source, :, BLOCK:].astype(F32)
    residual_out[...] = residual
    fix_out[...] = fix
    write_head(residual, residual, mat, fac, out)
    out[HEAD:, :] = rest[...]


def next_kernel(
    arrived, direction_in, residual_in, answer_in, scal_in, penalty, mat, fac, out, residual_out, answer_out
):
    hess = jnp.zeros((T, BLOCK + 128), F32)
    for source in range(N_ZH):
        hess = hess + arrived[source].astype(F32)
    square = hess[:, BLOCK : BLOCK + 1] + hess[:, BLOCK + 1 : BLOCK + 2]
    hess = hess[:, :BLOCK]
    inner, dd = scal_in[:, :1], scal_in[:, 1:2]
    ridge = penalty[:, :1]
    direction = direction_in[...]
    step = inner / (square + ridge * dd)
    answer = step * direction
    if answer_in is not None:
        answer = answer_in[...] + answer
    answer_out[...] = answer
    residual = residual_in[...] - step * (hess + ridge * direction)
    residual_out[...] = residual
    write_head(residual, direction, mat, fac, out)


def search_kernel(first, last, *refs):
    refs = list(refs)
    back = refs.pop(0)
    full = back if first else refs.pop(0)
    mat, fac, weights, residual_in = refs[:4]
    refs = refs[4:]
    if not first:
        direction_in, row_in, seen_in, scal_in = refs[:4]
        refs = refs[4:]
    out, direction_out, row_out, seen_out, scal_out = refs

    scaled = weights[0:1, :]
    projected = jnp.concatenate([back[384:432, :], back[432:480, :]], axis=1).astype(F32)
    tile = jnp.concatenate([back[SCAL:HEAD, :].astype(F32), jnp.zeros((96, 128), F32)], axis=0).T
    rr = tile[:T, 0:1] + tile[:T, 1:2]
    rd = tile[:T, 2:3] + tile[:T, 3:4]
    scaled = scaled * projected
    cross_inner = total_of(scaled * projected)
    inner = rr + cross_inner
    low = scaled.astype(BF)
    through = jnp.concatenate([dot(low, full[2560:2816, :]), dot(low, full[2816:3072, :])], axis=1)
    dd = rr + 2.0 * cross_inner + total_of(scaled * through)
    seen = projected + through
    direction = residual_in[...] + dot_t(low, fac[...])
    if not first:
        before, dd_before = scal_in[:, :1], scal_in[:, 1:2]
        beta = inner / before
        sd = rd + total_of(scaled * seen_in[...])
        dd = dd + 2.0 * beta * sd + beta * beta * dd_before
        seen = seen + beta * seen_in[...]
        direction = direction + beta * direction_in[...]
    direction_out[...] = direction
    seen_out[...] = seen
    scal_out[...] = columns([inner, dd])
    part = jnp.zeros((T, BLOCK), F32)
    square = jnp.zeros((T, 1), F32)
    for src in range(8):
        at = HEAD + src * 256
        row = back[src * T : (src + 1) * T, :].astype(F32)
        row = row + dot_t(low[:, :128], full[at : at + 128, :])
        row = row + dot_t(low[:, 128:], full[at + 128 : at + 256, :])
        if not first:
            row = row + beta * row_in[:, src * 128 : (src + 1) * 128]
        row_out[:, src * 128 : (src + 1) * 128] = row
        row_low = row.astype(BF)
        square = square + total_of(row * row_low.astype(F32))
        part = part + dot(row_low, mat[src, :128, :])
    extra = columns(split16(square)).astype(BF)
    high, low = split16(part)
    high, low = high.astype(BF), low.astype(BF)
    for to in range(N_ZH):
        if last:
            mine = slice(to * 256, (to + 1) * 256)
            out[to, :, :256] = high[:, mine]
            out[to, :, 256:512] = low[:, mine]
            out[to, :, 512:] = extra
        else:
            out[to, :, :BLOCK] = high
            out[to, :, BLOCK:] = extra


def split_again(tile):
    total = tile[0:4:2] + tile[1:4:2]
    high, low = high_low(total)
    return jnp.concatenate([jnp.stack([high, low], axis=1).reshape(4, 128), tile[4:]])


def shards(design, targets, factor, weights, penalty):
    zh = lax.axis_index("zh")
    me = lax.axis_index(MANY)
    low_factor = factor.astype(BF)
    slots = jnp.zeros((N_ZH, 256, RANK), BF)
    slots = lax.dynamic_update_slice(slots, low_factor[None], (zh, 0, 0))
    for shift in range(1, N_ZH):
        pairs = [(i, (i + shift) % N_ZH) for i in range(N_ZH)]
        other = lax.ppermute(low_factor, "zh", pairs)
        slots = lax.dynamic_update_slice(slots, other[None], ((zh - shift) % N_ZH, 0, 0))
    fac = slots.reshape(BLOCK, RANK)

    mat = exchange(pack(design, targets.T), OWN)
    arrived = call(start_kernel, shape(N_ZH, T, BLOCK + 256, dtype=BF))(mat)
    arrived = exchange(arrived, "zh")
    gram = lax.dot_general(fac, fac, (((0,), (0,)), ((), ())), preferred_element_type=F32)
    rest = call(cross_kernel, shape(2560, 128, dtype=BF))(mat, fac, gram)

    w = jnp.broadcast_to(weights[None, :], (8, RANK))
    ridge = jnp.broadcast_to(penalty[:, None], (T, 128))

    def over_many(packed):
        pieces = packed.reshape(N_MANY, -1, 128)
        count = pieces.shape[1]
        total = exchange(pieces, MANY).astype(F32).sum(axis=0)
        head = jnp.where(me == SCAL // count, split_again(total[:8]), total[:8])
        if count > 8:
            head = jnp.concatenate([head, total[8:]])
        return spread(head.astype(BF), MANY, N_MANY).reshape(N_MANY * count, 128)

    packed, residual, fix = call(
        first_kernel,
        (shape(3072, 128, dtype=BF), shape(T, BLOCK), shape(T, 256)),
    )(arrived, mat, fac, rest)
    answer = None
    for step_index in range(ITERS):
        first, last = step_index == 0, step_index == ITERS - 1
        back = over_many(packed)
        if first:
            full = back
            state = ()
        else:
            state = (direction, row_values, seen, scal)
        args = (back,) if first else (back, full)
        wide = 640 if last else BLOCK + 128
        send, direction, row_values, seen, scal = call(
            lambda *refs, first=first, last=last: search_kernel(first, last, *refs),
            (
                shape(N_ZH, T, wide, dtype=BF),
                shape(T, BLOCK),
                shape(T, BLOCK),
                shape(T, RANK),
                shape(T, 128),
            ),
        )(*args, mat, fac, w, residual, *state)
        arrived = exchange(send, "zh")
        if last:
            break
        if answer is None:
            packed, residual, answer = call(
                lambda a, d, r, s, p, m, f, *outs: next_kernel(a, d, r, None, s, p, m, f, *outs),
                (shape(HEAD, 128, dtype=BF), shape(T, BLOCK), shape(T, BLOCK)),
            )(arrived, direction, residual, scal, ridge, mat, fac)
        else:
            packed, residual, answer = call(
                next_kernel,
                (shape(HEAD, 128, dtype=BF), shape(T, BLOCK), shape(T, BLOCK)),
            )(arrived, direction, residual, answer, scal, ridge, mat, fac)

    total = arrived.astype(F32).sum(axis=0)
    curvature = total[:, 512] + total[:, 513]
    step = (scal[:, 0] / (curvature + penalty * scal[:, 1]))[:, None]

    def own(array):
        return lax.dynamic_slice(array, (0, zh * 256), (T, 256))

    mine = own(direction)
    answer = own(answer) + step * mine
    hess = total[:, :256] + total[:, 256:512] + penalty[:, None] * mine
    residual = own(residual) + fix - step * hess
    return answer.T, residual.T


def solution(mesh):
    finer = Mesh(mesh.devices.reshape(4, 2, 4, 4, 2), ("zh", "zl", "y", "x", "c"))
    spec = P((*FEAT, *ROW), None)
    in_specs = (P(ROW, FEAT), P(ROW, None), spec, P(), P())
    return jax.shard_map(
        shards, mesh=finer, in_specs=in_specs, out_specs=(spec, spec), check_vma=False
    )
```

```python
import jax
import jax.numpy as jnp
from jax import lax
from jax.experimental import pallas as pl
from jax.experimental.pallas import tpu as pltpu
from jax.sharding import Mesh
from jax.sharding import PartitionSpec as P

ITERS = 3
ROW = ("zh", "zl", "y")
FEAT = ("x", "c")
OWN = ("zl", "y")
MANY = ("zl", "y", "x", "c")
N_OWN, N_MANY, N_ZH = 8, 64, 4
T, RANK, BLOCK = 48, 256, 1024
SCAL = 480
HEAD = 512
BF = jnp.bfloat16
F32 = jnp.float32


def exchange(pieces, axes):
    return lax.all_to_all(pieces, axes, 0, 0, tiled=True)


def spread(shard, axes, count):
    return exchange(jnp.broadcast_to(shard[None], (count, *shard.shape)), axes)


def high_low(value):
    high = lax.reduce_precision(value, 8, 7)
    return high, value - high


def dot(a, b):
    return jnp.dot(a, b, preferred_element_type=F32)


def dot_t(a, b):
    return lax.dot_general(a, b, (((1,), (1,)), ((), ())), preferred_element_type=F32)


PARAMS = pltpu.CompilerParams(vmem_limit_bytes=20 * 1024 * 1024)


def call(body, out):
    return pl.pallas_call(body, out_shape=out, compiler_params=PARAMS)


def shape(*dims, dtype=F32):
    return jax.ShapeDtypeStruct(dims, dtype)


def columns(parts):
    lane = lax.broadcasted_iota(jnp.int32, (T, 128), 1)
    block = jnp.zeros((T, 128), F32)
    for index, part in enumerate(parts):
        block = jnp.where(lane == index, part, block)
    return block


def split16(value):
    high = value.astype(BF).astype(F32)
    return high, value - high


def total_of(array):
    return jnp.sum(array, axis=1, keepdims=True)


def pack_kernel(design, goal, out):
    for to in range(8):
        for index in range(4):
            at = (index * 8 + to) * 256
            out[to, :128, index * 256 : (index + 1) * 256] = design[:, at : at + 256]
        for index in range(6):
            out[to, 128:136, index * 128 : (index + 1) * 128] = goal[index * 8 : index * 8 + 8, :]
        out[to, 128:136, 768:] = jnp.zeros((8, 256), BF)


def start_kernel(mat, out):
    part = jnp.zeros((T, BLOCK), F32)
    for src in range(8):
        goal = jnp.concatenate(
            [mat[src, 128:136, t * 128 : (t + 1) * 128].astype(F32) for t in range(6)], axis=0
        ).astype(BF)
        part = part + dot(goal, mat[src, :128, :])
    high, low = split16(part)
    high, low = high.astype(BF), low.astype(BF)
    for to in range(N_ZH):
        out[to, :, :BLOCK] = high
        out[to, :, BLOCK:] = low[:, to * 256 : (to + 1) * 256]


def cross_kernel(mat, fac, gram, out):
    factor = fac[...]
    for src in range(8):
        block = dot(mat[src, :128, :], factor).astype(BF)
        out[src * 256 : src * 256 + 128, :] = block[:, :128]
        out[src * 256 + 128 : src * 256 + 256, :] = block[:, 128:]
    both = gram[...].astype(BF)
    out[2048:2304, :] = both[:, :128]
    out[2304:2560, :] = both[:, 128:]


def write_head(residual, direction, mat, fac, out):
    low = residual.astype(BF)
    for src in range(8):
        out[src * T : (src + 1) * T, :] = dot_t(low, mat[src, :128, :]).astype(BF)
    seen = dot(low, fac[...]).astype(BF)
    out[384:432, :] = seen[:, :128]
    out[432:480, :] = seen[:, 128:]
    rr = split16(total_of(residual * residual))
    rd = split16(total_of(residual * direction))
    block = jnp.concatenate([columns([*rr, *rd]), jnp.zeros((80, 128), F32)], axis=0)
    tile = block.T[:32, :]
    out[SCAL:HEAD, :] = tile.astype(BF)


def first_kernel(arrived, mat, fac, rest, out, residual_out, fix_out):
    residual = jnp.zeros((T, BLOCK), F32)
    fix = jnp.zeros((T, 256), F32)
    for source in range(N_ZH):
        residual = residual + arrived[source, :, :BLOCK].astype(F32)
        fix = fix + arrived[source, :, BLOCK:].astype(F32)
    residual_out[...] = residual
    fix_out[...] = fix
    write_head(residual, residual, mat, fac, out)
    out[HEAD:, :] = rest[...]


def next_kernel(
    arrived, direction_in, residual_in, answer_in, scal_in, penalty, mat, fac, out, residual_out, answer_out
):
    hess = jnp.zeros((T, BLOCK + 128), F32)
    for source in range(N_ZH):
        hess = hess + arrived[source].astype(F32)
    square = hess[:, BLOCK : BLOCK + 1] + hess[:, BLOCK + 1 : BLOCK + 2]
    hess = hess[:, :BLOCK]
    inner, dd = scal_in[:, :1], scal_in[:, 1:2]
    ridge = penalty[:, :1]
    direction = direction_in[...]
    step = inner / (square + ridge * dd)
    answer = step * direction
    if answer_in is not None:
        answer = answer_in[...] + answer
    answer_out[...] = answer
    residual = residual_in[...] - step * (hess + ridge * direction)
    residual_out[...] = residual
    write_head(residual, direction, mat, fac, out)


def search_kernel(first, last, *refs):
    refs = list(refs)
    back = refs.pop(0)
    full = back if first else refs.pop(0)
    mat, fac, weights, residual_in = refs[:4]
    refs = refs[4:]
    if not first:
        direction_in, row_in, seen_in, scal_in = refs[:4]
        refs = refs[4:]
    out, direction_out, row_out, seen_out, scal_out = refs

    scaled = weights[0:1, :]
    projected = jnp.concatenate([back[384:432, :], back[432:480, :]], axis=1).astype(F32)
    tile = jnp.concatenate([back[SCAL:HEAD, :].astype(F32), jnp.zeros((96, 128), F32)], axis=0).T
    rr = tile[:T, 0:1] + tile[:T, 1:2]
    rd = tile[:T, 2:3] + tile[:T, 3:4]
    scaled = scaled * projected
    cross_inner = total_of(scaled * projected)
    inner = rr + cross_inner
    low = scaled.astype(BF)
    through = jnp.concatenate([dot(low, full[2560:2816, :]), dot(low, full[2816:3072, :])], axis=1)
    dd = rr + 2.0 * cross_inner + total_of(scaled * through)
    seen = projected + through
    direction = residual_in[...] + dot_t(low, fac[...])
    if not first:
        before, dd_before = scal_in[:, :1], scal_in[:, 1:2]
        beta = inner / before
        sd = rd + total_of(scaled * seen_in[...])
        dd = dd + 2.0 * beta * sd + beta * beta * dd_before
        seen = seen + beta * seen_in[...]
        direction = direction + beta * direction_in[...]
    direction_out[...] = direction
    seen_out[...] = seen
    scal_out[...] = columns([inner, dd])
    part = jnp.zeros((T, BLOCK), F32)
    square = jnp.zeros((T, 1), F32)
    for src in range(8):
        at = HEAD + src * 256
        row = back[src * T : (src + 1) * T, :].astype(F32)
        row = row + dot_t(low[:, :128], full[at : at + 128, :])
        row = row + dot_t(low[:, 128:], full[at + 128 : at + 256, :])
        if not first:
            row = row + beta * row_in[:, src * 128 : (src + 1) * 128]
        row_out[:, src * 128 : (src + 1) * 128] = row
        row_low = row.astype(BF)
        square = square + total_of(row * row_low.astype(F32))
        part = part + dot(row_low, mat[src, :128, :])
    extra = columns(split16(square)).astype(BF)
    high, low = split16(part)
    high, low = high.astype(BF), low.astype(BF)
    for to in range(N_ZH):
        if last:
            mine = slice(to * 256, (to + 1) * 256)
            out[to, :, :256] = high[:, mine]
            out[to, :, 256:512] = low[:, mine]
            out[to, :, 512:] = extra
        else:
            out[to, :, :BLOCK] = high
            out[to, :, BLOCK:] = extra


def split_again(tile):
    total = tile[0:4:2] + tile[1:4:2]
    high, low = high_low(total)
    return jnp.concatenate([jnp.stack([high, low], axis=1).reshape(4, 128), tile[4:]])


def shards(design, targets, factor, weights, penalty):
    zh = lax.axis_index("zh")
    me = lax.axis_index(MANY)
    low_factor = factor.astype(BF)
    slots = jnp.zeros((N_ZH, 256, RANK), BF)
    slots = lax.dynamic_update_slice(slots, low_factor[None], (zh, 0, 0))
    for shift in range(1, N_ZH):
        pairs = [(i, (i + shift) % N_ZH) for i in range(N_ZH)]
        other = lax.ppermute(low_factor, "zh", pairs)
        slots = lax.dynamic_update_slice(slots, other[None], ((zh - shift) % N_ZH, 0, 0))
    fac = slots.reshape(BLOCK, RANK)

    mat = exchange(call(pack_kernel, shape(8, 136, BLOCK, dtype=BF))(design, targets.T), OWN)
    arrived = call(start_kernel, shape(N_ZH, T, BLOCK + 256, dtype=BF))(mat)
    arrived = exchange(arrived, "zh")
    gram = lax.dot_general(fac, fac, (((0,), (0,)), ((), ())), preferred_element_type=F32)
    rest = call(cross_kernel, shape(2560, 128, dtype=BF))(mat, fac, gram)

    w = jnp.broadcast_to(weights[None, :], (8, RANK))
    ridge = jnp.broadcast_to(penalty[:, None], (T, 128))

    def over_many(packed):
        pieces = packed.reshape(N_MANY, -1, 128)
        count = pieces.shape[1]
        total = exchange(pieces, MANY).astype(F32).sum(axis=0)
        head = jnp.where(me == SCAL // count, split_again(total[:8]), total[:8])
        if count > 8:
            head = jnp.concatenate([head, total[8:]])
        return spread(head.astype(BF), MANY, N_MANY).reshape(N_MANY * count, 128)

    packed, residual, fix = call(
        first_kernel,
        (shape(3072, 128, dtype=BF), shape(T, BLOCK), shape(T, 256)),
    )(arrived, mat, fac, rest)
    answer = None
    for step_index in range(ITERS):
        first, last = step_index == 0, step_index == ITERS - 1
        back = over_many(packed)
        if first:
            full = back
            state = ()
        else:
            state = (direction, row_values, seen, scal)
        args = (back,) if first else (back, full)
        wide = 640 if last else BLOCK + 128
        send, direction, row_values, seen, scal = call(
            lambda *refs, first=first, last=last: search_kernel(first, last, *refs),
            (
                shape(N_ZH, T, wide, dtype=BF),
                shape(T, BLOCK),
                shape(T, BLOCK),
                shape(T, RANK),
                shape(T, 128),
            ),
        )(*args, mat, fac, w, residual, *state)
        arrived = exchange(send, "zh")
        if last:
            break
        if answer is None:
            packed, residual, answer = call(
                lambda a, d, r, s, p, m, f, *outs: next_kernel(a, d, r, None, s, p, m, f, *outs),
                (shape(HEAD, 128, dtype=BF), shape(T, BLOCK), shape(T, BLOCK)),
            )(arrived, direction, residual, scal, ridge, mat, fac)
        else:
            packed, residual, answer = call(
                next_kernel,
                (shape(HEAD, 128, dtype=BF), shape(T, BLOCK), shape(T, BLOCK)),
            )(arrived, direction, residual, answer, scal, ridge, mat, fac)

    total = arrived.astype(F32).sum(axis=0)
    curvature = total[:, 512] + total[:, 513]
    step = (scal[:, 0] / (curvature + penalty * scal[:, 1]))[:, None]

    def own(array):
        return lax.dynamic_slice(array, (0, zh * 256), (T, 256))

    mine = own(direction)
    answer = own(answer) + step * mine
    hess = total[:, :256] + total[:, 256:512] + penalty[:, None] * mine
    residual = own(residual) + fix - step * hess
    return answer.T, residual.T


def solution(mesh):
    finer = Mesh(mesh.devices.reshape(4, 2, 4, 4, 2), ("zh", "zl", "y", "x", "c"))
    spec = P((*FEAT, *ROW), None)
    in_specs = (P(ROW, FEAT), P(ROW, None), spec, P(), P())
    return jax.shard_map(
        shards, mesh=finer, in_specs=in_specs, out_specs=(spec, spec), check_vma=False
    )
```

```python
import jax
import jax.numpy as jnp
from jax import lax
from jax.experimental import pallas as pl
from jax.experimental.pallas import tpu as pltpu
from jax.sharding import Mesh
from jax.sharding import PartitionSpec as P

ITERS = 3
ROW = ("zh", "zl", "y")
FEAT = ("x", "c")
OWN = ("zl", "y")
MANY = ("zl", "y", "x", "c")
N_OWN, N_MANY, N_ZH = 8, 64, 4
T, RANK, BLOCK = 48, 256, 1024
SCAL = 480
HEAD = 512
BF = jnp.bfloat16
F32 = jnp.float32


def exchange(pieces, axes):
    return lax.all_to_all(pieces, axes, 0, 0, tiled=True)


def dot(a, b):
    return jnp.dot(a, b, preferred_element_type=F32)


def dot_t(a, b):
    return lax.dot_general(a, b, (((1,), (1,)), ((), ())), preferred_element_type=F32)


PARAMS = pltpu.CompilerParams(vmem_limit_bytes=20 * 1024 * 1024)


IN_HBM = pl.BlockSpec(memory_space=pltpu.HBM)
IN_VMEM = pl.BlockSpec(memory_space=pltpu.VMEM)
IN_SMEM = pl.BlockSpec(memory_space=pltpu.SMEM)


def call(body, out):
    return pl.pallas_call(body, out_shape=out, compiler_params=PARAMS)


def fetch(pairs, sems):
    copies = [pltpu.make_async_copy(a, b, sems.at[i]) for i, (a, b) in enumerate(pairs)]
    for copy in copies:
        copy.start()
    return copies


def shape(*dims, dtype=F32):
    return jax.ShapeDtypeStruct(dims, dtype)


def columns(parts):
    lane = lax.broadcasted_iota(jnp.int32, (T, 128), 1)
    block = jnp.zeros((T, 128), F32)
    for index, part in enumerate(parts):
        block = jnp.where(lane == index, part, block)
    return block


def split16(value):
    high = value.astype(BF).astype(F32)
    return high, value - high


def total_of(array):
    return jnp.sum(array, axis=1, keepdims=True)


def pack_kernel(design, goal, out, sems, goal_sems):
    copies = []
    for to in range(8):
        for index in range(4):
            at = (index * 8 + to) * 256
            copies.append(
                pltpu.make_async_copy(
                    design.at[:, at : at + 256],
                    out.at[to, :128, index * 256 : (index + 1) * 256],
                    sems.at[to * 4 + index],
                )
            )
        for index in range(6):
            copies.append(
                pltpu.make_async_copy(
                    goal.at[index * 8 : index * 8 + 8, :],
                    out.at[to, 128:136, index * 128 : (index + 1) * 128],
                    goal_sems.at[to * 6 + index],
                )
            )
    for copy in copies:
        copy.start()
    for copy in copies:
        copy.wait()


def pack(design, goal):
    return pl.pallas_call(
        pack_kernel,
        out_shape=shape(8, 136, BLOCK, dtype=BF),
        in_specs=[IN_HBM, IN_VMEM],
        out_specs=IN_HBM,
        scratch_shapes=[pltpu.SemaphoreType.DMA((32,)), pltpu.SemaphoreType.DMA((48,))],
    )(design, goal)


def start_kernel(mat, out):
    part = jnp.zeros((T, BLOCK), F32)
    for src in range(8):
        goal = jnp.concatenate(
            [mat[src, 128:136, t * 128 : (t + 1) * 128].astype(F32) for t in range(6)], axis=0
        ).astype(BF)
        part = part + dot(goal, mat[src, :128, :])
    high, low = split16(part)
    high, low = high.astype(BF), low.astype(BF)
    for to in range(N_ZH):
        out[to, :, :BLOCK] = high
        out[to, :, BLOCK:] = low[:, to * 256 : (to + 1) * 256]


def cross_kernel(mat, fac, gram, out):
    factor = fac[...]
    for src in range(8):
        block = dot(mat[src, :128, :], factor).astype(BF)
        out[src * 256 : src * 256 + 128, :] = block[:, :128]
        out[src * 256 + 128 : src * 256 + 256, :] = block[:, 128:]
    both = gram[...].astype(BF)
    out[2048:2304, :] = both[:, :128]
    out[2304:2560, :] = both[:, 128:]


def write_head(residual, direction, mat, fac, out):
    low = residual.astype(BF)
    for src in range(8):
        out[src * T : (src + 1) * T, :] = dot_t(low, mat[src, :128, :]).astype(BF)
    seen = dot(low, fac[...]).astype(BF)
    out[384:432, :] = seen[:, :128]
    out[432:480, :] = seen[:, 128:]
    rr = split16(total_of(residual * residual))
    rd = split16(total_of(residual * direction))
    block = jnp.concatenate([columns([*rr, *rd]), jnp.zeros((80, 128), F32)], axis=0)
    tile = block.T[:32, :]
    out[SCAL:HEAD, :] = tile.astype(BF)


def first_kernel(arrived, mat, fac, rest, out, start_out, held, sem):
    total = jnp.zeros((T, BLOCK + 256), F32)
    for source in range(N_ZH):
        total = total + arrived[source].astype(F32)
    held[...] = total
    store = pltpu.make_async_copy(held, start_out, sem.at[0])
    store.start()
    residual = total[:, :BLOCK]
    write_head(residual, residual, mat, fac, out)
    out[HEAD:, :] = rest[...]
    store.wait()


def first_call(arrived, mat, fac, rest):
    return pl.pallas_call(
        first_kernel,
        out_shape=(shape(3072, 128, dtype=BF), shape(T, BLOCK + 256)),
        in_specs=[IN_VMEM] * 4,
        out_specs=(IN_VMEM, IN_HBM),
        scratch_shapes=[pltpu.VMEM((T, BLOCK + 256), F32), pltpu.SemaphoreType.DMA((1,))],
        compiler_params=PARAMS,
    )(arrived, mat, fac, rest)


def own_part(array, zh):
    mine = array[:, :256]
    for index in range(1, N_ZH):
        mine = jnp.where(zh == index, array[:, index * 256 : (index + 1) * 256], mine)
    return mine


D_AT, R_AT, S_AT, C_AT, WIDE = 0, BLOCK, 2 * BLOCK, 2 * BLOCK + RANK, 2 * BLOCK + RANK + 128


def next_kernel(more, arrived, zh, penalty, mat, state, residual_in, fac_in, *refs):
    refs = list(refs)
    answer_in = refs.pop(0) if more else None
    out, residual_out, answer_out, direction_v, scal_v, residual_v, fac_v, answer_v, sems = refs
    copies = fetch(
        [
            (state.at[:, D_AT:R_AT], direction_v),
            (state.at[:, C_AT:WIDE], scal_v),
            (residual_in.at[:, :BLOCK], residual_v),
            (fac_in, fac_v),
        ]
        + ([(answer_in, answer_v)] if more else []),
        sems,
    )
    hess = jnp.zeros((T, BLOCK + 128), F32)
    for source in range(N_ZH):
        hess = hess + arrived[source].astype(F32)
    square = hess[:, BLOCK : BLOCK + 1] + hess[:, BLOCK + 1 : BLOCK + 2]
    hess = hess[:, :BLOCK]
    ridge = penalty[:, :1]
    for copy in copies[:3]:
        copy.wait()
    inner, dd = scal_v[:, :1], scal_v[:, 1:2]
    direction = direction_v[...]
    step = inner / (square + ridge * dd)
    residual = residual_v[...] - step * (hess + ridge * direction)
    residual_v[...] = residual
    answer = step * own_part(direction, zh[0])
    if more:
        copies[4].wait()
        answer = answer_v[...] + answer
    answer_v[...] = answer
    stores = [
        pltpu.make_async_copy(residual_v, residual_out, sems.at[5]),
        pltpu.make_async_copy(answer_v, answer_out, sems.at[6]),
    ]
    for copy in stores:
        copy.start()
    copies[3].wait()
    write_head(residual, direction, mat, fac_v, out)
    for copy in stores:
        copy.wait()


def next_call(arrived, zh, ridge, mat, state, residual, fac, answer):
    more = answer is not None
    extra = (answer,) if more else ()
    return pl.pallas_call(
        lambda *refs: next_kernel(more, *refs),
        out_shape=(shape(HEAD, 128, dtype=BF), shape(T, BLOCK), shape(T, 256)),
        in_specs=[IN_VMEM, IN_SMEM, IN_VMEM, IN_VMEM] + [IN_HBM] * (3 + len(extra)),
        out_specs=(IN_VMEM, IN_HBM, IN_HBM),
        scratch_shapes=[
            pltpu.VMEM((T, BLOCK), F32),
            pltpu.VMEM((T, 128), F32),
            pltpu.VMEM((T, BLOCK), F32),
            pltpu.VMEM((BLOCK, RANK), BF),
            pltpu.VMEM((T, 256), F32),
            pltpu.SemaphoreType.DMA((7,)),
        ],
        compiler_params=PARAMS,
    )(arrived, zh, ridge, mat, state, residual, fac, *extra)


def search_kernel(first, last, back, zh, weights, mat, residual_in, fac_in, *refs):
    refs = list(refs)
    state_in = None if first else refs.pop(0)
    full = back if first else refs.pop(0)
    answer_in, fix_in = (refs.pop(0), refs.pop(0)) if last else (None, None)
    out, state_out, residual_v, fac_v, sems = refs[:5]
    refs = refs[5:]
    pairs = [(residual_in.at[:, :BLOCK], residual_v), (fac_in, fac_v)]
    if not first:
        state_v, full_v = refs[:2]
        pairs += [(state_in, state_v), (full.at[HEAD:, :], full_v)]
        full, base = full_v, 0
    else:
        state_v = refs[0]
        base = HEAD
    if last:
        answer_v, fix_v, tail_v = refs[2:]
        pairs += [(answer_in, answer_v), (fix_in.at[:, BLOCK:], fix_v)]
    copies = fetch(pairs, sems)

    projected = jnp.concatenate([back[384:432, :], back[432:480, :]], axis=1).astype(F32)
    tile = jnp.concatenate([back[SCAL:HEAD, :].astype(F32), jnp.zeros((96, 128), F32)], axis=0).T
    rr = tile[:T, 0:1] + tile[:T, 1:2]
    rd = tile[:T, 2:3] + tile[:T, 3:4]
    scaled = weights[0:1, :] * projected
    cross_inner = total_of(scaled * projected)
    inner = rr + cross_inner
    low = scaled.astype(BF)
    if not first:
        copies[2].wait()
        copies[3].wait()
    gram = base + 2048
    through = jnp.concatenate(
        [dot(low, full[gram : gram + 256, :]), dot(low, full[gram + 256 : gram + 512, :])], axis=1
    )
    dd = rr + 2.0 * cross_inner + total_of(scaled * through)
    seen = projected + through
    if not first:
        before, dd_before = state_v[:, C_AT : C_AT + 1], state_v[:, C_AT + 1 : C_AT + 2]
        beta = inner / before
        sd = rd + total_of(scaled * state_v[:, S_AT:C_AT])
        dd = dd + 2.0 * beta * sd + beta * beta * dd_before
        seen = seen + beta * state_v[:, S_AT:C_AT]
    part = jnp.zeros((T, BLOCK), F32)
    square = jnp.zeros((T, 1), F32)
    for src in range(8):
        at = base + src * 256
        row = back[src * T : (src + 1) * T, :].astype(F32)
        row = row + dot_t(low[:, :128], full[at : at + 128, :])
        row = row + dot_t(low[:, 128:], full[at + 128 : at + 256, :])
        lanes = slice(R_AT + src * 128, R_AT + (src + 1) * 128)
        if not first:
            row = row + beta * state_v[:, lanes]
        state_v[:, lanes] = row
        row_low = row.astype(BF)
        square = square + total_of(row * row_low.astype(F32))
        part = part + dot(row_low, mat[src, :128, :])
    copies[0].wait()
    copies[1].wait()
    direction = residual_v[...] + dot_t(low, fac_v[...])
    if not first:
        direction = direction + beta * state_v[:, D_AT:R_AT]
    if last:
        copies[4].wait()
        copies[5].wait()
        tail_v[:, :256] = own_part(direction, zh[0])
        tail_v[:, 256:512] = answer_v[...]
        tail_v[:, 512:768] = own_part(residual_v[...], zh[0]) + fix_v[...]
        tail_v[:, 768:] = columns([inner, dd])
        store = pltpu.make_async_copy(tail_v, state_out, sems.at[6])
    else:
        state_v[:, D_AT:R_AT] = direction
        state_v[:, S_AT:C_AT] = seen
        state_v[:, C_AT:WIDE] = columns([inner, dd])
        store = pltpu.make_async_copy(state_v, state_out, sems.at[6])
    store.start()
    extra = columns(split16(square)).astype(BF)
    high, low = split16(part)
    high, low = high.astype(BF), low.astype(BF)
    for to in range(N_ZH):
        if last:
            mine = slice(to * 256, (to + 1) * 256)
            out[to, :, :256] = high[:, mine]
            out[to, :, 256:512] = low[:, mine]
            out[to, :, 512:] = extra
        else:
            out[to, :, :BLOCK] = high
            out[to, :, BLOCK:] = extra
    store.wait()


def search_call(first, last, back, zh, weights, mat, residual, fac, state, full, answer, fix):
    hbm = [residual, fac]
    if not first:
        hbm += [state, full]
    if last:
        hbm += [answer, fix]
    scratch = [
        pltpu.VMEM((T, BLOCK), F32),
        pltpu.VMEM((BLOCK, RANK), BF),
        pltpu.SemaphoreType.DMA((7,)),
        pltpu.VMEM((T, WIDE), F32),
    ]
    if not first:
        scratch.append(pltpu.VMEM((2560, 128), BF))
    if last:
        scratch += [pltpu.VMEM((T, 256), F32), pltpu.VMEM((T, 256), F32), pltpu.VMEM((T, 896), F32)]
    return pl.pallas_call(
        lambda *refs: search_kernel(first, last, *refs),
        out_shape=(
            shape(N_ZH, T, 640 if last else BLOCK + 128, dtype=BF),
            shape(T, 896 if last else WIDE),
        ),
        in_specs=[IN_VMEM, IN_SMEM, IN_VMEM, IN_VMEM] + [IN_HBM] * len(hbm),
        out_specs=(IN_VMEM, IN_HBM),
        scratch_shapes=scratch,
        compiler_params=PARAMS,
    )(back, zh, weights, mat, *hbm)


def middle_kernel(pieces, me, out):
    count = pieces.shape[1]
    total = jnp.zeros((count, 128), F32)
    for source in range(N_MANY):
        total = total + pieces[source].astype(F32)
    tile = total[:8]
    high_a, low_a = split16(tile[0:1] + tile[1:2])
    high_b, low_b = split16(tile[2:3] + tile[3:4])
    line = lax.broadcasted_iota(jnp.int32, (8, 128), 0)
    again = tile
    for index, value in enumerate((high_a, low_a, high_b, low_b)):
        again = jnp.where(line == index, value, again)
    tile = jnp.where(me[0] == SCAL // count, again, tile)
    if count > 8:
        tile = jnp.concatenate([tile, total[8:]], axis=0)
    tile = tile.astype(BF)
    for target in range(N_MANY):
        out[target] = tile


def middle(pieces, me):
    return pl.pallas_call(
        middle_kernel,
        out_shape=shape(*pieces.shape, dtype=BF),
        in_specs=[IN_VMEM, IN_SMEM],
        out_specs=IN_VMEM,
        compiler_params=PARAMS,
    )(pieces, me)


def final_kernel(arrived, tail, penalty, answer_out, residual_out):
    total = jnp.zeros((T, 640), F32)
    for source in range(N_ZH):
        total = total + arrived[source].astype(F32)
    square = total[:, 512:513] + total[:, 513:514]
    ridge = penalty[:, :1]
    mine = tail[:, :256]
    step = tail[:, 768:769] / (square + ridge * tail[:, 769:770])
    hess = total[:, :256] + total[:, 256:512] + ridge * mine
    answer_out[...] = tail[:, 256:512] + step * mine
    residual_out[...] = tail[:, 512:768] - step * hess


def shards(design, targets, factor, weights, penalty):
    zh = lax.axis_index("zh")
    me = lax.axis_index(MANY).reshape(1)
    low_factor = factor.astype(BF)
    slots = jnp.zeros((N_ZH, 256, RANK), BF)
    slots = lax.dynamic_update_slice(slots, low_factor[None], (zh, 0, 0))
    for shift in range(1, N_ZH):
        pairs = [(i, (i + shift) % N_ZH) for i in range(N_ZH)]
        other = lax.ppermute(low_factor, "zh", pairs)
        slots = lax.dynamic_update_slice(slots, other[None], ((zh - shift) % N_ZH, 0, 0))
    fac = slots.reshape(BLOCK, RANK)

    mat = exchange(pack(design, targets.T), OWN)
    arrived = exchange(call(start_kernel, shape(N_ZH, T, BLOCK + 256, dtype=BF))(mat), "zh")
    gram = lax.dot_general(fac, fac, (((0,), (0,)), ((), ())), preferred_element_type=F32)
    rest = call(cross_kernel, shape(2560, 128, dtype=BF))(mat, fac, gram)

    w = jnp.broadcast_to(weights[None, :], (8, RANK))
    ridge = jnp.broadcast_to(penalty[:, None], (T, 128))
    spot = zh.reshape(1)

    def over_many(packed):
        pieces = packed.reshape(N_MANY, -1, 128)
        total = middle(exchange(pieces, MANY), me)
        return exchange(total, MANY).reshape(packed.shape)

    packed, residual = first_call(arrived, mat, fac, rest)
    fix = residual
    answer = state = full = None
    for step_index in range(ITERS):
        first, last = step_index == 0, step_index == ITERS - 1
        back = over_many(packed)
        full = back if first else full
        send, state = search_call(
            first, last, back, spot, w, mat, residual, fac, state, full, answer, fix
        )
        arrived = exchange(send, "zh")
        if not last:
            packed, residual, answer = next_call(
                arrived, spot, ridge, mat, state, residual, fac, answer
            )
    answer, residual = call(final_kernel, (shape(T, 256), shape(T, 256)))(arrived, state, ridge)
    return answer.T, residual.T


def solution(mesh):
    finer = Mesh(mesh.devices.reshape(4, 2, 4, 4, 2), ("zh", "zl", "y", "x", "c"))
    spec = P((*FEAT, *ROW), None)
    in_specs = (P(ROW, FEAT), P(ROW, None), spec, P(), P())
    return jax.shard_map(
        shards, mesh=finer, in_specs=in_specs, out_specs=(spec, spec), check_vma=False
    )
```

```python
import jax
import jax.numpy as jnp
from jax import lax
from jax.experimental import pallas as pl
from jax.experimental.pallas import tpu as pltpu
from jax.sharding import Mesh
from jax.sharding import PartitionSpec as P

ITERS = 3
ROW = ("zh", "zl", "y")
FEAT = ("x", "c")
OWN = ("zl", "y")
MANY = ("zl", "y", "x", "c")
N_OWN, N_MANY, N_ZH = 8, 64, 4
T, RANK, BLOCK = 48, 256, 1024
SCAL = 480
HEAD = 512
BF = jnp.bfloat16
F32 = jnp.float32


def exchange(pieces, axes):
    return lax.all_to_all(pieces, axes, 0, 0, tiled=True)


def dot(a, b):
    return jnp.dot(a, b, preferred_element_type=F32)


def dot_t(a, b):
    return lax.dot_general(a, b, (((1,), (1,)), ((), ())), preferred_element_type=F32)


PARAMS = pltpu.CompilerParams(vmem_limit_bytes=20 * 1024 * 1024)


IN_HBM = pl.BlockSpec(memory_space=pltpu.HBM)
IN_VMEM = pl.BlockSpec(memory_space=pltpu.VMEM)
IN_SMEM = pl.BlockSpec(memory_space=pltpu.SMEM)


def call(body, out):
    return pl.pallas_call(body, out_shape=out, compiler_params=PARAMS)


def fetch(pairs, sems):
    copies = [pltpu.make_async_copy(a, b, sems.at[i]) for i, (a, b) in enumerate(pairs)]
    for copy in copies:
        copy.start()
    return copies


def shape(*dims, dtype=F32):
    return jax.ShapeDtypeStruct(dims, dtype)


def columns(parts):
    lane = lax.broadcasted_iota(jnp.int32, (T, 128), 1)
    block = jnp.zeros((T, 128), F32)
    for index, part in enumerate(parts):
        block = jnp.where(lane == index, part, block)
    return block


def split16(value):
    high = value.astype(BF).astype(F32)
    return high, value - high


def total_of(array):
    return jnp.sum(array, axis=1, keepdims=True)


CHUNKS, DEEP = 4, 32


def pack_kernel(design, goal, out, rows, packed, goals, sems):
    def inward(index):
        at = pl.ds(index * DEEP, DEEP)
        return pltpu.make_async_copy(design.at[at, :], rows.at[at, :], sems.at[index])

    def outward(index):
        at = pl.ds(index * DEEP, DEEP)
        return pltpu.make_async_copy(
            packed.at[:, at, :], out.at[:, at, :], sems.at[CHUNKS + index]
        )

    for index in range(CHUNKS):
        inward(index).start()
    for to in range(8):
        for index in range(6):
            goals[to, :, index * 128 : (index + 1) * 128] = goal[index * 8 : index * 8 + 8, :]
        goals[to, :, 768:] = jnp.zeros((8, 256), BF)
    last = pltpu.make_async_copy(goals, out.at[:, 128:136, :], sems.at[2 * CHUNKS])
    last.start()
    for index in range(CHUNKS):
        inward(index).wait()
        low, high = index * DEEP, (index + 1) * DEEP
        for to in range(8):
            for part in range(4):
                at = (part * 8 + to) * 256
                packed[to, low:high, part * 256 : (part + 1) * 256] = rows[low:high, at : at + 256]
        outward(index).start()
    for index in range(CHUNKS):
        outward(index).wait()
    last.wait()


def pack(design, goal):
    return pl.pallas_call(
        pack_kernel,
        out_shape=shape(8, 136, BLOCK, dtype=BF),
        in_specs=[IN_HBM, IN_VMEM],
        out_specs=IN_HBM,
        scratch_shapes=[
            pltpu.VMEM((128, 8192), BF),
            pltpu.VMEM((8, 128, BLOCK), BF),
            pltpu.VMEM((8, 8, BLOCK), BF),
            pltpu.SemaphoreType.DMA((2 * CHUNKS + 1,)),
        ],
    )(design, goal)


def start_kernel(mat, out):
    part = jnp.zeros((T, BLOCK), F32)
    for src in range(8):
        goal = jnp.concatenate(
            [mat[src, 128:136, t * 128 : (t + 1) * 128].astype(F32) for t in range(6)], axis=0
        ).astype(BF)
        part = part + dot(goal, mat[src, :128, :])
    high, low = split16(part)
    high, low = high.astype(BF), low.astype(BF)
    for to in range(N_ZH):
        out[to, :, :BLOCK] = high
        out[to, :, BLOCK:] = low[:, to * 256 : (to + 1) * 256]


def cross_kernel(mat, fac, gram, out):
    factor = fac[...]
    for src in range(8):
        block = dot(mat[src, :128, :], factor).astype(BF)
        out[src * 256 : src * 256 + 128, :] = block[:, :128]
        out[src * 256 + 128 : src * 256 + 256, :] = block[:, 128:]
    both = gram[...].astype(BF)
    out[2048:2304, :] = both[:, :128]
    out[2304:2560, :] = both[:, 128:]


def write_head(residual, direction, mat, fac, out):
    low = residual.astype(BF)
    for src in range(8):
        out[src * T : (src + 1) * T, :] = dot_t(low, mat[src, :128, :]).astype(BF)
    seen = dot(low, fac[...]).astype(BF)
    out[384:432, :] = seen[:, :128]
    out[432:480, :] = seen[:, 128:]
    rr = split16(total_of(residual * residual))
    rd = split16(total_of(residual * direction))
    block = jnp.concatenate([columns([*rr, *rd]), jnp.zeros((80, 128), F32)], axis=0)
    tile = block.T[:32, :]
    out[SCAL:HEAD, :] = tile.astype(BF)


def first_kernel(arrived, mat, fac, rest, out, start_out, held, sem):
    total = jnp.zeros((T, BLOCK + 256), F32)
    for source in range(N_ZH):
        total = total + arrived[source].astype(F32)
    held[...] = total
    store = pltpu.make_async_copy(held, start_out, sem.at[0])
    store.start()
    residual = total[:, :BLOCK]
    write_head(residual, residual, mat, fac, out)
    out[HEAD:, :] = rest[...]
    store.wait()


def first_call(arrived, mat, fac, rest):
    return pl.pallas_call(
        first_kernel,
        out_shape=(shape(3072, 128, dtype=BF), shape(T, BLOCK + 256)),
        in_specs=[IN_VMEM] * 4,
        out_specs=(IN_VMEM, IN_HBM),
        scratch_shapes=[pltpu.VMEM((T, BLOCK + 256), F32), pltpu.SemaphoreType.DMA((1,))],
        compiler_params=PARAMS,
    )(arrived, mat, fac, rest)


def own_part(array, zh):
    mine = array[:, :256]
    for index in range(1, N_ZH):
        mine = jnp.where(zh == index, array[:, index * 256 : (index + 1) * 256], mine)
    return mine


D_AT, R_AT, S_AT, C_AT, WIDE = 0, BLOCK, 2 * BLOCK, 2 * BLOCK + RANK, 2 * BLOCK + RANK + 128


def next_kernel(more, arrived, zh, penalty, mat, state, residual_in, fac_in, *refs):
    refs = list(refs)
    answer_in = refs.pop(0) if more else None
    out, residual_out, answer_out, direction_v, scal_v, residual_v, fac_v, answer_v, sems = refs
    copies = fetch(
        [
            (state.at[:, D_AT:R_AT], direction_v),
            (state.at[:, C_AT:WIDE], scal_v),
            (residual_in.at[:, :BLOCK], residual_v),
            (fac_in, fac_v),
        ]
        + ([(answer_in, answer_v)] if more else []),
        sems,
    )
    hess = jnp.zeros((T, BLOCK + 128), F32)
    for source in range(N_ZH):
        hess = hess + arrived[source].astype(F32)
    square = hess[:, BLOCK : BLOCK + 1] + hess[:, BLOCK + 1 : BLOCK + 2]
    hess = hess[:, :BLOCK]
    ridge = penalty[:, :1]
    for copy in copies[:3]:
        copy.wait()
    inner, dd = scal_v[:, :1], scal_v[:, 1:2]
    direction = direction_v[...]
    step = inner / (square + ridge * dd)
    residual = residual_v[...] - step * (hess + ridge * direction)
    residual_v[...] = residual
    answer = step * own_part(direction, zh[0])
    if more:
        copies[4].wait()
        answer = answer_v[...] + answer
    answer_v[...] = answer
    stores = [
        pltpu.make_async_copy(residual_v, residual_out, sems.at[5]),
        pltpu.make_async_copy(answer_v, answer_out, sems.at[6]),
    ]
    for copy in stores:
        copy.start()
    copies[3].wait()
    write_head(residual, direction, mat, fac_v, out)
    for copy in stores:
        copy.wait()


def next_call(arrived, zh, ridge, mat, state, residual, fac, answer):
    more = answer is not None
    extra = (answer,) if more else ()
    return pl.pallas_call(
        lambda *refs: next_kernel(more, *refs),
        out_shape=(shape(HEAD, 128, dtype=BF), shape(T, BLOCK), shape(T, 256)),
        in_specs=[IN_VMEM, IN_SMEM, IN_VMEM, IN_VMEM] + [IN_HBM] * (3 + len(extra)),
        out_specs=(IN_VMEM, IN_HBM, IN_HBM),
        scratch_shapes=[
            pltpu.VMEM((T, BLOCK), F32),
            pltpu.VMEM((T, 128), F32),
            pltpu.VMEM((T, BLOCK), F32),
            pltpu.VMEM((BLOCK, RANK), BF),
            pltpu.VMEM((T, 256), F32),
            pltpu.SemaphoreType.DMA((7,)),
        ],
        compiler_params=PARAMS,
    )(arrived, zh, ridge, mat, state, residual, fac, *extra)


def search_kernel(first, last, back, zh, weights, mat, residual_in, fac_in, *refs):
    refs = list(refs)
    state_in = None if first else refs.pop(0)
    full = back if first else refs.pop(0)
    answer_in, fix_in = (refs.pop(0), refs.pop(0)) if last else (None, None)
    out, state_out, residual_v, fac_v, sems = refs[:5]
    refs = refs[5:]
    pairs = [(residual_in.at[:, :BLOCK], residual_v), (fac_in, fac_v)]
    if not first:
        state_v, full_v = refs[:2]
        pairs += [(state_in, state_v), (full.at[HEAD:, :], full_v)]
        full, base = full_v, 0
    else:
        state_v = refs[0]
        base = HEAD
    if last:
        answer_v, fix_v, tail_v = refs[2:]
        pairs += [(answer_in, answer_v), (fix_in.at[:, BLOCK:], fix_v)]
    copies = fetch(pairs, sems)

    projected = jnp.concatenate([back[384:432, :], back[432:480, :]], axis=1).astype(F32)
    tile = jnp.concatenate([back[SCAL:HEAD, :].astype(F32), jnp.zeros((96, 128), F32)], axis=0).T
    rr = tile[:T, 0:1] + tile[:T, 1:2]
    rd = tile[:T, 2:3] + tile[:T, 3:4]
    scaled = weights[0:1, :] * projected
    cross_inner = total_of(scaled * projected)
    inner = rr + cross_inner
    low = scaled.astype(BF)
    if not first:
        copies[2].wait()
        copies[3].wait()
    gram = base + 2048
    through = jnp.concatenate(
        [dot(low, full[gram : gram + 256, :]), dot(low, full[gram + 256 : gram + 512, :])], axis=1
    )
    dd = rr + 2.0 * cross_inner + total_of(scaled * through)
    seen = projected + through
    if not first:
        before, dd_before = state_v[:, C_AT : C_AT + 1], state_v[:, C_AT + 1 : C_AT + 2]
        beta = inner / before
        sd = rd + total_of(scaled * state_v[:, S_AT:C_AT])
        dd = dd + 2.0 * beta * sd + beta * beta * dd_before
        seen = seen + beta * state_v[:, S_AT:C_AT]
    part = jnp.zeros((T, BLOCK), F32)
    square = jnp.zeros((T, 1), F32)
    for src in range(8):
        at = base + src * 256
        row = back[src * T : (src + 1) * T, :].astype(F32)
        row = row + dot_t(low[:, :128], full[at : at + 128, :])
        row = row + dot_t(low[:, 128:], full[at + 128 : at + 256, :])
        lanes = slice(R_AT + src * 128, R_AT + (src + 1) * 128)
        if not first:
            row = row + beta * state_v[:, lanes]
        state_v[:, lanes] = row
        row_low = row.astype(BF)
        square = square + total_of(row * row_low.astype(F32))
        part = part + dot(row_low, mat[src, :128, :])
    copies[0].wait()
    copies[1].wait()
    direction = residual_v[...] + dot_t(low, fac_v[...])
    if not first:
        direction = direction + beta * state_v[:, D_AT:R_AT]
    if last:
        copies[4].wait()
        copies[5].wait()
        tail_v[:, :256] = own_part(direction, zh[0])
        tail_v[:, 256:512] = answer_v[...]
        tail_v[:, 512:768] = own_part(residual_v[...], zh[0]) + fix_v[...]
        tail_v[:, 768:] = columns([inner, dd])
        store = pltpu.make_async_copy(tail_v, state_out, sems.at[6])
    else:
        state_v[:, D_AT:R_AT] = direction
        state_v[:, S_AT:C_AT] = seen
        state_v[:, C_AT:WIDE] = columns([inner, dd])
        store = pltpu.make_async_copy(state_v, state_out, sems.at[6])
    store.start()
    extra = columns(split16(square)).astype(BF)
    high, low = split16(part)
    high, low = high.astype(BF), low.astype(BF)
    for to in range(N_ZH):
        if last:
            mine = slice(to * 256, (to + 1) * 256)
            out[to, :, :256] = high[:, mine]
            out[to, :, 256:512] = low[:, mine]
            out[to, :, 512:] = extra
        else:
            out[to, :, :BLOCK] = high
            out[to, :, BLOCK:] = extra
    store.wait()


def search_call(first, last, back, zh, weights, mat, residual, fac, state, full, answer, fix):
    hbm = [residual, fac]
    if not first:
        hbm += [state, full]
    if last:
        hbm += [answer, fix]
    scratch = [
        pltpu.VMEM((T, BLOCK), F32),
        pltpu.VMEM((BLOCK, RANK), BF),
        pltpu.SemaphoreType.DMA((7,)),
        pltpu.VMEM((T, WIDE), F32),
    ]
    if not first:
        scratch.append(pltpu.VMEM((2560, 128), BF))
    if last:
        scratch += [pltpu.VMEM((T, 256), F32), pltpu.VMEM((T, 256), F32), pltpu.VMEM((T, 896), F32)]
    return pl.pallas_call(
        lambda *refs: search_kernel(first, last, *refs),
        out_shape=(
            shape(N_ZH, T, 640 if last else BLOCK + 128, dtype=BF),
            shape(T, 896 if last else WIDE),
        ),
        in_specs=[IN_VMEM, IN_SMEM, IN_VMEM, IN_VMEM] + [IN_HBM] * len(hbm),
        out_specs=(IN_VMEM, IN_HBM),
        scratch_shapes=scratch,
        compiler_params=PARAMS,
    )(back, zh, weights, mat, *hbm)


def middle_kernel(pieces, me, out):
    count = pieces.shape[1]
    total = jnp.zeros((count, 128), F32)
    for source in range(N_MANY):
        total = total + pieces[source].astype(F32)
    tile = total[:8]
    high_a, low_a = split16(tile[0:1] + tile[1:2])
    high_b, low_b = split16(tile[2:3] + tile[3:4])
    line = lax.broadcasted_iota(jnp.int32, (8, 128), 0)
    again = tile
    for index, value in enumerate((high_a, low_a, high_b, low_b)):
        again = jnp.where(line == index, value, again)
    tile = jnp.where(me[0] == SCAL // count, again, tile)
    if count > 8:
        tile = jnp.concatenate([tile, total[8:]], axis=0)
    tile = tile.astype(BF)
    for target in range(N_MANY):
        out[target] = tile


def middle(pieces, me):
    return pl.pallas_call(
        middle_kernel,
        out_shape=shape(*pieces.shape, dtype=BF),
        in_specs=[IN_VMEM, IN_SMEM],
        out_specs=IN_VMEM,
        compiler_params=PARAMS,
    )(pieces, me)


def final_kernel(arrived, tail, penalty, answer_out, residual_out):
    total = jnp.zeros((T, 640), F32)
    for source in range(N_ZH):
        total = total + arrived[source].astype(F32)
    square = total[:, 512:513] + total[:, 513:514]
    ridge = penalty[:, :1]
    mine = tail[:, :256]
    step = tail[:, 768:769] / (square + ridge * tail[:, 769:770])
    hess = total[:, :256] + total[:, 256:512] + ridge * mine
    answer_out[...] = tail[:, 256:512] + step * mine
    residual_out[...] = tail[:, 512:768] - step * hess


def shards(design, targets, factor, weights, penalty):
    zh = lax.axis_index("zh")
    me = lax.axis_index(MANY).reshape(1)
    low_factor = factor.astype(BF)
    slots = jnp.zeros((N_ZH, 256, RANK), BF)
    slots = lax.dynamic_update_slice(slots, low_factor[None], (zh, 0, 0))
    for shift in range(1, N_ZH):
        pairs = [(i, (i + shift) % N_ZH) for i in range(N_ZH)]
        other = lax.ppermute(low_factor, "zh", pairs)
        slots = lax.dynamic_update_slice(slots, other[None], ((zh - shift) % N_ZH, 0, 0))
    fac = slots.reshape(BLOCK, RANK)

    mat = exchange(pack(design, targets.T), OWN)
    arrived = exchange(call(start_kernel, shape(N_ZH, T, BLOCK + 256, dtype=BF))(mat), "zh")
    gram = lax.dot_general(fac, fac, (((0,), (0,)), ((), ())), preferred_element_type=F32)
    rest = call(cross_kernel, shape(2560, 128, dtype=BF))(mat, fac, gram)

    w = jnp.broadcast_to(weights[None, :], (8, RANK))
    ridge = jnp.broadcast_to(penalty[:, None], (T, 128))
    spot = zh.reshape(1)

    def over_many(packed):
        pieces = packed.reshape(N_MANY, -1, 128)
        total = middle(exchange(pieces, MANY), me)
        return exchange(total, MANY).reshape(packed.shape)

    packed, residual = first_call(arrived, mat, fac, rest)
    fix = residual
    answer = state = full = None
    for step_index in range(ITERS):
        first, last = step_index == 0, step_index == ITERS - 1
        back = over_many(packed)
        full = back if first else full
        send, state = search_call(
            first, last, back, spot, w, mat, residual, fac, state, full, answer, fix
        )
        arrived = exchange(send, "zh")
        if not last:
            packed, residual, answer = next_call(
                arrived, spot, ridge, mat, state, residual, fac, answer
            )
    answer, residual = call(final_kernel, (shape(T, 256), shape(T, 256)))(arrived, state, ridge)
    return answer.T, residual.T


def solution(mesh):
    finer = Mesh(mesh.devices.reshape(4, 2, 4, 4, 2), ("zh", "zl", "y", "x", "c"))
    spec = P((*FEAT, *ROW), None)
    in_specs = (P(ROW, FEAT), P(ROW, None), spec, P(), P())
    return jax.shard_map(
        shards, mesh=finer, in_specs=in_specs, out_specs=(spec, spec), check_vma=False
    )
```

```python
import jax
import jax.numpy as jnp
from jax import lax
from jax.experimental import pallas as pl
from jax.experimental.pallas import tpu as pltpu
from jax.sharding import Mesh
from jax.sharding import PartitionSpec as P

ITERS = 3
ROW = ("z", "y")
FEAT = ("x", "c")
MANY = ("y", "x", "c")
N_Y, N_MANY, N_Z = 4, 32, 8
T, RANK, OWN = 48, 256, 256
ROWS, WIDTH = 128, N_Z * OWN
SEEN, SCAL, HEAD = N_Y * T, 320, 512
CROSS, REST = N_Y * 256, N_Y * 256 + 512
BF = jnp.bfloat16
F32 = jnp.float32
IN_HBM = pl.BlockSpec(memory_space=pltpu.HBM)
IN_VMEM = pl.BlockSpec(memory_space=pltpu.VMEM)
IN_SMEM = pl.BlockSpec(memory_space=pltpu.SMEM)
PARAMS = pltpu.CompilerParams(vmem_limit_bytes=20 * 1024 * 1024)


def exchange(pieces, axes):
    return lax.all_to_all(pieces, axes, 0, 0, tiled=True)


def dot(a, b):
    return jnp.dot(a, b, preferred_element_type=F32)


def dot_t(a, b):
    return lax.dot_general(a, b, (((1,), (1,)), ((), ())), preferred_element_type=F32)


def call(body, out):
    return pl.pallas_call(body, out_shape=out, compiler_params=PARAMS)


def shape(*dims, dtype=F32):
    return jax.ShapeDtypeStruct(dims, dtype)


def columns(parts):
    lane = lax.broadcasted_iota(jnp.int32, (T, 128), 1)
    block = jnp.zeros((T, 128), F32)
    for index, part in enumerate(parts):
        block = jnp.where(lane == index, part, block)
    return block


def split16(value):
    high = value.astype(BF).astype(F32)
    return high, value - high


def total_of(array):
    return jnp.sum(array, axis=1, keepdims=True)


def as_tile(column, rows):
    block = jnp.concatenate([columns(split16(column)), jnp.zeros((80, 128), F32)], axis=0)
    return block.T[:rows, :].astype(BF)


def from_tile(tile):
    block = jnp.concatenate([tile, jnp.zeros((120, 128), F32)], axis=0).T
    return block[:T, 0:1] + block[:T, 1:2]


CHUNKS, DEEP = 4, 32


def pack_kernel(design, goal, out, rows, packed, goals, sems):
    def inward(index):
        at = pl.ds(index * DEEP, DEEP)
        return pltpu.make_async_copy(design.at[at, :], rows.at[at, :], sems.at[index])

    def outward(index):
        at = pl.ds(index * DEEP, DEEP)
        return pltpu.make_async_copy(
            packed.at[:, at, :], out.at[:, at, :], sems.at[CHUNKS + index]
        )

    for index in range(CHUNKS):
        inward(index).start()
    for to in range(N_Y):
        for index in range(6):
            goals[to, :, index * 128 : (index + 1) * 128] = goal[index * 8 : index * 8 + 8, :]
        goals[to, :, 768:] = jnp.zeros((8, WIDTH - 768), BF)
    last = pltpu.make_async_copy(goals, out.at[:, ROWS : ROWS + 8, :], sems.at[2 * CHUNKS])
    last.start()
    for index in range(CHUNKS):
        inward(index).wait()
        low, high = index * DEEP, (index + 1) * DEEP
        for to in range(N_Y):
            for part in range(N_Z):
                at = (part * N_Y + to) * OWN
                packed[to, low:high, part * OWN : (part + 1) * OWN] = rows[low:high, at : at + OWN]
        outward(index).start()
    for index in range(CHUNKS):
        outward(index).wait()
    last.wait()


def pack(design, goal):
    return pl.pallas_call(
        pack_kernel,
        out_shape=shape(N_Y, ROWS + 8, WIDTH, dtype=BF),
        in_specs=[IN_HBM, IN_VMEM],
        out_specs=IN_HBM,
        scratch_shapes=[
            pltpu.VMEM((ROWS, N_Y * WIDTH), BF),
            pltpu.VMEM((N_Y, ROWS, WIDTH), BF),
            pltpu.VMEM((N_Y, 8, WIDTH), BF),
            pltpu.SemaphoreType.DMA((2 * CHUNKS + 1,)),
        ],
    )(design, goal)


def start_kernel(mat, out):
    part = jnp.zeros((T, WIDTH), F32)
    for src in range(N_Y):
        goal = jnp.concatenate(
            [mat[src, ROWS:, t * 128 : (t + 1) * 128].astype(F32) for t in range(6)], axis=0
        ).astype(BF)
        part = part + dot(goal, mat[src, :ROWS, :])
    for half, values in enumerate(split16(part)):
        values = values.astype(BF)
        for to in range(N_Z):
            for side in range(2):
                at = to * OWN + side * 128
                row = (half * 2 + side) * T
                out[to, row : row + T, :] = values[:, at : at + 128]


def send_own(own, out):
    low = own.astype(BF)
    for to in range(N_Z):
        out[to, :T, :] = low[:, :128]
        out[to, T:, :] = low[:, 128:]


def begin_kernel(arrived, own_out, out):
    total = jnp.zeros((4 * T, 128), F32)
    for source in range(N_Z):
        total = total + arrived[source].astype(F32)
    both = total[: 2 * T] + total[2 * T :]
    own = jnp.concatenate([both[:T], both[T:]], axis=1)
    own_out[...] = own
    send_own(own, out)


def cross_kernel(mat, fac, z, out):
    for src in range(N_Y):
        block = jnp.zeros((ROWS, RANK), F32)
        for index in range(N_Z):
            at = pl.multiple_of(lax.rem(z[0] - index + N_Z, N_Z) * OWN, OWN)
            block = block + dot(mat[src, :ROWS, pl.ds(at, OWN)], fac[index])
        block = block.astype(BF)
        out[src * 256 : src * 256 + 128, :] = block[:, :128]
        out[src * 256 + 128 : src * 256 + 256, :] = block[:, 128:]
    gram = jnp.zeros((RANK, RANK), F32)
    for index in range(N_Z):
        gram = gram + lax.dot_general(
            fac[index], fac[index], (((0,), (0,)), ((), ())), preferred_element_type=F32
        )
    gram = gram.astype(BF)
    out[CROSS : CROSS + 256, :] = gram[:, :128]
    out[CROSS + 256 :, :] = gram[:, 128:]


def head_kernel(first, gathered, mat, z, fac_in, *refs):
    refs = list(refs)
    rest = refs.pop(0) if first else None
    out, fac, sems = refs
    fetch = pltpu.make_async_copy(fac_in, fac, sems.at[0])
    fetch.start()
    residual = jnp.concatenate(
        [gathered[src, side * T : (side + 1) * T, :] for src in range(N_Z) for side in range(2)],
        axis=1,
    )
    for src in range(N_Y):
        out[src * T : (src + 1) * T, :] = dot_t(residual, mat[src, :ROWS, :]).astype(BF)
    wide = residual.astype(F32)
    out[SEEN + 2 * T : SCAL, :] = jnp.zeros((SCAL - SEEN - 2 * T, 128), BF)
    out[SCAL : SCAL + 32, :] = as_tile(total_of(wide * wide), 32)
    out[SCAL + 32 : HEAD, :] = jnp.zeros((HEAD - SCAL - 32, 128), BF)
    if first:
        out[HEAD:, :] = rest[...]
    fetch.wait()
    seen = jnp.zeros((T, RANK), F32)
    for index in range(N_Z):
        src = lax.rem(z[0] - index + N_Z, N_Z)
        block = jnp.concatenate([gathered[src, :T, :], gathered[src, T:, :]], axis=1)
        seen = seen + dot(block, fac[index])
    seen = seen.astype(BF)
    out[SEEN : SEEN + T, :] = seen[:, :128]
    out[SEEN + T : SEEN + 2 * T, :] = seen[:, 128:]


def head(gathered, mat, z, fac, rest=None):
    first = rest is not None
    extra = (rest,) if first else ()
    return pl.pallas_call(
        lambda *refs: head_kernel(first, *refs),
        out_shape=shape(HEAD + (REST if first else 0), 128, dtype=BF),
        in_specs=[IN_VMEM, IN_VMEM, IN_SMEM, IN_HBM] + [IN_VMEM] * len(extra),
        out_specs=IN_VMEM,
        scratch_shapes=[pltpu.VMEM((N_Z, OWN, RANK), BF), pltpu.SemaphoreType.DMA((1,))],
        compiler_params=PARAMS,
    )(gathered, mat, z, fac, *extra)


def middle_kernel(pieces, me, out):
    count = pieces.shape[1]
    total = jnp.zeros((count, 128), F32)
    for source in range(N_MANY):
        total = total + pieces[source].astype(F32)
    tile = total[:8]
    high, low = split16(tile[0:1] + tile[1:2])
    line = lax.broadcasted_iota(jnp.int32, (8, 128), 0)
    again = jnp.where(line == 0, high, jnp.where(line == 1, low, tile))
    tile = jnp.where(me[0] == SCAL // count, again, tile)
    total = jnp.concatenate([tile, total[8:]], axis=0).astype(BF)
    for target in range(N_MANY):
        out[target] = total


def middle(pieces, me):
    return pl.pallas_call(
        middle_kernel,
        out_shape=shape(*pieces.shape, dtype=BF),
        in_specs=[IN_VMEM, IN_SMEM],
        out_specs=IN_VMEM,
        compiler_params=PARAMS,
    )(pieces, me)


def search_kernel(first, back, mat, factor, weights, own_in, *refs):
    refs = list(refs)
    full, direction_in, row_in, seen_in, scal_in = (back, *[None] * 4) if first else refs[:5]
    out, direction_out, row_out, seen_out, scal_out = refs if first else refs[5:]
    projected = jnp.concatenate(
        [back[SEEN : SEEN + T, :], back[SEEN + T : SEEN + 2 * T, :]], axis=1
    ).astype(F32)
    rr = from_tile(back[SCAL : SCAL + 16, :].astype(F32)[:8])
    scaled = weights[0:1, :] * projected
    cross_inner = total_of(scaled * projected)
    inner = rr + cross_inner
    low = scaled.astype(BF)
    gram = HEAD + CROSS
    through = jnp.concatenate(
        [dot(low, full[gram : gram + 256, :]), dot(low, full[gram + 256 : gram + 512, :])], axis=1
    )
    dd = rr + 2.0 * cross_inner + total_of(scaled * through)
    seen = projected + through
    direction = own_in[...] + dot_t(low, factor[...])
    if not first:
        before, dd_before = scal_in[:, :1], scal_in[:, 1:2]
        beta = inner / before
        dd = dd + 2.0 * beta * total_of(scaled * seen_in[...]) + beta * beta * dd_before
        seen = seen + beta * seen_in[...]
        direction = direction + beta * direction_in[...]
    direction_out[...] = direction
    seen_out[...] = seen
    scal_out[...] = columns([inner, dd])
    part = jnp.zeros((T, WIDTH), F32)
    square = jnp.zeros((T, 1), F32)
    for src in range(N_Y):
        at = HEAD + src * 256
        row = back[src * T : (src + 1) * T, :].astype(F32)
        row = row + dot_t(low[:, :128], full[at : at + 128, :])
        row = row + dot_t(low[:, 128:], full[at + 128 : at + 256, :])
        if not first:
            row = row + beta * row_in[:, src * 128 : (src + 1) * 128]
        row_out[:, src * 128 : (src + 1) * 128] = row
        row_low = row.astype(BF)
        square = square + total_of(row * row_low.astype(F32))
        part = part + dot(row_low, mat[src, :ROWS, :])
    part = part.astype(BF)
    tile = as_tile(square, 8)
    for to in range(N_Z):
        for side in range(2):
            at = to * OWN + side * 128
            out[to, side * T : (side + 1) * T, :] = part[:, at : at + 128]
        out[to, 2 * T :, :] = tile


def search(first, *args):
    return pl.pallas_call(
        lambda *refs: search_kernel(first, *refs),
        out_shape=(
            shape(N_Z, 2 * T + 8, 128, dtype=BF),
            shape(T, OWN),
            shape(T, N_Y * 128),
            shape(T, RANK),
            shape(T, 128),
        ),
        compiler_params=PARAMS,
    )(*args)


def stepped(arrived, direction_in, own_in, scal, penalty):
    total = jnp.zeros((2 * T + 8, 128), F32)
    for source in range(N_Z):
        total = total + arrived[source].astype(F32)
    hess = jnp.concatenate([total[:T], total[T : 2 * T]], axis=1)
    square = from_tile(total[2 * T :])
    ridge = penalty[:, :1]
    direction = direction_in[...]
    step = scal[:, :1] / (square + ridge * scal[:, 1:2])
    return own_in[...] - step * (hess + ridge * direction), step * direction


def next_kernel(arrived, direction, own, scal, penalty, *refs):
    refs = list(refs)
    answer = refs.pop(0) if len(refs) == 4 else None
    own_out, answer_out, out = refs
    left, moved = stepped(arrived, direction, own, scal, penalty)
    own_out[...] = left
    answer_out[...] = moved if answer is None else answer[...] + moved
    send_own(left, out)


def final_kernel(arrived, direction, own, scal, penalty, answer, answer_out, own_out):
    left, moved = stepped(arrived, direction, own, scal, penalty)
    own_out[...] = left
    answer_out[...] = answer[...] + moved


def shards(design, targets, factor, weights, penalty):
    z = lax.axis_index("z").reshape(1)
    me = lax.axis_index(MANY).reshape(1)
    low_factor = factor.astype(BF)
    blocks = [low_factor]
    for shift in range(1, N_Z):
        pairs = [(i, (i + shift) % N_Z) for i in range(N_Z)]
        blocks.append(lax.ppermute(low_factor, "z", pairs))
    fac = jnp.stack(blocks)

    mat = exchange(pack(design, targets.T), "y")
    arrived = exchange(call(start_kernel, shape(N_Z, 4 * T, 128, dtype=BF))(mat), "z")
    own, send = call(begin_kernel, (shape(T, OWN), shape(N_Z, 2 * T, 128, dtype=BF)))(arrived)
    gathered = exchange(send, "z")
    rest = pl.pallas_call(
        cross_kernel,
        out_shape=shape(REST, 128, dtype=BF),
        in_specs=[IN_VMEM, IN_VMEM, IN_SMEM],
        out_specs=IN_VMEM,
        compiler_params=PARAMS,
    )(mat, fac, z)

    w = jnp.broadcast_to(weights[None, :], (8, RANK))
    ridge = jnp.broadcast_to(penalty[:, None], (T, 128))
    answer = full = None
    state = ()
    for step_index in range(ITERS):
        first = step_index == 0
        packed = head(gathered, mat, z, fac, rest if first else None)
        pieces = packed.reshape(N_MANY, -1, 128)
        back = exchange(middle(exchange(pieces, MANY), me), MANY).reshape(packed.shape)
        if not first:
            state = (full, direction, row_values, seen, scal)
        else:
            full = back
        send, direction, row_values, seen, scal = search(
            first, back, mat, low_factor, w, own, *state
        )
        arrived = exchange(send, "z")
        args = (arrived, direction, own, scal, ridge) + (() if first else (answer,))
        if step_index + 1 < ITERS:
            own, answer, send = call(
                next_kernel,
                (shape(T, OWN), shape(T, OWN), shape(N_Z, 2 * T, 128, dtype=BF)),
            )(*args)
            gathered = exchange(send, "z")
    answer, own = call(final_kernel, (shape(T, OWN), shape(T, OWN)))(*args)
    return answer.T, own.T


def solution(mesh):
    finer = Mesh(mesh.devices.reshape(8, 4, 4, 2), ("z", "y", "x", "c"))
    spec = P((*FEAT, *ROW), None)
    in_specs = (P(ROW, FEAT), P(ROW, None), spec, P(), P())
    return jax.shard_map(
        shards, mesh=finer, in_specs=in_specs, out_specs=(spec, spec), check_vma=False
    )
```

```python
import jax
import jax.numpy as jnp
from jax import lax
from jax.experimental import pallas as pl
from jax.experimental.pallas import tpu as pltpu
from jax.sharding import Mesh
from jax.sharding import PartitionSpec as P

ITERS = 3
ROW = ("zh", "zl", "y")
FEAT = ("x", "c")
OWNERS = ("zl", "y")
MANY = ("zl", "y", "x", "c")
N_Y, N_MANY, N_Z = 8, 64, 4
T, RANK, OWN = 48, 256, 256
ROWS, WIDTH = 128, N_Z * OWN
SEEN, SCAL, HEAD = N_Y * T, 480, 512
CROSS, REST = N_Y * 256, N_Y * 256 + 512
BF = jnp.bfloat16
F32 = jnp.float32
IN_HBM = pl.BlockSpec(memory_space=pltpu.HBM)
IN_VMEM = pl.BlockSpec(memory_space=pltpu.VMEM)
IN_SMEM = pl.BlockSpec(memory_space=pltpu.SMEM)
PARAMS = pltpu.CompilerParams(vmem_limit_bytes=20 * 1024 * 1024)


def exchange(pieces, axes):
    return lax.all_to_all(pieces, axes, 0, 0, tiled=True)


def dot(a, b):
    return jnp.dot(a, b, preferred_element_type=F32)


def dot_t(a, b):
    return lax.dot_general(a, b, (((1,), (1,)), ((), ())), preferred_element_type=F32)


def call(body, out):
    return pl.pallas_call(body, out_shape=out, compiler_params=PARAMS)


def shape(*dims, dtype=F32):
    return jax.ShapeDtypeStruct(dims, dtype)


def columns(parts):
    lane = lax.broadcasted_iota(jnp.int32, (T, 128), 1)
    block = jnp.zeros((T, 128), F32)
    for index, part in enumerate(parts):
        block = jnp.where(lane == index, part, block)
    return block


def split16(value):
    high = value.astype(BF).astype(F32)
    return high, value - high


def total_of(array):
    return jnp.sum(array, axis=1, keepdims=True)


def as_tile(column, rows):
    block = jnp.concatenate([columns(split16(column)), jnp.zeros((80, 128), F32)], axis=0)
    return block.T[:rows, :].astype(BF)


def from_tile(tile):
    block = jnp.concatenate([tile, jnp.zeros((120, 128), F32)], axis=0).T
    return block[:T, 0:1] + block[:T, 1:2]


CHUNKS, DEEP = 4, 32


def pack_kernel(design, goal, out, rows, packed, goals, sems):
    def inward(index):
        at = pl.ds(index * DEEP, DEEP)
        return pltpu.make_async_copy(design.at[at, :], rows.at[at, :], sems.at[index])

    def outward(index):
        at = pl.ds(index * DEEP, DEEP)
        return pltpu.make_async_copy(
            packed.at[:, at, :], out.at[:, at, :], sems.at[CHUNKS + index]
        )

    for index in range(CHUNKS):
        inward(index).start()
    for to in range(N_Y):
        for index in range(6):
            goals[to, :, index * 128 : (index + 1) * 128] = goal[index * 8 : index * 8 + 8, :]
        goals[to, :, 768:] = jnp.zeros((8, WIDTH - 768), BF)
    last = pltpu.make_async_copy(goals, out.at[:, ROWS : ROWS + 8, :], sems.at[2 * CHUNKS])
    last.start()
    for index in range(CHUNKS):
        inward(index).wait()
        low, high = index * DEEP, (index + 1) * DEEP
        for to in range(N_Y):
            for part in range(N_Z):
                at = (part * N_Y + to) * OWN
                packed[to, low:high, part * OWN : (part + 1) * OWN] = rows[low:high, at : at + OWN]
        outward(index).start()
    for index in range(CHUNKS):
        outward(index).wait()
    last.wait()


def pack(design, goal):
    return pl.pallas_call(
        pack_kernel,
        out_shape=shape(N_Y, ROWS + 8, WIDTH, dtype=BF),
        in_specs=[IN_HBM, IN_VMEM],
        out_specs=IN_HBM,
        scratch_shapes=[
            pltpu.VMEM((ROWS, N_Y * WIDTH), BF),
            pltpu.VMEM((N_Y, ROWS, WIDTH), BF),
            pltpu.VMEM((N_Y, 8, WIDTH), BF),
            pltpu.SemaphoreType.DMA((2 * CHUNKS + 1,)),
        ],
    )(design, goal)


def start_kernel(mat, out):
    part = jnp.zeros((T, WIDTH), F32)
    for src in range(N_Y):
        goal = jnp.concatenate(
            [mat[src, ROWS:, t * 128 : (t + 1) * 128].astype(F32) for t in range(6)], axis=0
        ).astype(BF)
        part = part + dot(goal, mat[src, :ROWS, :])
    for half, values in enumerate(split16(part)):
        values = values.astype(BF)
        for to in range(N_Z):
            for side in range(2):
                at = to * OWN + side * 128
                row = (half * 2 + side) * T
                out[to, row : row + T, :] = values[:, at : at + 128]


def send_own(own, out):
    low = own.astype(BF)
    for to in range(N_Z):
        out[to, :T, :] = low[:, :128]
        out[to, T:, :] = low[:, 128:]


def begin_kernel(arrived, own_out, out):
    total = jnp.zeros((4 * T, 128), F32)
    for source in range(N_Z):
        total = total + arrived[source].astype(F32)
    both = total[: 2 * T] + total[2 * T :]
    own = jnp.concatenate([both[:T], both[T:]], axis=1)
    own_out[...] = own
    send_own(own, out)


def cross_kernel(mat, fac, z, out):
    for src in range(N_Y):
        block = jnp.zeros((ROWS, RANK), F32)
        for index in range(N_Z):
            at = pl.multiple_of(lax.rem(z[0] - index + N_Z, N_Z) * OWN, OWN)
            block = block + dot(mat[src, :ROWS, pl.ds(at, OWN)], fac[index])
        block = block.astype(BF)
        out[src * 256 : src * 256 + 128, :] = block[:, :128]
        out[src * 256 + 128 : src * 256 + 256, :] = block[:, 128:]
    gram = jnp.zeros((RANK, RANK), F32)
    for index in range(N_Z):
        gram = gram + lax.dot_general(
            fac[index], fac[index], (((0,), (0,)), ((), ())), preferred_element_type=F32
        )
    gram = gram.astype(BF)
    out[CROSS : CROSS + 256, :] = gram[:, :128]
    out[CROSS + 256 :, :] = gram[:, 128:]


def head_kernel(first, gathered, mat, z, fac_in, *refs):
    refs = list(refs)
    rest = refs.pop(0) if first else None
    out, fac, sems = refs
    fetch = pltpu.make_async_copy(fac_in, fac, sems.at[0])
    fetch.start()
    residual = jnp.concatenate(
        [gathered[src, side * T : (side + 1) * T, :] for src in range(N_Z) for side in range(2)],
        axis=1,
    )
    for src in range(N_Y):
        out[src * T : (src + 1) * T, :] = dot_t(residual, mat[src, :ROWS, :]).astype(BF)
    wide = residual.astype(F32)
    out[SCAL : SCAL + 32, :] = as_tile(total_of(wide * wide), 32)
    if first:
        out[HEAD:, :] = rest[...]
    fetch.wait()
    seen = jnp.zeros((T, RANK), F32)
    for index in range(N_Z):
        src = lax.rem(z[0] - index + N_Z, N_Z)
        block = jnp.concatenate([gathered[src, :T, :], gathered[src, T:, :]], axis=1)
        seen = seen + dot(block, fac[index])
    seen = seen.astype(BF)
    out[SEEN : SEEN + T, :] = seen[:, :128]
    out[SEEN + T : SEEN + 2 * T, :] = seen[:, 128:]


def head(gathered, mat, z, fac, rest=None):
    first = rest is not None
    extra = (rest,) if first else ()
    return pl.pallas_call(
        lambda *refs: head_kernel(first, *refs),
        out_shape=shape(HEAD + (REST if first else 0), 128, dtype=BF),
        in_specs=[IN_VMEM, IN_VMEM, IN_SMEM, IN_HBM] + [IN_VMEM] * len(extra),
        out_specs=IN_VMEM,
        scratch_shapes=[pltpu.VMEM((N_Z, OWN, RANK), BF), pltpu.SemaphoreType.DMA((1,))],
        compiler_params=PARAMS,
    )(gathered, mat, z, fac, *extra)


def middle_kernel(pieces, me, out):
    count = pieces.shape[1]
    total = jnp.zeros((count, 128), F32)
    for source in range(N_MANY):
        total = total + pieces[source].astype(F32)
    tile = total[:8]
    high, low = split16(tile[0:1] + tile[1:2])
    line = lax.broadcasted_iota(jnp.int32, (8, 128), 0)
    again = jnp.where(line == 0, high, jnp.where(line == 1, low, tile))
    tile = jnp.where(me[0] == SCAL // count, again, tile)
    if count > 8:
        tile = jnp.concatenate([tile, total[8:]], axis=0)
    total = tile.astype(BF)
    for target in range(N_MANY):
        out[target] = total


def middle(pieces, me):
    return pl.pallas_call(
        middle_kernel,
        out_shape=shape(*pieces.shape, dtype=BF),
        in_specs=[IN_VMEM, IN_SMEM],
        out_specs=IN_VMEM,
        compiler_params=PARAMS,
    )(pieces, me)


def search_kernel(first, back, mat, factor, weights, own_in, *refs):
    refs = list(refs)
    full, direction_in, row_in, seen_in, scal_in = (back, *[None] * 4) if first else refs[:5]
    out, direction_out, row_out, seen_out, scal_out = refs if first else refs[5:]
    projected = jnp.concatenate(
        [back[SEEN : SEEN + T, :], back[SEEN + T : SEEN + 2 * T, :]], axis=1
    ).astype(F32)
    rr = from_tile(back[SCAL : SCAL + 16, :].astype(F32)[:8])
    scaled = weights[0:1, :] * projected
    cross_inner = total_of(scaled * projected)
    inner = rr + cross_inner
    low = scaled.astype(BF)
    gram = HEAD + CROSS
    through = jnp.concatenate(
        [dot(low, full[gram : gram + 256, :]), dot(low, full[gram + 256 : gram + 512, :])], axis=1
    )
    dd = rr + 2.0 * cross_inner + total_of(scaled * through)
    seen = projected + through
    direction = own_in[...] + dot_t(low, factor[...])
    if not first:
        before, dd_before = scal_in[:, :1], scal_in[:, 1:2]
        beta = inner / before
        dd = dd + 2.0 * beta * total_of(scaled * seen_in[...]) + beta * beta * dd_before
        seen = seen + beta * seen_in[...]
        direction = direction + beta * direction_in[...]
    direction_out[...] = direction
    seen_out[...] = seen
    scal_out[...] = columns([inner, dd])
    part = jnp.zeros((T, WIDTH), F32)
    square = jnp.zeros((T, 1), F32)
    for src in range(N_Y):
        at = HEAD + src * 256
        row = back[src * T : (src + 1) * T, :].astype(F32)
        row = row + dot_t(low[:, :128], full[at : at + 128, :])
        row = row + dot_t(low[:, 128:], full[at + 128 : at + 256, :])
        if not first:
            row = row + beta * row_in[:, src * 128 : (src + 1) * 128]
        row_out[:, src * 128 : (src + 1) * 128] = row
        row_low = row.astype(BF)
        square = square + total_of(row * row_low.astype(F32))
        part = part + dot(row_low, mat[src, :ROWS, :])
    part = part.astype(BF)
    tile = as_tile(square, 8)
    for to in range(N_Z):
        for side in range(2):
            at = to * OWN + side * 128
            out[to, side * T : (side + 1) * T, :] = part[:, at : at + 128]
        out[to, 2 * T :, :] = tile


def search(first, *args):
    return pl.pallas_call(
        lambda *refs: search_kernel(first, *refs),
        out_shape=(
            shape(N_Z, 2 * T + 8, 128, dtype=BF),
            shape(T, OWN),
            shape(T, N_Y * 128),
            shape(T, RANK),
            shape(T, 128),
        ),
        compiler_params=PARAMS,
    )(*args)


def stepped(arrived, direction_in, own_in, scal, penalty):
    total = jnp.zeros((2 * T + 8, 128), F32)
    for source in range(N_Z):
        total = total + arrived[source].astype(F32)
    hess = jnp.concatenate([total[:T], total[T : 2 * T]], axis=1)
    square = from_tile(total[2 * T :])
    ridge = penalty[:, :1]
    direction = direction_in[...]
    step = scal[:, :1] / (square + ridge * scal[:, 1:2])
    return own_in[...] - step * (hess + ridge * direction), step * direction


def next_kernel(arrived, direction, own, scal, penalty, *refs):
    refs = list(refs)
    answer = refs.pop(0) if len(refs) == 4 else None
    own_out, answer_out, out = refs
    left, moved = stepped(arrived, direction, own, scal, penalty)
    own_out[...] = left
    answer_out[...] = moved if answer is None else answer[...] + moved
    send_own(left, out)


def final_kernel(arrived, direction, own, scal, penalty, answer, answer_out, own_out):
    left, moved = stepped(arrived, direction, own, scal, penalty)
    own_out[...] = left
    answer_out[...] = answer[...] + moved


def shards(design, targets, factor, weights, penalty):
    z = lax.axis_index("zh").reshape(1)
    me = lax.axis_index(MANY).reshape(1)
    low_factor = factor.astype(BF)
    blocks = [low_factor]
    for shift in range(1, N_Z):
        pairs = [(i, (i + shift) % N_Z) for i in range(N_Z)]
        blocks.append(lax.ppermute(low_factor, "zh", pairs))
    fac = jnp.stack(blocks)

    mat = exchange(pack(design, targets.T), OWNERS)
    arrived = exchange(call(start_kernel, shape(N_Z, 4 * T, 128, dtype=BF))(mat), "zh")
    own, send = call(begin_kernel, (shape(T, OWN), shape(N_Z, 2 * T, 128, dtype=BF)))(arrived)
    gathered = exchange(send, "zh")
    rest = pl.pallas_call(
        cross_kernel,
        out_shape=shape(REST, 128, dtype=BF),
        in_specs=[IN_VMEM, IN_VMEM, IN_SMEM],
        out_specs=IN_VMEM,
        compiler_params=PARAMS,
    )(mat, fac, z)

    w = jnp.broadcast_to(weights[None, :], (8, RANK))
    ridge = jnp.broadcast_to(penalty[:, None], (T, 128))
    answer = full = None
    state = ()
    for step_index in range(ITERS):
        first = step_index == 0
        packed = head(gathered, mat, z, fac, rest if first else None)
        pieces = packed.reshape(N_MANY, -1, 128)
        back = exchange(middle(exchange(pieces, MANY), me), MANY).reshape(packed.shape)
        if not first:
            state = (full, direction, row_values, seen, scal)
        else:
            full = back
        send, direction, row_values, seen, scal = search(
            first, back, mat, low_factor, w, own, *state
        )
        arrived = exchange(send, "zh")
        args = (arrived, direction, own, scal, ridge) + (() if first else (answer,))
        if step_index + 1 < ITERS:
            own, answer, send = call(
                next_kernel,
                (shape(T, OWN), shape(T, OWN), shape(N_Z, 2 * T, 128, dtype=BF)),
            )(*args)
            gathered = exchange(send, "zh")
    answer, own = call(final_kernel, (shape(T, OWN), shape(T, OWN)))(*args)
    return answer.T, own.T


def solution(mesh):
    finer = Mesh(mesh.devices.reshape(4, 2, 4, 4, 2), ("zh", "zl", "y", "x", "c"))
    spec = P((*FEAT, *ROW), None)
    in_specs = (P(ROW, FEAT), P(ROW, None), spec, P(), P())
    return jax.shard_map(
        shards, mesh=finer, in_specs=in_specs, out_specs=(spec, spec), check_vma=False
    )
```

```python
import jax
import jax.numpy as jnp
from jax import lax
from jax.experimental import pallas as pl
from jax.experimental.pallas import tpu as pltpu
from jax.sharding import Mesh
from jax.sharding import PartitionSpec as P

ITERS = 3
ROW = ("zh", "zl", "y")
FEAT = ("x", "c")
OWN = ("zl", "y")
MANY = ("zl", "y", "x", "c")
N_OWN, N_MANY, N_ZH = 8, 64, 4
T, RANK, BLOCK = 48, 256, 1024
SCAL = 480
HEAD = 512
BF = jnp.bfloat16
F32 = jnp.float32


def exchange(pieces, axes):
    return lax.all_to_all(pieces, axes, 0, 0, tiled=True)


def dot(a, b):
    return jnp.dot(a, b, preferred_element_type=F32)


def dot_t(a, b):
    return lax.dot_general(a, b, (((1,), (1,)), ((), ())), preferred_element_type=F32)


PARAMS = pltpu.CompilerParams(vmem_limit_bytes=20 * 1024 * 1024)


IN_HBM = pl.BlockSpec(memory_space=pltpu.HBM)
IN_VMEM = pl.BlockSpec(memory_space=pltpu.VMEM)
IN_SMEM = pl.BlockSpec(memory_space=pltpu.SMEM)


def call(body, out):
    return pl.pallas_call(body, out_shape=out, compiler_params=PARAMS)


def fetch(pairs, sems):
    copies = [pltpu.make_async_copy(a, b, sems.at[i]) for i, (a, b) in enumerate(pairs)]
    for copy in copies:
        copy.start()
    return copies


def shape(*dims, dtype=F32):
    return jax.ShapeDtypeStruct(dims, dtype)


def columns(parts):
    lane = lax.broadcasted_iota(jnp.int32, (T, 128), 1)
    block = jnp.zeros((T, 128), F32)
    for index, part in enumerate(parts):
        block = jnp.where(lane == index, part, block)
    return block


def split16(value):
    high = value.astype(BF).astype(F32)
    return high, value - high


def total_of(array):
    return jnp.sum(array, axis=1, keepdims=True)


CHUNKS, DEEP = 4, 32


def pack_kernel(design, goal, out, rows, packed, goals, sems):
    def inward(index):
        at = pl.ds(index * DEEP, DEEP)
        return pltpu.make_async_copy(design.at[at, :], rows.at[at, :], sems.at[index])

    def outward(index):
        at = pl.ds(index * DEEP, DEEP)
        return pltpu.make_async_copy(
            packed.at[:, at, :], out.at[:, at, :], sems.at[CHUNKS + index]
        )

    for index in range(CHUNKS):
        inward(index).start()
    for to in range(8):
        for index in range(6):
            goals[to, :, index * 128 : (index + 1) * 128] = goal[index * 8 : index * 8 + 8, :]
        goals[to, :, 768:] = jnp.zeros((8, 256), BF)
    last = pltpu.make_async_copy(goals, out.at[:, 128:136, :], sems.at[2 * CHUNKS])
    last.start()
    for index in range(CHUNKS):
        inward(index).wait()
        low, high = index * DEEP, (index + 1) * DEEP
        for to in range(8):
            for part in range(4):
                at = (part * 8 + to) * 256
                packed[to, low:high, part * 256 : (part + 1) * 256] = rows[low:high, at : at + 256]
        outward(index).start()
    for index in range(CHUNKS):
        outward(index).wait()
    last.wait()


def pack(design, goal):
    return pl.pallas_call(
        pack_kernel,
        out_shape=shape(8, 136, BLOCK, dtype=BF),
        in_specs=[IN_HBM, IN_VMEM],
        out_specs=IN_HBM,
        scratch_shapes=[
            pltpu.VMEM((128, 8192), BF),
            pltpu.VMEM((8, 128, BLOCK), BF),
            pltpu.VMEM((8, 8, BLOCK), BF),
            pltpu.SemaphoreType.DMA((2 * CHUNKS + 1,)),
        ],
    )(design, goal)


def start_kernel(mat, zh, *outs):
    part = jnp.zeros((T, BLOCK), F32)
    for src in range(8):
        goal = jnp.concatenate(
            [mat[src, 128:136, t * 128 : (t + 1) * 128].astype(F32) for t in range(6)], axis=0
        ).astype(BF)
        part = part + dot(goal, mat[src, :128, :])
    high, low = split16(part)
    for shift, out in enumerate(outs):
        out[:, :BLOCK] = high.astype(BF)
        out[:, BLOCK:] = own_part(low, lax.rem(zh[0] + shift, N_ZH)).astype(BF)


def start(mat, zh):
    return pl.pallas_call(
        start_kernel,
        out_shape=(shape(T, BLOCK + 256, dtype=BF),) * N_ZH,
        in_specs=[IN_VMEM, IN_SMEM],
        compiler_params=PARAMS,
    )(mat, zh)


def cross_kernel(mat, fac, gram, out):
    factor = fac[...]
    both = gram[...].astype(BF)
    for src in range(8):
        block = dot(mat[src, :128, :], factor).astype(BF)
        for half in range(2):
            for part in range(4):
                rows = block[part * 32 : (part + 1) * 32, half * 128 : (half + 1) * 128]
                out[src * 8 + half * 4 + part, :32, :] = rows
    for half in range(2):
        for part in range(32):
            rows = both[part * 8 : (part + 1) * 8, half * 128 : (half + 1) * 128]
            out[half * 32 + part, 32:40, :] = rows


def write_head(residual, direction, mat, fac, out):
    low = residual.astype(BF)
    for src in range(8):
        out[src * T : (src + 1) * T, :] = dot_t(low, mat[src, :128, :]).astype(BF)
    seen = dot(low, fac[...]).astype(BF)
    out[384:432, :] = seen[:, :128]
    out[432:480, :] = seen[:, 128:]
    rr = split16(total_of(residual * residual))
    rd = split16(total_of(residual * direction))
    block = jnp.concatenate([columns([*rr, *rd]), jnp.zeros((80, 128), F32)], axis=0)
    tile = block.T[:32, :]
    out[SCAL:HEAD, :] = tile.astype(BF)


def first_kernel(a0, a1, a2, a3, mat, fac, out, start_out, held, sem):
    total = a0[...].astype(F32)
    for other in (a1, a2, a3):
        total = total + other[...].astype(F32)
    held[...] = total
    store = pltpu.make_async_copy(held, start_out, sem.at[0])
    store.start()
    residual = total[:, :BLOCK]
    write_head(residual, residual, mat, fac, out)
    store.wait()


def first_call(arrived, mat, fac):
    return pl.pallas_call(
        first_kernel,
        out_shape=(shape(HEAD, 128, dtype=BF), shape(T, BLOCK + 256)),
        in_specs=[IN_VMEM] * 6,
        out_specs=(IN_VMEM, IN_HBM),
        scratch_shapes=[pltpu.VMEM((T, BLOCK + 256), F32), pltpu.SemaphoreType.DMA((1,))],
        compiler_params=PARAMS,
    )(*arrived, mat, fac)


def own_part(array, zh):
    mine = array[:, :256]
    for index in range(1, N_ZH):
        mine = jnp.where(zh == index, array[:, index * 256 : (index + 1) * 256], mine)
    return mine


D_AT, R_AT, S_AT, C_AT, WIDE = 0, BLOCK, 2 * BLOCK, 2 * BLOCK + RANK, 2 * BLOCK + RANK + 128


def next_kernel(more, arrived, zh, penalty, mat, state, residual_in, fac_in, *refs):
    refs = list(refs)
    answer_in = refs.pop(0) if more else None
    out, residual_out, answer_out, direction_v, scal_v, residual_v, fac_v, answer_v, sems = refs
    copies = fetch(
        [
            (state.at[:, D_AT:R_AT], direction_v),
            (state.at[:, C_AT:WIDE], scal_v),
            (residual_in.at[:, :BLOCK], residual_v),
            (fac_in, fac_v),
        ]
        + ([(answer_in, answer_v)] if more else []),
        sems,
    )
    hess = jnp.zeros((T, BLOCK + 128), F32)
    for source in range(N_ZH):
        hess = hess + arrived[source].astype(F32)
    square = hess[:, BLOCK : BLOCK + 1] + hess[:, BLOCK + 1 : BLOCK + 2]
    hess = hess[:, :BLOCK]
    ridge = penalty[:, :1]
    for copy in copies[:3]:
        copy.wait()
    inner, dd = scal_v[:, :1], scal_v[:, 1:2]
    direction = direction_v[...]
    step = inner / (square + ridge * dd)
    residual = residual_v[...] - step * (hess + ridge * direction)
    residual_v[...] = residual
    answer = step * own_part(direction, zh[0])
    if more:
        copies[4].wait()
        answer = answer_v[...] + answer
    answer_v[...] = answer
    stores = [
        pltpu.make_async_copy(residual_v, residual_out, sems.at[5]),
        pltpu.make_async_copy(answer_v, answer_out, sems.at[6]),
    ]
    for copy in stores:
        copy.start()
    copies[3].wait()
    write_head(residual, direction, mat, fac_v, out)
    for copy in stores:
        copy.wait()


def next_call(arrived, zh, ridge, mat, state, residual, fac, answer):
    more = answer is not None
    extra = (answer,) if more else ()
    return pl.pallas_call(
        lambda *refs: next_kernel(more, *refs),
        out_shape=(shape(HEAD, 128, dtype=BF), shape(T, BLOCK), shape(T, 256)),
        in_specs=[IN_VMEM, IN_SMEM, IN_VMEM, IN_VMEM] + [IN_HBM] * (3 + len(extra)),
        out_specs=(IN_VMEM, IN_HBM, IN_HBM),
        scratch_shapes=[
            pltpu.VMEM((T, BLOCK), F32),
            pltpu.VMEM((T, 128), F32),
            pltpu.VMEM((T, BLOCK), F32),
            pltpu.VMEM((BLOCK, RANK), BF),
            pltpu.VMEM((T, 256), F32),
            pltpu.SemaphoreType.DMA((7,)),
        ],
        compiler_params=PARAMS,
    )(arrived, zh, ridge, mat, state, residual, fac, *extra)


def search_kernel(first, last, back, zh, weights, mat, residual_in, fac_in, *refs):
    refs = list(refs)
    state_in = None if first else refs.pop(0)
    full = back if first else refs.pop(0)
    answer_in, fix_in = (refs.pop(0), refs.pop(0)) if last else (None, None)
    out, state_out, residual_v, fac_v, sems, state_v = refs[:6]
    refs = refs[6:]

    def lanes(array, low, high):
        return array.at[:, low:high]

    pairs = [(residual_in.at[:, :BLOCK], residual_v), (fac_in, fac_v)]
    if not first:
        full_v = refs.pop(0)
        pairs = [
            (full, full_v),
            (lanes(state_in, S_AT, WIDE), lanes(state_v, S_AT, WIDE)),
            (lanes(state_in, R_AT, S_AT), lanes(state_v, R_AT, S_AT)),
            (lanes(state_in, D_AT, R_AT), lanes(state_v, D_AT, R_AT)),
        ] + pairs
        full = full_v
    late = 0 if first else 3
    if last:
        answer_v, fix_v, tail_v = refs
        pairs += [(answer_in, answer_v), (fix_in.at[:, BLOCK:], fix_v)]
    copies = fetch(pairs, sems)

    def head(tile, count):
        if first:
            return jnp.concatenate(
                [back[t, 40:48, :].astype(F32) for t in range(tile, tile + count)], axis=0
            )
        return back[tile * 8 : (tile + count) * 8, :].astype(F32)

    def crossed(src, half):
        at = src * 8 + half * 4
        return full[at : at + 4, :32, :].reshape(128, 128)

    def grammed(half):
        return full[half * 32 : half * 32 + 32, 32:40, :].astype(F32).reshape(256, 128).astype(BF)

    projected = jnp.concatenate([head(48, 6), head(54, 6)], axis=1)
    tile = jnp.concatenate([head(60, 1), jnp.zeros((120, 128), F32)], axis=0).T
    rr = tile[:T, 0:1] + tile[:T, 1:2]
    rd = tile[:T, 2:3] + tile[:T, 3:4]
    scaled = weights[0:1, :] * projected
    cross_inner = total_of(scaled * projected)
    inner = rr + cross_inner
    low = scaled.astype(BF)
    if not first:
        for copy in copies[:late]:
            copy.wait()
        beta = inner / state_v[:, C_AT : C_AT + 1]
    row_lows = []
    square = jnp.zeros((T, 1), F32)
    for src in range(8):
        row = head(src * 6, 6) + dot_t(low[:, :128], crossed(src, 0))
        row = row + dot_t(low[:, 128:], crossed(src, 1))
        at = R_AT + src * 128
        if not first:
            row = row + beta * state_v[:, at : at + 128]
        state_v[:, at : at + 128] = row
        row_low = row.astype(BF)
        square = square + total_of(row * row_low.astype(F32))
        row_lows.append(row_low)
    through = jnp.concatenate([dot(low, grammed(0)), dot(low, grammed(1))], axis=1)
    dd = rr + 2.0 * cross_inner + total_of(scaled * through)
    seen = projected + through
    if not first:
        sd = rd + total_of(scaled * state_v[:, S_AT:C_AT])
        dd = dd + 2.0 * beta * sd + beta * beta * state_v[:, C_AT + 1 : C_AT + 2]
        seen = seen + beta * state_v[:, S_AT:C_AT]
    for copy in copies[late:]:
        copy.wait()
    direction = residual_v[...] + dot_t(low, fac_v[...])
    if not first:
        direction = direction + beta * state_v[:, D_AT:R_AT]
    if last:
        tail_v[:, :256] = own_part(direction, zh[0])
        tail_v[:, 256:512] = answer_v[...]
        tail_v[:, 512:768] = own_part(residual_v[...], zh[0]) + fix_v[...]
        tail_v[:, 768:] = columns([inner, dd])
        store = pltpu.make_async_copy(tail_v, state_out, sems.at[8])
    else:
        state_v[:, D_AT:R_AT] = direction
        state_v[:, S_AT:C_AT] = seen
        state_v[:, C_AT:WIDE] = columns([inner, dd])
        store = pltpu.make_async_copy(state_v, state_out, sems.at[8])
    store.start()
    part = jnp.zeros((T, BLOCK), F32)
    for src in range(8):
        part = part + dot(row_lows[src], mat[src, :128, :])
    extra = columns(split16(square)).astype(BF)
    high, low = split16(part)
    high, low = high.astype(BF), low.astype(BF)
    for to in range(N_ZH):
        if last:
            mine = slice(to * 256, (to + 1) * 256)
            out[to, :, :256] = high[:, mine]
            out[to, :, 256:512] = low[:, mine]
            out[to, :, 512:] = extra
        else:
            out[to, :, :BLOCK] = high
            out[to, :, BLOCK:] = extra
    store.wait()


def search_call(first, last, back, zh, weights, mat, residual, fac, state, full, answer, fix):
    hbm = [residual, fac]
    if not first:
        hbm += [state, full]
    if last:
        hbm += [answer, fix]
    scratch = [
        pltpu.VMEM((T, BLOCK), F32),
        pltpu.VMEM((BLOCK, RANK), BF),
        pltpu.SemaphoreType.DMA((9,)),
        pltpu.VMEM((T, WIDE), F32),
    ]
    if not first:
        scratch.append(pltpu.VMEM((N_MANY, 48, 128), BF))
    if last:
        scratch += [pltpu.VMEM((T, 256), F32), pltpu.VMEM((T, 256), F32), pltpu.VMEM((T, 896), F32)]
    return pl.pallas_call(
        lambda *refs: search_kernel(first, last, *refs),
        out_shape=(
            shape(N_ZH, T, 640 if last else BLOCK + 128, dtype=BF),
            shape(T, 896 if last else WIDE),
        ),
        in_specs=[IN_VMEM, IN_SMEM, IN_VMEM, IN_VMEM] + [IN_HBM] * len(hbm),
        out_specs=(IN_VMEM, IN_HBM),
        scratch_shapes=scratch,
        compiler_params=PARAMS,
    )(back, zh, weights, mat, *hbm)


def middle_kernel(pieces, me, *refs):
    cross, out = refs if len(refs) == 2 else (None, *refs)
    tile = jnp.zeros((8, 128), F32)
    for source in range(N_MANY):
        tile = tile + pieces[source].astype(F32)
    high_a, low_a = split16(tile[0:1] + tile[1:2])
    high_b, low_b = split16(tile[2:3] + tile[3:4])
    line = lax.broadcasted_iota(jnp.int32, (8, 128), 0)
    again = tile
    for index, value in enumerate((high_a, low_a, high_b, low_b)):
        again = jnp.where(line == index, value, again)
    tile = jnp.where(me[0] == SCAL // 8, again, tile)
    if cross is not None:
        total = jnp.zeros((40, 128), F32)
        for source in range(N_MANY):
            total = total + cross[source].astype(F32)
        tile = jnp.concatenate([total, tile], axis=0)
    tile = tile.astype(BF)
    for target in range(N_MANY):
        out[target] = tile


def middle(pieces, me, cross=None):
    extra = () if cross is None else (cross,)
    return pl.pallas_call(
        middle_kernel,
        out_shape=shape(N_MANY, 48 if extra else 8, 128, dtype=BF),
        in_specs=[IN_VMEM, IN_SMEM] + [IN_VMEM] * len(extra),
        out_specs=IN_VMEM,
        compiler_params=PARAMS,
    )(pieces, me, *extra)


def final_kernel(arrived, tail, penalty, answer_out, residual_out):
    total = jnp.zeros((T, 640), F32)
    for source in range(N_ZH):
        total = total + arrived[source].astype(F32)
    square = total[:, 512:513] + total[:, 513:514]
    ridge = penalty[:, :1]
    mine = tail[:, :256]
    step = tail[:, 768:769] / (square + ridge * tail[:, 769:770])
    hess = total[:, :256] + total[:, 256:512] + ridge * mine
    answer_out[...] = tail[:, 256:512] + step * mine
    residual_out[...] = tail[:, 512:768] - step * hess


def shards(design, targets, factor, weights, penalty):
    zh = lax.axis_index("zh")
    me = lax.axis_index(MANY).reshape(1)
    low_factor = factor.astype(BF)
    slots = jnp.zeros((N_ZH, 256, RANK), BF)
    slots = lax.dynamic_update_slice(slots, low_factor[None], (zh, 0, 0))
    for shift in range(1, N_ZH):
        pairs = [(i, (i + shift) % N_ZH) for i in range(N_ZH)]
        other = lax.ppermute(low_factor, "zh", pairs)
        slots = lax.dynamic_update_slice(slots, other[None], ((zh - shift) % N_ZH, 0, 0))
    fac = slots.reshape(BLOCK, RANK)

    spot = zh.reshape(1)
    mat = exchange(pack(design, targets.T), OWN)
    arrived = list(start(mat, spot))
    for shift in range(1, N_ZH):
        pairs = [(i, (i + shift) % N_ZH) for i in range(N_ZH)]
        arrived[shift] = lax.ppermute(arrived[shift], "zh", pairs)
    gram = lax.dot_general(fac, fac, (((0,), (0,)), ((), ())), preferred_element_type=F32)
    cross = call(cross_kernel, shape(N_MANY, 40, 128, dtype=BF))(mat, fac, gram)
    cross = exchange(cross, MANY)

    w = jnp.broadcast_to(weights[None, :], (8, RANK))
    ridge = jnp.broadcast_to(penalty[:, None], (T, 128))

    packed, residual = first_call(arrived, mat, fac)
    packed, cross = lax.optimization_barrier((packed, cross))
    fix = residual
    answer = state = full = None
    for step_index in range(ITERS):
        first, last = step_index == 0, step_index == ITERS - 1
        pieces = exchange(packed.reshape(N_MANY, 8, 128), MANY)
        back = exchange(middle(pieces, me, cross if first else None), MANY)
        if first:
            full = back
        else:
            back = back.reshape(HEAD, 128)
        send, state = search_call(
            first, last, back, spot, w, mat, residual, fac, state, full, answer, fix
        )
        arrived = exchange(send, "zh")
        if not last:
            packed, residual, answer = next_call(
                arrived, spot, ridge, mat, state, residual, fac, answer
            )
    answer, residual = call(final_kernel, (shape(T, 256), shape(T, 256)))(arrived, state, ridge)
    return answer.T, residual.T


def solution(mesh):
    finer = Mesh(mesh.devices.reshape(4, 2, 4, 4, 2), ("zh", "zl", "y", "x", "c"))
    spec = P((*FEAT, *ROW), None)
    in_specs = (P(ROW, FEAT), P(ROW, None), spec, P(), P())
    return jax.shard_map(
        shards, mesh=finer, in_specs=in_specs, out_specs=(spec, spec), check_vma=False
    )
```

```python
import jax
import jax.numpy as jnp
from jax import lax
from jax.experimental import pallas as pl
from jax.experimental.pallas import tpu as pltpu
from jax.sharding import Mesh
from jax.sharding import PartitionSpec as P


ITERS = 3
ROW = ("zh", "zl", "y")
FEAT = ("x", "c")
OWN = ("zl", "y")
MANY = ("zl", "y", "x", "c")
N_MANY, N_ZH = 64, 4
T, RANK, BLOCK = 48, 256, 1024
SCAL = 480
HEAD = 512
BF = jnp.bfloat16
F32 = jnp.float32


def exchange(pieces, axes):
    return lax.all_to_all(pieces, axes, 0, 0, tiled=True)


def dot(a, b):
    return jnp.dot(a, b, preferred_element_type=F32)


def dot_t(a, b):
    return lax.dot_general(a, b, (((1,), (1,)), ((), ())), preferred_element_type=F32)


PARAMS = pltpu.CompilerParams(vmem_limit_bytes=20 * 1024 * 1024)


IN_HBM = pl.BlockSpec(memory_space=pltpu.HBM)
IN_VMEM = pl.BlockSpec(memory_space=pltpu.VMEM)
IN_SMEM = pl.BlockSpec(memory_space=pltpu.SMEM)


def call(body, out):
    return pl.pallas_call(body, out_shape=out, compiler_params=PARAMS)


def fetch(pairs, sems):
    copies = [pltpu.make_async_copy(a, b, sems.at[i]) for i, (a, b) in enumerate(pairs)]
    for copy in copies:
        copy.start()
    return copies


def shape(*dims, dtype=F32):
    return jax.ShapeDtypeStruct(dims, dtype)


def columns(parts):
    lane = lax.broadcasted_iota(jnp.int32, (T, 128), 1)
    block = jnp.zeros((T, 128), F32)
    for index, part in enumerate(parts):
        block = jnp.where(lane == index, part, block)
    return block


def split16(value):
    high = value.astype(BF).astype(F32)
    return high, value - high


def total_of(array):
    return jnp.sum(array, axis=1, keepdims=True)


CHUNKS, DEEP = 4, 32


def pack_kernel(design, goal, out, rows, packed, goals, sems):
    def inward(index):
        at = pl.ds(index * DEEP, DEEP)
        return pltpu.make_async_copy(design.at[at, :], rows.at[at, :], sems.at[index])

    def outward(index):
        at = pl.ds(index * DEEP, DEEP)
        return pltpu.make_async_copy(
            packed.at[:, at, :], out.at[:, at, :], sems.at[CHUNKS + index]
        )

    for index in range(CHUNKS):
        inward(index).start()
    for to in range(8):
        for index in range(6):
            goals[to, :, index * 128 : (index + 1) * 128] = goal[index * 8 : index * 8 + 8, :]
        goals[to, :, 768:] = jnp.zeros((8, 256), BF)
    last = pltpu.make_async_copy(goals, out.at[:, 128:136, :], sems.at[2 * CHUNKS])
    last.start()
    for index in range(CHUNKS):
        inward(index).wait()
        low, high = index * DEEP, (index + 1) * DEEP
        for to in range(8):
            for part in range(4):
                at = (part * 8 + to) * 256
                packed[to, low:high, part * 256 : (part + 1) * 256] = rows[low:high, at : at + 256]
        outward(index).start()
    for index in range(CHUNKS):
        outward(index).wait()
    last.wait()


def pack(design, goal):
    return pl.pallas_call(
        pack_kernel,
        out_shape=shape(8, 136, BLOCK, dtype=BF),
        in_specs=[IN_HBM, IN_VMEM],
        out_specs=IN_HBM,
        scratch_shapes=[
            pltpu.VMEM((128, 8192), BF),
            pltpu.VMEM((8, 128, BLOCK), BF),
            pltpu.VMEM((8, 8, BLOCK), BF),
            pltpu.SemaphoreType.DMA((2 * CHUNKS + 1,)),
        ],
    )(design, goal)


def start_kernel(mat, zh, *outs):
    part = jnp.zeros((T, BLOCK), F32)
    for src in range(8):
        goal = jnp.concatenate(
            [mat[src, 128:136, t * 128 : (t + 1) * 128].astype(F32) for t in range(6)], axis=0
        ).astype(BF)
        part = part + dot(goal, mat[src, :128, :])
    high, low = split16(part)
    for shift, out in enumerate(outs):
        out[:, :BLOCK] = high.astype(BF)
        out[:, BLOCK:] = own_part(low, lax.rem(zh[0] + shift, N_ZH)).astype(BF)


def start(mat, zh):
    return pl.pallas_call(
        start_kernel,
        out_shape=(shape(T, BLOCK + 256, dtype=BF),) * N_ZH,
        in_specs=[IN_VMEM, IN_SMEM],
        compiler_params=PARAMS,
    )(mat, zh)


def cross_kernel(mat, fac, out):
    factor = fac[...]
    both = jnp.zeros((RANK, RANK), F32)
    for index in range(4):
        rows = fac[index * 256 : (index + 1) * 256, :]
        both = both + lax.dot_general(
            rows, rows, (((0,), (0,)), ((), ())), preferred_element_type=F32
        )
    both = both.astype(BF)
    for src in range(8):
        block = dot(mat[src, :128, :], factor).astype(BF)
        for half in range(2):
            for part in range(4):
                rows = block[part * 32 : (part + 1) * 32, half * 128 : (half + 1) * 128]
                out[src * 8 + half * 4 + part, :32, :] = rows
    for half in range(2):
        for part in range(32):
            rows = both[part * 8 : (part + 1) * 8, half * 128 : (half + 1) * 128]
            out[half * 32 + part, 32:40, :] = rows


def write_head(residual, direction, mat, fac, out):
    low = residual.astype(BF)
    for src in range(8):
        out[src * T : (src + 1) * T, :] = dot_t(low, mat[src, :128, :]).astype(BF)
    seen = dot(low, fac[...]).astype(BF)
    out[384:432, :] = seen[:, :128]
    out[432:480, :] = seen[:, 128:]
    rr = split16(total_of(residual * residual))
    rd = split16(total_of(residual * direction))
    block = jnp.concatenate([columns([*rr, *rd]), jnp.zeros((80, 128), F32)], axis=0)
    tile = block.T[:32, :]
    out[SCAL:HEAD, :] = tile.astype(BF)


def first_kernel(a0, a1, a2, a3, mat, fac, out, start_out, held, sem):
    total = a0[...].astype(F32)
    for other in (a1, a2, a3):
        total = total + other[...].astype(F32)
    held[...] = total
    store = pltpu.make_async_copy(held, start_out, sem.at[0])
    store.start()
    residual = total[:, :BLOCK]
    write_head(residual, residual, mat, fac, out)
    store.wait()


def first_call(arrived, mat, fac):
    return pl.pallas_call(
        first_kernel,
        out_shape=(shape(HEAD, 128, dtype=BF), shape(T, BLOCK + 256)),
        in_specs=[IN_VMEM] * 6,
        out_specs=(IN_VMEM, IN_HBM),
        scratch_shapes=[pltpu.VMEM((T, BLOCK + 256), F32), pltpu.SemaphoreType.DMA((1,))],
        compiler_params=PARAMS,
    )(*arrived, mat, fac)


def own_part(array, zh):
    mine = array[:, :256]
    for index in range(1, N_ZH):
        mine = jnp.where(zh == index, array[:, index * 256 : (index + 1) * 256], mine)
    return mine


D_AT, R_AT, S_AT, C_AT, WIDE = 0, BLOCK, 2 * BLOCK, 2 * BLOCK + RANK, 2 * BLOCK + RANK + 128


def next_kernel(more, arrived, zh, penalty, mat, state, residual_in, fac_in, *refs):
    refs = list(refs)
    answer_in = refs.pop(0) if more else None
    out, residual_out, answer_out, direction_v, scal_v, residual_v, fac_v, answer_v, sems = refs
    copies = fetch(
        [
            (state.at[:, D_AT:R_AT], direction_v),
            (state.at[:, C_AT:WIDE], scal_v),
            (residual_in.at[:, :BLOCK], residual_v),
            (fac_in, fac_v),
        ]
        + ([(answer_in, answer_v)] if more else []),
        sems,
    )
    hess = jnp.zeros((T, BLOCK + 128), F32)
    for source in range(N_ZH):
        hess = hess + arrived[source].astype(F32)
    square = hess[:, BLOCK : BLOCK + 1] + hess[:, BLOCK + 1 : BLOCK + 2]
    hess = hess[:, :BLOCK]
    ridge = penalty[:, :1]
    for copy in copies[:3]:
        copy.wait()
    inner, dd = scal_v[:, :1], scal_v[:, 1:2]
    direction = direction_v[...]
    step = inner / (square + ridge * dd)
    residual = residual_v[...] - step * (hess + ridge * direction)
    residual_v[...] = residual
    answer = step * own_part(direction, zh[0])
    if more:
        copies[4].wait()
        answer = answer_v[...] + answer
    answer_v[...] = answer
    stores = [
        pltpu.make_async_copy(residual_v, residual_out, sems.at[5]),
        pltpu.make_async_copy(answer_v, answer_out, sems.at[6]),
    ]
    for copy in stores:
        copy.start()
    copies[3].wait()
    write_head(residual, direction, mat, fac_v, out)
    for copy in stores:
        copy.wait()


def next_call(arrived, zh, ridge, mat, state, residual, fac, answer):
    more = answer is not None
    extra = (answer,) if more else ()
    return pl.pallas_call(
        lambda *refs: next_kernel(more, *refs),
        out_shape=(shape(HEAD, 128, dtype=BF), shape(T, BLOCK), shape(T, 256)),
        in_specs=[IN_VMEM, IN_SMEM, IN_VMEM, IN_VMEM] + [IN_HBM] * (3 + len(extra)),
        out_specs=(IN_VMEM, IN_HBM, IN_HBM),
        scratch_shapes=[
            pltpu.VMEM((T, BLOCK), F32),
            pltpu.VMEM((T, 128), F32),
            pltpu.VMEM((T, BLOCK), F32),
            pltpu.VMEM((BLOCK, RANK), BF),
            pltpu.VMEM((T, 256), F32),
            pltpu.SemaphoreType.DMA((7,)),
        ],
        compiler_params=PARAMS,
    )(arrived, zh, ridge, mat, state, residual, fac, *extra)


def search_kernel(first, last, back, zh, weights, mat, residual_in, fac_in, *refs):
    refs = list(refs)
    state_in = None if first else refs.pop(0)
    full = back if first else refs.pop(0)
    answer_in, fix_in = (refs.pop(0), refs.pop(0)) if last else (None, None)
    out, state_out, residual_v, fac_v, sems, state_v = refs[:6]
    refs = refs[6:]

    def lanes(array, low, high):
        return array.at[:, low:high]

    pairs = [(residual_in.at[:, :BLOCK], residual_v), (fac_in, fac_v)]
    if not first:
        full_v = refs.pop(0)
        pairs = [
            (full, full_v),
            (lanes(state_in, S_AT, WIDE), lanes(state_v, S_AT, WIDE)),
            (lanes(state_in, R_AT, S_AT), lanes(state_v, R_AT, S_AT)),
            (lanes(state_in, D_AT, R_AT), lanes(state_v, D_AT, R_AT)),
        ] + pairs
        full = full_v
    late = 0 if first else 3
    if last:
        answer_v, fix_v, tail_v = refs
        pairs += [(answer_in, answer_v), (fix_in.at[:, BLOCK:], fix_v)]
    copies = fetch(pairs, sems)

    def head(tile, count):
        if first:
            return jnp.concatenate(
                [back[t, 40:48, :].astype(F32) for t in range(tile, tile + count)], axis=0
            )
        return back[tile * 8 : (tile + count) * 8, :].astype(F32)

    def crossed(src, half):
        at = src * 8 + half * 4
        return full[at : at + 4, :32, :].reshape(128, 128)

    def grammed(half):
        return full[half * 32 : half * 32 + 32, 32:40, :].astype(F32).reshape(256, 128).astype(BF)

    projected = jnp.concatenate([head(48, 6), head(54, 6)], axis=1)
    tile = jnp.concatenate([head(60, 1), jnp.zeros((120, 128), F32)], axis=0).T
    rr = tile[:T, 0:1] + tile[:T, 1:2]
    rd = tile[:T, 2:3] + tile[:T, 3:4]
    scaled = weights[0:1, :] * projected
    cross_inner = total_of(scaled * projected)
    inner = rr + cross_inner
    low = scaled.astype(BF)
    if not first:
        for copy in copies[:late]:
            copy.wait()
        beta = inner / state_v[:, C_AT : C_AT + 1]
    row_lows = []
    square = jnp.zeros((T, 1), F32)
    for src in range(8):
        row = head(src * 6, 6) + dot_t(low[:, :128], crossed(src, 0))
        row = row + dot_t(low[:, 128:], crossed(src, 1))
        at = R_AT + src * 128
        if not first:
            row = row + beta * state_v[:, at : at + 128]
        state_v[:, at : at + 128] = row
        row_low = row.astype(BF)
        square = square + total_of(row * row_low.astype(F32))
        row_lows.append(row_low)
    through = jnp.concatenate([dot(low, grammed(0)), dot(low, grammed(1))], axis=1)
    dd = rr + 2.0 * cross_inner + total_of(scaled * through)
    seen = projected + through
    if not first:
        sd = rd + total_of(scaled * state_v[:, S_AT:C_AT])
        dd = dd + 2.0 * beta * sd + beta * beta * state_v[:, C_AT + 1 : C_AT + 2]
        seen = seen + beta * state_v[:, S_AT:C_AT]
    for copy in copies[late:]:
        copy.wait()
    direction = residual_v[...] + dot_t(low, fac_v[...])
    if not first:
        direction = direction + beta * state_v[:, D_AT:R_AT]
    if last:
        tail_v[:, :256] = own_part(direction, zh[0])
        tail_v[:, 256:512] = answer_v[...]
        tail_v[:, 512:768] = own_part(residual_v[...], zh[0]) + fix_v[...]
        tail_v[:, 768:] = columns([inner, dd])
        store = pltpu.make_async_copy(tail_v, state_out, sems.at[8])
    else:
        state_v[:, D_AT:R_AT] = direction
        state_v[:, S_AT:C_AT] = seen
        state_v[:, C_AT:WIDE] = columns([inner, dd])
        store = pltpu.make_async_copy(state_v, state_out, sems.at[8])
    store.start()
    part = jnp.zeros((T, BLOCK), F32)
    for src in range(8):
        part = part + dot(row_lows[src], mat[src, :128, :])
    extra = columns(split16(square)).astype(BF)
    high, low = split16(part)
    high, low = high.astype(BF), low.astype(BF)
    for to in range(N_ZH):
        if last:
            mine = slice(to * 256, (to + 1) * 256)
            out[to, :, :256] = high[:, mine]
            out[to, :, 256:512] = low[:, mine]
            out[to, :, 512:] = extra
        else:
            out[to, :, :BLOCK] = high
            out[to, :, BLOCK:] = extra
    store.wait()


def search_call(first, last, back, zh, weights, mat, residual, fac, state, full, answer, fix):
    hbm = [residual, fac]
    if not first:
        hbm += [state, full]
    if last:
        hbm += [answer, fix]
    scratch = [
        pltpu.VMEM((T, BLOCK), F32),
        pltpu.VMEM((BLOCK, RANK), BF),
        pltpu.SemaphoreType.DMA((9,)),
        pltpu.VMEM((T, WIDE), F32),
    ]
    if not first:
        scratch.append(pltpu.VMEM((N_MANY, 48, 128), BF))
    if last:
        scratch += [pltpu.VMEM((T, 256), F32), pltpu.VMEM((T, 256), F32), pltpu.VMEM((T, 896), F32)]
    return pl.pallas_call(
        lambda *refs: search_kernel(first, last, *refs),
        out_shape=(
            shape(N_ZH, T, 640 if last else BLOCK + 128, dtype=BF),
            shape(T, 896 if last else WIDE),
        ),
        in_specs=[IN_VMEM, IN_SMEM, IN_VMEM, IN_VMEM] + [IN_HBM] * len(hbm),
        out_specs=(IN_VMEM, IN_HBM),
        scratch_shapes=scratch,
        compiler_params=PARAMS,
    )(back, zh, weights, mat, *hbm)


def middle_kernel(pieces, me, *refs):
    cross, out = refs if len(refs) == 2 else (None, *refs)
    tile = jnp.zeros((8, 128), F32)
    for source in range(N_MANY):
        tile = tile + pieces[source].astype(F32)
    high_a, low_a = split16(tile[0:1] + tile[1:2])
    high_b, low_b = split16(tile[2:3] + tile[3:4])
    line = lax.broadcasted_iota(jnp.int32, (8, 128), 0)
    again = tile
    for index, value in enumerate((high_a, low_a, high_b, low_b)):
        again = jnp.where(line == index, value, again)
    tile = jnp.where(me[0] == SCAL // 8, again, tile)
    if cross is not None:
        total = jnp.zeros((40, 128), F32)
        for source in range(N_MANY):
            total = total + cross[source].astype(F32)
        tile = jnp.concatenate([total, tile], axis=0)
    tile = tile.astype(BF)
    for target in range(N_MANY):
        out[target] = tile


def middle(pieces, me, cross=None):
    extra = () if cross is None else (cross,)
    return pl.pallas_call(
        middle_kernel,
        out_shape=shape(N_MANY, 48 if extra else 8, 128, dtype=BF),
        in_specs=[IN_VMEM, IN_SMEM] + [IN_VMEM] * len(extra),
        out_specs=IN_VMEM,
        compiler_params=PARAMS,
    )(pieces, me, *extra)


def final_kernel(arrived, tail, penalty, answer_out, residual_out):
    total = jnp.zeros((T, 640), F32)
    for source in range(N_ZH):
        total = total + arrived[source].astype(F32)
    square = total[:, 512:513] + total[:, 513:514]
    ridge = penalty[:, :1]
    mine = tail[:, :256]
    step = tail[:, 768:769] / (square + ridge * tail[:, 769:770])
    hess = total[:, :256] + total[:, 256:512] + ridge * mine
    answer_out[...] = tail[:, 256:512] + step * mine
    residual_out[...] = tail[:, 512:768] - step * hess


def program(design, targets, factor, weights, penalty):
    zh = lax.axis_index("zh")
    me = lax.axis_index(MANY).reshape(1)
    low_factor = factor.astype(BF)
    slots = jnp.zeros((N_ZH, 256, RANK), BF)
    slots = lax.dynamic_update_slice(slots, low_factor[None], (zh, 0, 0))
    for shift in range(1, N_ZH):
        pairs = [(i, (i + shift) % N_ZH) for i in range(N_ZH)]
        other = lax.ppermute(low_factor, "zh", pairs)
        slots = lax.dynamic_update_slice(slots, other[None], ((zh - shift) % N_ZH, 0, 0))
    fac = slots.reshape(BLOCK, RANK)

    spot = zh.reshape(1)
    mat = exchange(pack(design, targets.T), OWN)
    arrived = list(start(mat, spot))
    for shift in range(1, N_ZH):
        pairs = [(i, (i + shift) % N_ZH) for i in range(N_ZH)]
        arrived[shift] = lax.ppermute(arrived[shift], "zh", pairs)
    cross = call(cross_kernel, shape(N_MANY, 40, 128, dtype=BF))(mat, fac)
    cross = exchange(cross, MANY)

    w = jnp.broadcast_to(weights[None, :], (8, RANK))
    ridge = jnp.broadcast_to(penalty[:, None], (T, 128))

    packed, residual = first_call(arrived, mat, fac)
    packed, cross = lax.optimization_barrier((packed, cross))
    fix = residual
    answer = state = full = None
    for step_index in range(ITERS):
        first, last = step_index == 0, step_index == ITERS - 1
        pieces = exchange(packed.reshape(N_MANY, 8, 128), MANY)
        back = exchange(middle(pieces, me, cross if first else None), MANY)
        if first:
            full = back
        else:
            back = back.reshape(HEAD, 128)
        send, state = search_call(
            first, last, back, spot, w, mat, residual, fac, state, full, answer, fix
        )
        arrived = exchange(send, "zh")
        if not last:
            packed, residual, answer = next_call(
                arrived, spot, ridge, mat, state, residual, fac, answer
            )
    answer, residual = call(final_kernel, (shape(T, 256), shape(T, 256)))(arrived, state, ridge)
    return answer.T, residual.T


def solution(mesh):
    finer = Mesh(mesh.devices.reshape(4, 2, 4, 4, 2), ("zh", "zl", "y", "x", "c"))
    spec = P((*FEAT, *ROW), None)
    in_specs = (P(ROW, FEAT), P(ROW, None), spec, P(), P())
    return jax.shard_map(
        program, mesh=finer, in_specs=in_specs, out_specs=(spec, spec), check_vma=False
    )
```

```python
import jax
import jax.numpy as jnp
from jax import lax
from jax.experimental import pallas as pl
from jax.experimental.pallas import tpu as pltpu
from jax.sharding import Mesh
from jax.sharding import PartitionSpec as P


ITERS = 3
ROW = ("zh", "zl", "y")
FEAT = ("x", "c")
OWN = ("zl", "y")
MANY = ("zl", "y", "x", "c")
N_MANY, N_ZH = 64, 4
T, RANK, BLOCK = 48, 256, 1024
SCAL = 480
HEAD = 512
BF = jnp.bfloat16
F32 = jnp.float32


def exchange(pieces, axes):
    return lax.all_to_all(pieces, axes, 0, 0, tiled=True)


def dot(a, b):
    return jnp.dot(a, b, preferred_element_type=F32)


def dot_t(a, b):
    return lax.dot_general(a, b, (((1,), (1,)), ((), ())), preferred_element_type=F32)


PARAMS = pltpu.CompilerParams(vmem_limit_bytes=20 * 1024 * 1024)


IN_HBM = pl.BlockSpec(memory_space=pltpu.HBM)
IN_VMEM = pl.BlockSpec(memory_space=pltpu.VMEM)
IN_SMEM = pl.BlockSpec(memory_space=pltpu.SMEM)


def call(body, out):
    return pl.pallas_call(body, out_shape=out, compiler_params=PARAMS)


def fetch(pairs, sems):
    copies = [pltpu.make_async_copy(a, b, sems.at[i]) for i, (a, b) in enumerate(pairs)]
    for copy in copies:
        copy.start()
    return copies


def shape(*dims, dtype=F32):
    return jax.ShapeDtypeStruct(dims, dtype)


def columns(parts):
    lane = lax.broadcasted_iota(jnp.int32, (T, 128), 1)
    block = jnp.zeros((T, 128), F32)
    for index, part in enumerate(parts):
        block = jnp.where(lane == index, part, block)
    return block


def split16(value):
    high = value.astype(BF).astype(F32)
    return high, value - high


def as_tile(column):
    block = jnp.concatenate([columns(split16(column)), jnp.zeros((80, 128), F32)], axis=0)
    return block.T[:8, :].astype(BF)


def from_tile(tile):
    block = jnp.concatenate([tile, jnp.zeros((120, 128), F32)], axis=0).T
    return block[:T, 0:1] + block[:T, 1:2]


def total_of(array):
    return jnp.sum(array, axis=1, keepdims=True)


CHUNKS, DEEP = 4, 32


def pack_kernel(design, goal, out, rows, packed, goals, sems):
    def inward(index):
        at = pl.ds(index * DEEP, DEEP)
        return pltpu.make_async_copy(design.at[at, :], rows.at[at, :], sems.at[index])

    def outward(index):
        at = pl.ds(index * DEEP, DEEP)
        return pltpu.make_async_copy(
            packed.at[:, at, :], out.at[:, at, :], sems.at[CHUNKS + index]
        )

    for index in range(CHUNKS):
        inward(index).start()
    for to in range(8):
        for index in range(6):
            goals[to, :, index * 128 : (index + 1) * 128] = goal[index * 8 : index * 8 + 8, :]
        goals[to, :, 768:] = jnp.zeros((8, 256), BF)
    last = pltpu.make_async_copy(goals, out.at[:, 128:136, :], sems.at[2 * CHUNKS])
    last.start()
    for index in range(CHUNKS):
        inward(index).wait()
        low, high = index * DEEP, (index + 1) * DEEP
        for to in range(8):
            for part in range(4):
                at = (part * 8 + to) * 256
                packed[to, low:high, part * 256 : (part + 1) * 256] = rows[low:high, at : at + 256]
        outward(index).start()
    for index in range(CHUNKS):
        outward(index).wait()
    last.wait()


def pack(design, goal):
    return pl.pallas_call(
        pack_kernel,
        out_shape=shape(8, 136, BLOCK, dtype=BF),
        in_specs=[IN_HBM, IN_VMEM],
        out_specs=IN_HBM,
        scratch_shapes=[
            pltpu.VMEM((128, 8192), BF),
            pltpu.VMEM((8, 128, BLOCK), BF),
            pltpu.VMEM((8, 8, BLOCK), BF),
            pltpu.SemaphoreType.DMA((2 * CHUNKS + 1,)),
        ],
    )(design, goal)


def start_kernel(mat, out):
    part = jnp.zeros((T, BLOCK), F32)
    for src in range(8):
        goal = jnp.concatenate(
            [mat[src, 128:136, t * 128 : (t + 1) * 128].astype(F32) for t in range(6)], axis=0
        ).astype(BF)
        part = part + dot(goal, mat[src, :128, :])
    high, low = split16(part)
    high, low = high.astype(BF), low.astype(BF)
    for to in range(N_ZH):
        out[to, :, :BLOCK] = high
        out[to, :, BLOCK:] = low[:, to * 256 : (to + 1) * 256]


def cross_kernel(mat, fac, out):
    factor = fac[...]
    both = jnp.zeros((RANK, RANK), F32)
    for index in range(4):
        rows = fac[index * 256 : (index + 1) * 256, :]
        both = both + lax.dot_general(
            rows, rows, (((0,), (0,)), ((), ())), preferred_element_type=F32
        )
    both = both.astype(BF)
    for src in range(8):
        block = dot(mat[src, :128, :], factor).astype(BF)
        for half in range(2):
            for part in range(4):
                rows = block[part * 32 : (part + 1) * 32, half * 128 : (half + 1) * 128]
                out[src * 8 + half * 4 + part, :32, :] = rows
    for half in range(2):
        for part in range(32):
            rows = both[part * 8 : (part + 1) * 8, half * 128 : (half + 1) * 128]
            out[half * 32 + part, 32:40, :] = rows


def write_head(residual, direction, mat, fac, put):
    low = residual.astype(BF)
    for src in range(8):
        put(src * 6, dot_t(low, mat[src, :128, :]))
    seen = dot(low, fac[...])
    put(48, seen[:, :128])
    put(54, seen[:, 128:])
    rr = split16(total_of(residual * residual))
    rd = split16(total_of(residual * direction))
    block = jnp.concatenate([columns([*rr, *rd]), jnp.zeros((80, 128), F32)], axis=0)
    put(60, block.T[:32, :])


def first_kernel(arrived, mat, fac, cross, out, start_out, held, sem):
    total = jnp.zeros((T, BLOCK + 256), F32)
    for source in range(N_ZH):
        total = total + arrived[source].astype(F32)
    held[...] = total
    store = pltpu.make_async_copy(held, start_out, sem.at[0])
    store.start()
    out[:, :40, :] = cross[...]

    def put(tile, rows):
        for index in range(rows.shape[0] // 8):
            out[tile + index, 40:48, :] = rows[index * 8 : index * 8 + 8, :].astype(BF)

    residual = total[:, :BLOCK]
    write_head(residual, residual, mat, fac, put)
    store.wait()


def first_call(arrived, mat, fac, cross):
    return pl.pallas_call(
        first_kernel,
        out_shape=(shape(N_MANY, 48, 128, dtype=BF), shape(T, BLOCK + 256)),
        in_specs=[IN_VMEM] * 4,
        out_specs=(IN_VMEM, IN_HBM),
        scratch_shapes=[pltpu.VMEM((T, BLOCK + 256), F32), pltpu.SemaphoreType.DMA((1,))],
        compiler_params=PARAMS,
    )(arrived, mat, fac, cross)


def own_part(array, zh):
    mine = array[:, :256]
    for index in range(1, N_ZH):
        mine = jnp.where(zh == index, array[:, index * 256 : (index + 1) * 256], mine)
    return mine


D_AT, R_AT, S_AT, C_AT, WIDE = 0, BLOCK, 2 * BLOCK, 2 * BLOCK + RANK, 2 * BLOCK + RANK + 128


def next_kernel(more, arrived, zh, penalty, mat, state, residual_in, fac_in, *refs):
    refs = list(refs)
    answer_in = refs.pop(0) if more else None
    out, residual_out, answer_out, direction_v, scal_v, residual_v, fac_v, answer_v, sems = refs
    copies = fetch(
        [
            (state.at[:, D_AT:R_AT], direction_v),
            (state.at[:, C_AT:WIDE], scal_v),
            (residual_in.at[:, :BLOCK], residual_v),
            (fac_in, fac_v),
        ]
        + ([(answer_in, answer_v)] if more else []),
        sems,
    )
    total = jnp.zeros((8 * T + 8, 128), F32)
    for source in range(N_ZH):
        total = total + arrived[source].astype(F32)
    square = from_tile(total[8 * T :])
    hess = jnp.concatenate([total[at * T : (at + 1) * T] for at in range(8)], axis=1)
    ridge = penalty[:, :1]
    for copy in copies[:3]:
        copy.wait()
    inner, dd = scal_v[:, :1], scal_v[:, 1:2]
    direction = direction_v[...]
    step = inner / (square + ridge * dd)
    residual = residual_v[...] - step * (hess + ridge * direction)
    residual_v[...] = residual
    answer = step * own_part(direction, zh[0])
    if more:
        copies[4].wait()
        answer = answer_v[...] + answer
    answer_v[...] = answer
    stores = [
        pltpu.make_async_copy(residual_v, residual_out, sems.at[5]),
        pltpu.make_async_copy(answer_v, answer_out, sems.at[6]),
    ]
    for copy in stores:
        copy.start()
    copies[3].wait()

    def put(tile, rows):
        out[tile * 8 : tile * 8 + rows.shape[0], :] = rows.astype(BF)

    write_head(residual, direction, mat, fac_v, put)
    for copy in stores:
        copy.wait()


def next_call(arrived, zh, ridge, mat, state, residual, fac, answer):
    more = answer is not None
    extra = (answer,) if more else ()
    return pl.pallas_call(
        lambda *refs: next_kernel(more, *refs),
        out_shape=(shape(HEAD, 128, dtype=BF), shape(T, BLOCK), shape(T, 256)),
        in_specs=[IN_VMEM, IN_SMEM, IN_VMEM, IN_VMEM] + [IN_HBM] * (3 + len(extra)),
        out_specs=(IN_VMEM, IN_HBM, IN_HBM),
        scratch_shapes=[
            pltpu.VMEM((T, BLOCK), F32),
            pltpu.VMEM((T, 128), F32),
            pltpu.VMEM((T, BLOCK), F32),
            pltpu.VMEM((BLOCK, RANK), BF),
            pltpu.VMEM((T, 256), F32),
            pltpu.SemaphoreType.DMA((7,)),
        ],
        compiler_params=PARAMS,
    )(arrived, zh, ridge, mat, state, residual, fac, *extra)


def search_kernel(first, last, back, zh, weights, mat, residual_in, fac_in, *refs):
    refs = list(refs)
    state_in = None if first else refs.pop(0)
    full = back if first else refs.pop(0)
    answer_in, fix_in = (refs.pop(0), refs.pop(0)) if last else (None, None)
    out, state_out, residual_v, fac_v, sems, state_v = refs[:6]
    refs = refs[6:]

    def lanes(array, low, high):
        return array.at[:, low:high]

    pairs = [(residual_in.at[:, :BLOCK], residual_v), (fac_in, fac_v)]
    if not first:
        full_v = refs.pop(0)
        pairs = [
            (full, full_v),
            (lanes(state_in, S_AT, WIDE), lanes(state_v, S_AT, WIDE)),
            (lanes(state_in, R_AT, S_AT), lanes(state_v, R_AT, S_AT)),
            (lanes(state_in, D_AT, R_AT), lanes(state_v, D_AT, R_AT)),
        ] + pairs
        full = full_v
    late = 0 if first else 3
    if last:
        answer_v, fix_v, tail_v = refs
        pairs += [(answer_in, answer_v), (fix_in.at[:, BLOCK:], fix_v)]
    copies = fetch(pairs, sems)

    def head(tile, count):
        if first:
            return jnp.concatenate(
                [back[t, 40:48, :].astype(F32) for t in range(tile, tile + count)], axis=0
            )
        return back[tile * 8 : (tile + count) * 8, :].astype(F32)

    def crossed(src, half):
        at = src * 8 + half * 4
        return full[at : at + 4, :32, :].reshape(128, 128)

    def grammed(half):
        return full[half * 32 : half * 32 + 32, 32:40, :].astype(F32).reshape(256, 128).astype(BF)

    projected = jnp.concatenate([head(48, 6), head(54, 6)], axis=1)
    tile = jnp.concatenate([head(60, 1), jnp.zeros((120, 128), F32)], axis=0).T
    rr = tile[:T, 0:1] + tile[:T, 1:2]
    rd = tile[:T, 2:3] + tile[:T, 3:4]
    scaled = weights[0:1, :] * projected
    cross_inner = total_of(scaled * projected)
    inner = rr + cross_inner
    low = scaled.astype(BF)
    if not first:
        for copy in copies[:late]:
            copy.wait()
        beta = inner / state_v[:, C_AT : C_AT + 1]
    row_lows = []
    square = jnp.zeros((T, 1), F32)
    for src in range(8):
        row = head(src * 6, 6) + dot_t(low[:, :128], crossed(src, 0))
        row = row + dot_t(low[:, 128:], crossed(src, 1))
        at = R_AT + src * 128
        if not first:
            row = row + beta * state_v[:, at : at + 128]
        state_v[:, at : at + 128] = row
        row_low = row.astype(BF)
        square = square + total_of(row * row_low.astype(F32))
        row_lows.append(row_low)
    through = jnp.concatenate([dot(low, grammed(0)), dot(low, grammed(1))], axis=1)
    dd = rr + 2.0 * cross_inner + total_of(scaled * through)
    seen = projected + through
    if not first:
        sd = rd + total_of(scaled * state_v[:, S_AT:C_AT])
        dd = dd + 2.0 * beta * sd + beta * beta * state_v[:, C_AT + 1 : C_AT + 2]
        seen = seen + beta * state_v[:, S_AT:C_AT]
    for copy in copies[late:]:
        copy.wait()
    direction = residual_v[...] + dot_t(low, fac_v[...])
    if not first:
        direction = direction + beta * state_v[:, D_AT:R_AT]
    if last:
        tail_v[:, :256] = own_part(direction, zh[0])
        tail_v[:, 256:512] = answer_v[...]
        tail_v[:, 512:768] = own_part(residual_v[...], zh[0]) + fix_v[...]
        tail_v[:, 768:] = columns([inner, dd])
        store = pltpu.make_async_copy(tail_v, state_out, sems.at[8])
    else:
        state_v[:, D_AT:R_AT] = direction
        state_v[:, S_AT:C_AT] = seen
        state_v[:, C_AT:WIDE] = columns([inner, dd])
        store = pltpu.make_async_copy(state_v, state_out, sems.at[8])
    store.start()
    part = jnp.zeros((T, BLOCK), F32)
    for src in range(8):
        part = part + dot(row_lows[src], mat[src, :128, :])
    part = part.astype(BF)
    tile = as_tile(square)
    for to in range(N_ZH):
        blocks = range(2 * to, 2 * to + 2) if last else range(8)
        for index, at in enumerate(blocks):
            out[to, index * T : (index + 1) * T, :] = part[:, at * 128 : (at + 1) * 128]
        out[to, len(blocks) * T :, :] = tile
    store.wait()


def search_call(first, last, back, zh, weights, mat, residual, fac, state, full, answer, fix):
    hbm = [residual, fac]
    if not first:
        hbm += [state, full]
    if last:
        hbm += [answer, fix]
    scratch = [
        pltpu.VMEM((T, BLOCK), F32),
        pltpu.VMEM((BLOCK, RANK), BF),
        pltpu.SemaphoreType.DMA((9,)),
        pltpu.VMEM((T, WIDE), F32),
    ]
    if not first:
        scratch.append(pltpu.VMEM((N_MANY, 48, 128), BF))
    if last:
        scratch += [pltpu.VMEM((T, 256), F32), pltpu.VMEM((T, 256), F32), pltpu.VMEM((T, 896), F32)]
    return pl.pallas_call(
        lambda *refs: search_kernel(first, last, *refs),
        out_shape=(
            shape(N_ZH, (2 if last else 8) * T + 8, 128, dtype=BF),
            shape(T, 896 if last else WIDE),
        ),
        in_specs=[IN_VMEM, IN_SMEM, IN_VMEM, IN_VMEM] + [IN_HBM] * len(hbm),
        out_specs=(IN_VMEM, IN_HBM),
        scratch_shapes=scratch,
        compiler_params=PARAMS,
    )(back, zh, weights, mat, *hbm)


def middle_kernel(pieces, me, out):
    total = jnp.zeros(pieces.shape[1:], F32)
    for source in range(N_MANY):
        total = total + pieces[source].astype(F32)
    tile = total[-8:]
    high_a, low_a = split16(tile[0:1] + tile[1:2])
    high_b, low_b = split16(tile[2:3] + tile[3:4])
    line = lax.broadcasted_iota(jnp.int32, (8, 128), 0)
    again = tile
    for index, value in enumerate((high_a, low_a, high_b, low_b)):
        again = jnp.where(line == index, value, again)
    tile = jnp.where(me[0] == SCAL // 8, again, tile)
    if total.shape[0] > 8:
        tile = jnp.concatenate([total[:-8], tile], axis=0)
    tile = tile.astype(BF)
    for target in range(N_MANY):
        out[target] = tile


def middle(pieces, me):
    return pl.pallas_call(
        middle_kernel,
        out_shape=shape(*pieces.shape, dtype=BF),
        in_specs=[IN_VMEM, IN_SMEM],
        out_specs=IN_VMEM,
        compiler_params=PARAMS,
    )(pieces, me)


def final_kernel(arrived, tail, penalty, answer_out, residual_out):
    total = jnp.zeros((2 * T + 8, 128), F32)
    for source in range(N_ZH):
        total = total + arrived[source].astype(F32)
    square = from_tile(total[2 * T :])
    ridge = penalty[:, :1]
    mine = tail[:, :256]
    step = tail[:, 768:769] / (square + ridge * tail[:, 769:770])
    hess = jnp.concatenate([total[:T], total[T : 2 * T]], axis=1) + ridge * mine
    answer_out[...] = tail[:, 256:512] + step * mine
    residual_out[...] = tail[:, 512:768] - step * hess


def program(design, targets, factor, weights, penalty):
    zh = lax.axis_index("zh")
    me = lax.axis_index(MANY).reshape(1)
    low_factor = factor.astype(BF)
    slots = jnp.zeros((N_ZH, 256, RANK), BF)
    slots = lax.dynamic_update_slice(slots, low_factor[None], (zh, 0, 0))
    for shift in range(1, N_ZH):
        pairs = [(i, (i + shift) % N_ZH) for i in range(N_ZH)]
        other = lax.ppermute(low_factor, "zh", pairs)
        slots = lax.dynamic_update_slice(slots, other[None], ((zh - shift) % N_ZH, 0, 0))
    fac = slots.reshape(BLOCK, RANK)

    spot = zh.reshape(1)
    spot = zh.reshape(1)
    mat = exchange(pack(design, targets.T), OWN)
    arrived = call(start_kernel, shape(N_ZH, T, BLOCK + 256, dtype=BF))(mat)
    arrived = exchange(arrived, "zh")
    cross = call(cross_kernel, shape(N_MANY, 40, 128, dtype=BF))(mat, fac)

    w = jnp.broadcast_to(weights[None, :], (8, RANK))
    ridge = jnp.broadcast_to(penalty[:, None], (T, 128))

    packed, residual = first_call(arrived, mat, fac, cross)
    fix = residual
    answer = state = full = None
    for step_index in range(ITERS):
        first, last = step_index == 0, step_index == ITERS - 1
        pieces = exchange(packed.reshape(N_MANY, -1, 128), MANY)
        back = exchange(middle(pieces, me), MANY)
        if first:
            full = back
        else:
            back = back.reshape(HEAD, 128)
        send, state = search_call(
            first, last, back, spot, w, mat, residual, fac, state, full, answer, fix
        )
        arrived = exchange(send, "zh")
        if not last:
            packed, residual, answer = next_call(
                arrived, spot, ridge, mat, state, residual, fac, answer
            )
    answer, residual = call(final_kernel, (shape(T, 256), shape(T, 256)))(arrived, state, ridge)
    return answer.T, residual.T


def solution(mesh):
    finer = Mesh(mesh.devices.reshape(4, 2, 4, 4, 2), ("zh", "zl", "y", "x", "c"))
    spec = P((*FEAT, *ROW), None)
    in_specs = (P(ROW, FEAT), P(ROW, None), spec, P(), P())
    return jax.shard_map(
        program, mesh=finer, in_specs=in_specs, out_specs=(spec, spec), check_vma=False
    )
```

```python
import jax
import jax.numpy as jnp
from jax import lax
from jax.experimental import pallas as pl
from jax.experimental.pallas import tpu as pltpu
from jax.sharding import Mesh
from jax.sharding import PartitionSpec as P


ITERS = 3
ROW = ("zh", "zl", "y")
FEAT = ("x", "c")
OWN = ("zl", "y")
MANY = ("zl", "y", "x", "c")
N_MANY, N_ZH = 64, 4
T, RANK, BLOCK = 48, 256, 1024
SCAL = 480
HEAD = 512
BF = jnp.bfloat16
F32 = jnp.float32


def exchange(pieces, axes):
    return lax.all_to_all(pieces, axes, 0, 0, tiled=True)


def dot(a, b):
    return jnp.dot(a, b, preferred_element_type=F32)


def dot_t(a, b):
    return lax.dot_general(a, b, (((1,), (1,)), ((), ())), preferred_element_type=F32)


PARAMS = pltpu.CompilerParams(vmem_limit_bytes=20 * 1024 * 1024)


IN_HBM = pl.BlockSpec(memory_space=pltpu.HBM)
IN_VMEM = pl.BlockSpec(memory_space=pltpu.VMEM)
IN_SMEM = pl.BlockSpec(memory_space=pltpu.SMEM)


def call(body, out):
    return pl.pallas_call(body, out_shape=out, compiler_params=PARAMS)


def fetch(pairs, sems):
    copies = [pltpu.make_async_copy(a, b, sems.at[i]) for i, (a, b) in enumerate(pairs)]
    for copy in copies:
        copy.start()
    return copies


def shape(*dims, dtype=F32):
    return jax.ShapeDtypeStruct(dims, dtype)


def columns(parts):
    lane = lax.broadcasted_iota(jnp.int32, (T, 128), 1)
    block = jnp.zeros((T, 128), F32)
    for index, part in enumerate(parts):
        block = jnp.where(lane == index, part, block)
    return block


def split16(value):
    high = value.astype(BF).astype(F32)
    return high, value - high


def as_tile(column):
    block = jnp.concatenate([columns(split16(column)), jnp.zeros((80, 128), F32)], axis=0)
    return block.T[:8, :].astype(BF)


def from_tile(tile):
    block = jnp.concatenate([tile, jnp.zeros((120, 128), F32)], axis=0).T
    return block[:T, 0:1] + block[:T, 1:2]


def total_of(array):
    return jnp.sum(array, axis=1, keepdims=True)


CHUNKS, DEEP = 4, 32


def pack_kernel(design, goal, out, rows, packed, goals, sems):
    def inward(index):
        at = pl.ds(index * DEEP, DEEP)
        return pltpu.make_async_copy(design.at[at, :], rows.at[at, :], sems.at[index])

    def outward(index):
        at = pl.ds(index * DEEP, DEEP)
        return pltpu.make_async_copy(
            packed.at[:, at, :], out.at[:, at, :], sems.at[CHUNKS + index]
        )

    for index in range(CHUNKS):
        inward(index).start()
    for to in range(8):
        for index in range(6):
            goals[to, :, index * 128 : (index + 1) * 128] = goal[index * 8 : index * 8 + 8, :]
        goals[to, :, 768:] = jnp.zeros((8, 256), BF)
    last = pltpu.make_async_copy(goals, out.at[:, 128:136, :], sems.at[2 * CHUNKS])
    last.start()
    for index in range(CHUNKS):
        inward(index).wait()
        low, high = index * DEEP, (index + 1) * DEEP
        for to in range(8):
            for part in range(4):
                at = (part * 8 + to) * 256
                packed[to, low:high, part * 256 : (part + 1) * 256] = rows[low:high, at : at + 256]
        outward(index).start()
    for index in range(CHUNKS):
        outward(index).wait()
    last.wait()


def pack(design, goal):
    return pl.pallas_call(
        pack_kernel,
        out_shape=shape(8, 136, BLOCK, dtype=BF),
        in_specs=[IN_HBM, IN_VMEM],
        out_specs=IN_HBM,
        scratch_shapes=[
            pltpu.VMEM((128, 8192), BF),
            pltpu.VMEM((8, 128, BLOCK), BF),
            pltpu.VMEM((8, 8, BLOCK), BF),
            pltpu.SemaphoreType.DMA((2 * CHUNKS + 1,)),
        ],
    )(design, goal)


def start_kernel(mat, out):
    part = jnp.zeros((T, BLOCK), F32)
    for src in range(8):
        goal = jnp.concatenate(
            [mat[src, 128:136, t * 128 : (t + 1) * 128].astype(F32) for t in range(6)], axis=0
        ).astype(BF)
        part = part + dot(goal, mat[src, :128, :])
    high, low = split16(part)
    high, low = high.astype(BF), low.astype(BF)
    for to in range(N_ZH):
        out[to, :, :BLOCK] = high
        out[to, :, BLOCK:] = low[:, to * 256 : (to + 1) * 256]


def cross_kernel(mat, fac, out):
    factor = fac[...]
    both = jnp.zeros((RANK, RANK), F32)
    for index in range(4):
        rows = fac[index * 256 : (index + 1) * 256, :]
        both = both + lax.dot_general(
            rows, rows, (((0,), (0,)), ((), ())), preferred_element_type=F32
        )
    both = both.astype(BF)
    for src in range(8):
        block = dot(mat[src, :128, :], factor).astype(BF)
        for half in range(2):
            for part in range(4):
                rows = block[part * 32 : (part + 1) * 32, half * 128 : (half + 1) * 128]
                out[src * 8 + half * 4 + part, :32, :] = rows
    for half in range(2):
        for part in range(32):
            rows = both[part * 8 : (part + 1) * 8, half * 128 : (half + 1) * 128]
            out[half * 32 + part, 32:40, :] = rows


def write_head(residual, direction, mat, fac, put):
    low = residual.astype(BF)
    for src in range(8):
        put(src * 6, dot_t(low, mat[src, :128, :]))
    seen = dot(low, fac[...])
    put(48, seen[:, :128])
    put(54, seen[:, 128:])
    rr = split16(total_of(residual * residual))
    rd = split16(total_of(residual * direction))
    block = jnp.concatenate([columns([*rr, *rd]), jnp.zeros((80, 128), F32)], axis=0)
    put(60, block.T[:32, :])


def first_kernel(arrived, mat, fac, cross, out, start_out, held, sem):
    total = jnp.zeros((T, BLOCK + 256), F32)
    for source in range(N_ZH):
        total = total + arrived[source].astype(F32)
    held[...] = total
    store = pltpu.make_async_copy(held, start_out, sem.at[0])
    store.start()
    out[:, :40, :] = cross[...]

    def put(tile, rows):
        for index in range(rows.shape[0] // 8):
            out[tile + index, 40:48, :] = rows[index * 8 : index * 8 + 8, :].astype(BF)

    residual = total[:, :BLOCK]
    write_head(residual, residual, mat, fac, put)
    store.wait()


def first_call(arrived, mat, fac, cross):
    return pl.pallas_call(
        first_kernel,
        out_shape=(shape(N_MANY, 48, 128, dtype=BF), shape(T, BLOCK + 256)),
        in_specs=[IN_VMEM] * 4,
        out_specs=(IN_VMEM, IN_HBM),
        scratch_shapes=[pltpu.VMEM((T, BLOCK + 256), F32), pltpu.SemaphoreType.DMA((1,))],
        compiler_params=PARAMS,
    )(arrived, mat, fac, cross)


def own_part(array, zh):
    mine = array[:, :256]
    for index in range(1, N_ZH):
        mine = jnp.where(zh == index, array[:, index * 256 : (index + 1) * 256], mine)
    return mine


D_AT, R_AT, S_AT, C_AT, WIDE = 0, BLOCK, 2 * BLOCK, 2 * BLOCK + RANK, 2 * BLOCK + RANK + 128


def next_kernel(more, arrived, zh, penalty, mat, state, residual_in, fac_in, *refs):
    refs = list(refs)
    answer_in = refs.pop(0) if more else None
    out, residual_out, answer_out, direction_v, scal_v, residual_v, fac_v, answer_v, sems = refs
    copies = fetch(
        [
            (state.at[:, D_AT:R_AT], direction_v),
            (state.at[:, C_AT:WIDE], scal_v),
            (residual_in.at[:, :BLOCK], residual_v),
            (fac_in, fac_v),
        ]
        + ([(answer_in, answer_v)] if more else []),
        sems,
    )
    total = jnp.zeros((8 * T + 8, 128), F32)
    for source in range(N_ZH):
        total = total + arrived[source].astype(F32)
    square = from_tile(total[8 * T :])
    hess = jnp.concatenate([total[at * T : (at + 1) * T] for at in range(8)], axis=1)
    ridge = penalty[:, :1]
    for copy in copies[:3]:
        copy.wait()
    inner, dd = scal_v[:, :1], scal_v[:, 1:2]
    direction = direction_v[...]
    step = inner / (square + ridge * dd)
    residual = residual_v[...] - step * (hess + ridge * direction)
    residual_v[...] = residual
    answer = step * own_part(direction, zh[0])
    if more:
        copies[4].wait()
        answer = answer_v[...] + answer
    answer_v[...] = answer
    stores = [
        pltpu.make_async_copy(residual_v, residual_out, sems.at[5]),
        pltpu.make_async_copy(answer_v, answer_out, sems.at[6]),
    ]
    for copy in stores:
        copy.start()
    copies[3].wait()

    def put(tile, rows):
        out[tile * 8 : tile * 8 + rows.shape[0], :] = rows.astype(BF)

    write_head(residual, direction, mat, fac_v, put)
    for copy in stores:
        copy.wait()


def next_call(arrived, zh, ridge, mat, state, residual, fac, answer):
    more = answer is not None
    extra = (answer,) if more else ()
    return pl.pallas_call(
        lambda *refs: next_kernel(more, *refs),
        out_shape=(shape(HEAD, 128, dtype=BF), shape(T, BLOCK), shape(T, 256)),
        in_specs=[IN_VMEM, IN_SMEM, IN_VMEM, IN_VMEM] + [IN_HBM] * (3 + len(extra)),
        out_specs=(IN_VMEM, IN_HBM, IN_HBM),
        scratch_shapes=[
            pltpu.VMEM((T, BLOCK), F32),
            pltpu.VMEM((T, 128), F32),
            pltpu.VMEM((T, BLOCK), F32),
            pltpu.VMEM((BLOCK, RANK), BF),
            pltpu.VMEM((T, 256), F32),
            pltpu.SemaphoreType.DMA((7,)),
        ],
        compiler_params=PARAMS,
    )(arrived, zh, ridge, mat, state, residual, fac, *extra)


def search_kernel(first, last, back, zh, weights, mat, residual_in, fac_in, *refs):
    refs = list(refs)
    state_in = None if first else refs.pop(0)
    full = back if first else refs.pop(0)
    answer_in, fix_in = (refs.pop(0), refs.pop(0)) if last else (None, None)
    out, state_out, residual_v, fac_v, sems, state_v = refs[:6]
    refs = refs[6:]

    def lanes(array, low, high):
        return array.at[:, low:high]

    pairs = [(residual_in.at[:, :BLOCK], residual_v), (fac_in, fac_v)]
    if not first:
        full_v = refs.pop(0)
        pairs = [
            (full, full_v),
            (lanes(state_in, S_AT, WIDE), lanes(state_v, S_AT, WIDE)),
            (lanes(state_in, R_AT, S_AT), lanes(state_v, R_AT, S_AT)),
            (lanes(state_in, D_AT, R_AT), lanes(state_v, D_AT, R_AT)),
        ] + pairs
        full = full_v
    late = 0 if first else 3
    if last:
        answer_v, fix_v, tail_v = refs
        pairs += [(answer_in, answer_v), (fix_in.at[:, BLOCK:], fix_v)]
    copies = fetch(pairs, sems)

    def head(tile, count):
        if first:
            return jnp.concatenate(
                [back[t, 40:48, :].astype(F32) for t in range(tile, tile + count)], axis=0
            )
        return back[tile * 8 : (tile + count) * 8, :].astype(F32)

    def crossed(src, half):
        at = src * 8 + half * 4
        return full[at : at + 4, :32, :].reshape(128, 128)

    def grammed(half):
        return full[half * 32 : half * 32 + 32, 32:40, :].astype(F32).reshape(256, 128).astype(BF)

    projected = jnp.concatenate([head(48, 6), head(54, 6)], axis=1)
    tile = jnp.concatenate([head(60, 1), jnp.zeros((120, 128), F32)], axis=0).T
    rr = tile[:T, 0:1] + tile[:T, 1:2]
    rd = tile[:T, 2:3] + tile[:T, 3:4]
    scaled = weights[0:1, :] * projected
    cross_inner = total_of(scaled * projected)
    inner = rr + cross_inner
    low = scaled.astype(BF)
    if not first:
        for copy in copies[:late]:
            copy.wait()
        beta = inner / state_v[:, C_AT : C_AT + 1]
    row_lows = []
    square = jnp.zeros((T, 1), F32)
    for src in range(8):
        row = head(src * 6, 6) + dot_t(low[:, :128], crossed(src, 0))
        row = row + dot_t(low[:, 128:], crossed(src, 1))
        at = R_AT + src * 128
        if not first:
            row = row + beta * state_v[:, at : at + 128]
        state_v[:, at : at + 128] = row
        row_low = row.astype(BF)
        square = square + total_of(row * row_low.astype(F32))
        row_lows.append(row_low)
    through = jnp.concatenate([dot(low, grammed(0)), dot(low, grammed(1))], axis=1)
    dd = rr + 2.0 * cross_inner + total_of(scaled * through)
    seen = projected + through
    if not first:
        sd = rd + total_of(scaled * state_v[:, S_AT:C_AT])
        dd = dd + 2.0 * beta * sd + beta * beta * state_v[:, C_AT + 1 : C_AT + 2]
        seen = seen + beta * state_v[:, S_AT:C_AT]
    for copy in copies[late:]:
        copy.wait()
    direction = residual_v[...] + dot_t(low, fac_v[...])
    if not first:
        direction = direction + beta * state_v[:, D_AT:R_AT]
    if last:
        tail_v[:, :256] = own_part(direction, zh[0])
        tail_v[:, 256:512] = answer_v[...]
        tail_v[:, 512:768] = own_part(residual_v[...], zh[0]) + fix_v[...]
        tail_v[:, 768:] = columns([inner, dd])
        store = pltpu.make_async_copy(tail_v, state_out, sems.at[8])
    else:
        state_v[:, D_AT:R_AT] = direction
        state_v[:, S_AT:C_AT] = seen
        state_v[:, C_AT:WIDE] = columns([inner, dd])
        store = pltpu.make_async_copy(state_v, state_out, sems.at[8])
    store.start()
    part = jnp.zeros((T, BLOCK), F32)
    for src in range(8):
        part = part + dot(row_lows[src], mat[src, :128, :])
    part = part.astype(BF)
    tile = as_tile(square)
    for to in range(N_ZH):
        blocks = range(2 * to, 2 * to + 2) if last else range(8)
        for index, at in enumerate(blocks):
            out[to, index * T : (index + 1) * T, :] = part[:, at * 128 : (at + 1) * 128]
        out[to, len(blocks) * T :, :] = tile
    store.wait()


def search_call(first, last, back, zh, weights, mat, residual, fac, state, full, answer, fix):
    hbm = [residual, fac]
    if not first:
        hbm += [state, full]
    if last:
        hbm += [answer, fix]
    scratch = [
        pltpu.VMEM((T, BLOCK), F32),
        pltpu.VMEM((BLOCK, RANK), BF),
        pltpu.SemaphoreType.DMA((9,)),
        pltpu.VMEM((T, WIDE), F32),
    ]
    if not first:
        scratch.append(pltpu.VMEM((N_MANY, 48, 128), BF))
    if last:
        scratch += [pltpu.VMEM((T, 256), F32), pltpu.VMEM((T, 256), F32), pltpu.VMEM((T, 896), F32)]
    return pl.pallas_call(
        lambda *refs: search_kernel(first, last, *refs),
        out_shape=(
            shape(N_ZH, (2 if last else 8) * T + 8, 128, dtype=BF),
            shape(T, 896 if last else WIDE),
        ),
        in_specs=[IN_VMEM, IN_SMEM, IN_VMEM, IN_VMEM] + [IN_HBM] * len(hbm),
        out_specs=(IN_VMEM, IN_HBM),
        scratch_shapes=scratch,
        compiler_params=PARAMS,
    )(back, zh, weights, mat, *hbm)


def middle_kernel(pieces, me, out):
    total = jnp.zeros(pieces.shape[1:], F32)
    for source in range(N_MANY):
        total = total + pieces[source].astype(F32)
    tile = total[-8:]
    high_a, low_a = split16(tile[0:1] + tile[1:2])
    high_b, low_b = split16(tile[2:3] + tile[3:4])
    line = lax.broadcasted_iota(jnp.int32, (8, 128), 0)
    again = tile
    for index, value in enumerate((high_a, low_a, high_b, low_b)):
        again = jnp.where(line == index, value, again)
    tile = jnp.where(me[0] == SCAL // 8, again, tile)
    if total.shape[0] > 8:
        tile = jnp.concatenate([total[:-8], tile], axis=0)
    tile = tile.astype(BF)
    for target in range(N_MANY):
        out[target] = tile


def middle(pieces, me):
    return pl.pallas_call(
        middle_kernel,
        out_shape=shape(*pieces.shape, dtype=BF),
        in_specs=[IN_VMEM, IN_SMEM],
        out_specs=IN_VMEM,
        compiler_params=PARAMS,
    )(pieces, me)


def final_kernel(arrived, tail, penalty, answer_out, residual_out):
    total = jnp.zeros((2 * T + 8, 128), F32)
    for source in range(N_ZH):
        total = total + arrived[source].astype(F32)
    square = from_tile(total[2 * T :])
    ridge = penalty[:, :1]
    mine = tail[:, :256]
    step = tail[:, 768:769] / (square + ridge * tail[:, 769:770])
    hess = jnp.concatenate([total[:T], total[T : 2 * T]], axis=1) + ridge * mine
    answer_out[...] = tail[:, 256:512] + step * mine
    residual_out[...] = tail[:, 512:768] - step * hess


def program(design, targets, factor, weights, penalty):
    zh = lax.axis_index("zh")
    me = lax.axis_index(MANY).reshape(1)
    w = jnp.broadcast_to(weights[None, :], (8, RANK))
    ridge = jnp.broadcast_to(penalty[:, None], (T, 128))
    low_factor, spot, me, w, ridge = lax.optimization_barrier(
        (factor.astype(BF), zh.reshape(1), me, w, ridge)
    )
    slots = jnp.zeros((N_ZH, 256, RANK), BF)
    slots = lax.dynamic_update_slice(slots, low_factor[None], (zh, 0, 0))
    for shift in range(1, N_ZH):
        pairs = [(i, (i + shift) % N_ZH) for i in range(N_ZH)]
        other = lax.ppermute(low_factor, "zh", pairs)
        slots = lax.dynamic_update_slice(slots, other[None], ((zh - shift) % N_ZH, 0, 0))
    fac = slots.reshape(BLOCK, RANK)

    spot = zh.reshape(1)
    mat = exchange(pack(design, targets.T), OWN)
    arrived = call(start_kernel, shape(N_ZH, T, BLOCK + 256, dtype=BF))(mat)
    arrived = exchange(arrived, "zh")
    cross = call(cross_kernel, shape(N_MANY, 40, 128, dtype=BF))(mat, fac)

    packed, residual = first_call(arrived, mat, fac, cross)
    fix = residual
    answer = state = full = None
    for step_index in range(ITERS):
        first, last = step_index == 0, step_index == ITERS - 1
        pieces = exchange(packed.reshape(N_MANY, -1, 128), MANY)
        back = exchange(middle(pieces, me), MANY)
        if first:
            full = back
        else:
            back = back.reshape(HEAD, 128)
        send, state = search_call(
            first, last, back, spot, w, mat, residual, fac, state, full, answer, fix
        )
        arrived = exchange(send, "zh")
        if not last:
            packed, residual, answer = next_call(
                arrived, spot, ridge, mat, state, residual, fac, answer
            )
    answer, residual = call(final_kernel, (shape(T, 256), shape(T, 256)))(arrived, state, ridge)
    return answer.T, residual.T


def solution(mesh):
    finer = Mesh(mesh.devices.reshape(4, 2, 4, 4, 2), ("zh", "zl", "y", "x", "c"))
    spec = P((*FEAT, *ROW), None)
    in_specs = (P(ROW, FEAT), P(ROW, None), spec, P(), P())
    return jax.shard_map(
        program, mesh=finer, in_specs=in_specs, out_specs=(spec, spec), check_vma=False
    )
```

```python
import jax
import jax.numpy as jnp
from jax import lax
from jax.experimental import pallas as pl
from jax.experimental.pallas import tpu as pltpu
from jax.sharding import Mesh
from jax.sharding import PartitionSpec as P


ITERS = 3
ROW = ("zh", "zl", "y")
FEAT = ("x", "c")
OWN = ("zl", "y")
MANY = ("zl", "y", "x", "c")
N_OWN, N_MANY, N_ZH = 8, 64, 4
T, RANK, BLOCK = 48, 256, 1024
SCAL = 480
HEAD = 512
BF = jnp.bfloat16
F32 = jnp.float32


def exchange(pieces, axes):
    return lax.all_to_all(pieces, axes, 0, 0, tiled=True)


def dot(a, b):
    return jnp.dot(a, b, preferred_element_type=F32)


def dot_t(a, b):
    return lax.dot_general(a, b, (((1,), (1,)), ((), ())), preferred_element_type=F32)


PARAMS = pltpu.CompilerParams(vmem_limit_bytes=20 * 1024 * 1024)


IN_HBM = pl.BlockSpec(memory_space=pltpu.HBM)
IN_VMEM = pl.BlockSpec(memory_space=pltpu.VMEM)
IN_SMEM = pl.BlockSpec(memory_space=pltpu.SMEM)


def call(body, out):
    return pl.pallas_call(body, out_shape=out, compiler_params=PARAMS)


def fetch(pairs, sems):
    copies = [pltpu.make_async_copy(a, b, sems.at[i]) for i, (a, b) in enumerate(pairs)]
    for copy in copies:
        copy.start()
    return copies


def shape(*dims, dtype=F32):
    return jax.ShapeDtypeStruct(dims, dtype)


def columns(parts):
    lane = lax.broadcasted_iota(jnp.int32, (T, 128), 1)
    block = jnp.zeros((T, 128), F32)
    for index, part in enumerate(parts):
        block = jnp.where(lane == index, part, block)
    return block


def split16(value):
    high = value.astype(BF).astype(F32)
    return high, value - high


def as_tile(column):
    block = jnp.concatenate([columns(split16(column)), jnp.zeros((80, 128), F32)], axis=0)
    return block.T[:8, :].astype(BF)


def from_tile(tile):
    block = jnp.concatenate([tile, jnp.zeros((120, 128), F32)], axis=0).T
    return block[:T, 0:1] + block[:T, 1:2]


def total_of(array):
    return jnp.sum(array, axis=1, keepdims=True)


CHUNKS, DEEP = 4, 32


def pack_kernel(design, out, rows, packed, sems):
    def inward(index):
        at = pl.ds(index * DEEP, DEEP)
        return pltpu.make_async_copy(design.at[at, :], rows.at[at, :], sems.at[index])

    def outward(index):
        at = pl.ds(index * DEEP, DEEP)
        return pltpu.make_async_copy(
            packed.at[:, at, :], out.at[:, at, :], sems.at[CHUNKS + index]
        )

    for index in range(CHUNKS):
        inward(index).start()
    for index in range(CHUNKS):
        inward(index).wait()
        low, high = index * DEEP, (index + 1) * DEEP
        for to in range(8):
            for part in range(4):
                at = (part * 8 + to) * 256
                packed[to, low:high, part * 256 : (part + 1) * 256] = rows[low:high, at : at + 256]
        outward(index).start()
    for index in range(CHUNKS):
        outward(index).wait()


def pack(design):
    return pl.pallas_call(
        pack_kernel,
        out_shape=shape(8, 128, BLOCK, dtype=BF),
        in_specs=[IN_HBM],
        out_specs=IN_HBM,
        scratch_shapes=[
            pltpu.VMEM((128, 8192), BF),
            pltpu.VMEM((8, 128, BLOCK), BF),
            pltpu.SemaphoreType.DMA((2 * CHUNKS,)),
        ],
    )(design)


def start_kernel(mat, owner, *refs):
    goals, out = refs[:-1], refs[-1]
    part = jnp.zeros((T, BLOCK), F32)
    for shift, goal in enumerate(goals):
        part = part + dot(goal[...], mat[lax.rem(owner[0] - shift + N_OWN, N_OWN)])
    high, low = split16(part)
    high, low = high.astype(BF), low.astype(BF)
    for to in range(N_ZH):
        out[to, :, :BLOCK] = high
        out[to, :, BLOCK:] = low[:, to * 256 : (to + 1) * 256]


def start(mat, owner, goals):
    return pl.pallas_call(
        start_kernel,
        out_shape=shape(N_ZH, T, BLOCK + 256, dtype=BF),
        in_specs=[IN_VMEM, IN_SMEM] + [IN_VMEM] * len(goals),
        out_specs=IN_VMEM,
        compiler_params=PARAMS,
    )(mat, owner, *goals)


def cross_kernel(mat, fac, out):
    factor = fac[...]
    both = jnp.zeros((RANK, RANK), F32)
    for index in range(4):
        rows = fac[index * 256 : (index + 1) * 256, :]
        both = both + lax.dot_general(
            rows, rows, (((0,), (0,)), ((), ())), preferred_element_type=F32
        )
    both = both.astype(BF)
    for src in range(8):
        block = dot(mat[src, :128, :], factor).astype(BF)
        for half in range(2):
            for part in range(4):
                rows = block[part * 32 : (part + 1) * 32, half * 128 : (half + 1) * 128]
                out[src * 8 + half * 4 + part, :32, :] = rows
    for half in range(2):
        for part in range(32):
            rows = both[part * 8 : (part + 1) * 8, half * 128 : (half + 1) * 128]
            out[half * 32 + part, 32:40, :] = rows


def write_head(residual, direction, mat, fac, put):
    low = residual.astype(BF)
    for src in range(8):
        put(src * 6, dot_t(low, mat[src, :128, :]))
    seen = dot(low, fac[...])
    put(48, seen[:, :128])
    put(54, seen[:, 128:])
    rr = split16(total_of(residual * residual))
    rd = split16(total_of(residual * direction))
    block = jnp.concatenate([columns([*rr, *rd]), jnp.zeros((80, 128), F32)], axis=0)
    put(60, block.T[:32, :])


def first_kernel(arrived, mat, fac, cross, out, start_out, held, sem):
    total = jnp.zeros((T, BLOCK + 256), F32)
    for source in range(N_ZH):
        total = total + arrived[source].astype(F32)
    held[...] = total
    store = pltpu.make_async_copy(held, start_out, sem.at[0])
    store.start()
    out[:, :40, :] = cross[...]

    def put(tile, rows):
        for index in range(rows.shape[0] // 8):
            out[tile + index, 40:48, :] = rows[index * 8 : index * 8 + 8, :].astype(BF)

    residual = total[:, :BLOCK]
    write_head(residual, residual, mat, fac, put)
    store.wait()


def first_call(arrived, mat, fac, cross):
    return pl.pallas_call(
        first_kernel,
        out_shape=(shape(N_MANY, 48, 128, dtype=BF), shape(T, BLOCK + 256)),
        in_specs=[IN_VMEM] * 4,
        out_specs=(IN_VMEM, IN_HBM),
        scratch_shapes=[pltpu.VMEM((T, BLOCK + 256), F32), pltpu.SemaphoreType.DMA((1,))],
        compiler_params=PARAMS,
    )(arrived, mat, fac, cross)


def own_part(array, zh):
    mine = array[:, :256]
    for index in range(1, N_ZH):
        mine = jnp.where(zh == index, array[:, index * 256 : (index + 1) * 256], mine)
    return mine


D_AT, R_AT, S_AT, C_AT, WIDE = 0, BLOCK, 2 * BLOCK, 2 * BLOCK + RANK, 2 * BLOCK + RANK + 128


def next_kernel(more, arrived, zh, penalty, mat, state, residual_in, fac_in, *refs):
    refs = list(refs)
    answer_in = refs.pop(0) if more else None
    out, residual_out, answer_out, direction_v, scal_v, residual_v, fac_v, answer_v, sems = refs
    copies = fetch(
        [
            (state.at[:, D_AT:R_AT], direction_v),
            (state.at[:, C_AT:WIDE], scal_v),
            (residual_in.at[:, :BLOCK], residual_v),
            (fac_in, fac_v),
        ]
        + ([(answer_in, answer_v)] if more else []),
        sems,
    )
    total = jnp.zeros((8 * T + 8, 128), F32)
    for source in range(N_ZH):
        total = total + arrived[source].astype(F32)
    square = from_tile(total[8 * T :])
    hess = jnp.concatenate([total[at * T : (at + 1) * T] for at in range(8)], axis=1)
    ridge = penalty[:, :1]
    for copy in copies[:3]:
        copy.wait()
    inner, dd = scal_v[:, :1], scal_v[:, 1:2]
    direction = direction_v[...]
    step = inner / (square + ridge * dd)
    residual = residual_v[...] - step * (hess + ridge * direction)
    residual_v[...] = residual
    answer = step * own_part(direction, zh[0])
    if more:
        copies[4].wait()
        answer = answer_v[...] + answer
    answer_v[...] = answer
    stores = [
        pltpu.make_async_copy(residual_v, residual_out, sems.at[5]),
        pltpu.make_async_copy(answer_v, answer_out, sems.at[6]),
    ]
    for copy in stores:
        copy.start()
    copies[3].wait()

    def put(tile, rows):
        out[tile * 8 : tile * 8 + rows.shape[0], :] = rows.astype(BF)

    write_head(residual, direction, mat, fac_v, put)
    for copy in stores:
        copy.wait()


def next_call(arrived, zh, ridge, mat, state, residual, fac, answer):
    more = answer is not None
    extra = (answer,) if more else ()
    return pl.pallas_call(
        lambda *refs: next_kernel(more, *refs),
        out_shape=(shape(HEAD, 128, dtype=BF), shape(T, BLOCK), shape(T, 256)),
        in_specs=[IN_VMEM, IN_SMEM, IN_VMEM, IN_VMEM] + [IN_HBM] * (3 + len(extra)),
        out_specs=(IN_VMEM, IN_HBM, IN_HBM),
        scratch_shapes=[
            pltpu.VMEM((T, BLOCK), F32),
            pltpu.VMEM((T, 128), F32),
            pltpu.VMEM((T, BLOCK), F32),
            pltpu.VMEM((BLOCK, RANK), BF),
            pltpu.VMEM((T, 256), F32),
            pltpu.SemaphoreType.DMA((7,)),
        ],
        compiler_params=PARAMS,
    )(arrived, zh, ridge, mat, state, residual, fac, *extra)


def search_kernel(first, last, back, zh, weights, mat, residual_in, fac_in, *refs):
    refs = list(refs)
    state_in = None if first else refs.pop(0)
    full = back if first else refs.pop(0)
    answer_in, fix_in = (refs.pop(0), refs.pop(0)) if last else (None, None)
    out, state_out, residual_v, fac_v, sems, state_v = refs[:6]
    refs = refs[6:]

    def lanes(array, low, high):
        return array.at[:, low:high]

    pairs = [(residual_in.at[:, :BLOCK], residual_v), (fac_in, fac_v)]
    if not first:
        full_v = refs.pop(0)
        pairs = [
            (full, full_v),
            (lanes(state_in, S_AT, WIDE), lanes(state_v, S_AT, WIDE)),
            (lanes(state_in, R_AT, S_AT), lanes(state_v, R_AT, S_AT)),
            (lanes(state_in, D_AT, R_AT), lanes(state_v, D_AT, R_AT)),
        ] + pairs
        full = full_v
    late = 0 if first else 3
    if last:
        answer_v, fix_v, tail_v = refs
        pairs += [(answer_in, answer_v), (fix_in.at[:, BLOCK:], fix_v)]
    copies = fetch(pairs, sems)

    def head(tile, count):
        if first:
            return jnp.concatenate(
                [back[t, 40:48, :].astype(F32) for t in range(tile, tile + count)], axis=0
            )
        return back[tile * 8 : (tile + count) * 8, :].astype(F32)

    def crossed(src, half):
        at = src * 8 + half * 4
        return full[at : at + 4, :32, :].reshape(128, 128)

    def grammed(half):
        return full[half * 32 : half * 32 + 32, 32:40, :].astype(F32).reshape(256, 128).astype(BF)

    projected = jnp.concatenate([head(48, 6), head(54, 6)], axis=1)
    tile = jnp.concatenate([head(60, 1), jnp.zeros((120, 128), F32)], axis=0).T
    rr = tile[:T, 0:1] + tile[:T, 1:2]
    rd = tile[:T, 2:3] + tile[:T, 3:4]
    scaled = weights[0:1, :] * projected
    cross_inner = total_of(scaled * projected)
    inner = rr + cross_inner
    low = scaled.astype(BF)
    if not first:
        for copy in copies[:late]:
            copy.wait()
        beta = inner / state_v[:, C_AT : C_AT + 1]
    row_lows = []
    square = jnp.zeros((T, 1), F32)
    for src in range(8):
        row = head(src * 6, 6) + dot_t(low[:, :128], crossed(src, 0))
        row = row + dot_t(low[:, 128:], crossed(src, 1))
        at = R_AT + src * 128
        if not first:
            row = row + beta * state_v[:, at : at + 128]
        state_v[:, at : at + 128] = row
        row_low = row.astype(BF)
        square = square + total_of(row * row_low.astype(F32))
        row_lows.append(row_low)
    through = jnp.concatenate([dot(low, grammed(0)), dot(low, grammed(1))], axis=1)
    dd = rr + 2.0 * cross_inner + total_of(scaled * through)
    seen = projected + through
    if not first:
        sd = rd + total_of(scaled * state_v[:, S_AT:C_AT])
        dd = dd + 2.0 * beta * sd + beta * beta * state_v[:, C_AT + 1 : C_AT + 2]
        seen = seen + beta * state_v[:, S_AT:C_AT]
    for copy in copies[late:]:
        copy.wait()
    direction = residual_v[...] + dot_t(low, fac_v[...])
    if not first:
        direction = direction + beta * state_v[:, D_AT:R_AT]
    if last:
        tail_v[:, :256] = own_part(direction, zh[0])
        tail_v[:, 256:512] = answer_v[...]
        tail_v[:, 512:768] = own_part(residual_v[...], zh[0]) + fix_v[...]
        tail_v[:, 768:] = columns([inner, dd])
        store = pltpu.make_async_copy(tail_v, state_out, sems.at[8])
    else:
        state_v[:, D_AT:R_AT] = direction
        state_v[:, S_AT:C_AT] = seen
        state_v[:, C_AT:WIDE] = columns([inner, dd])
        store = pltpu.make_async_copy(state_v, state_out, sems.at[8])
    store.start()
    part = jnp.zeros((T, BLOCK), F32)
    for src in range(8):
        part = part + dot(row_lows[src], mat[src, :128, :])
    part = part.astype(BF)
    tile = as_tile(square)
    for to in range(N_ZH):
        blocks = range(2 * to, 2 * to + 2) if last else range(8)
        for index, at in enumerate(blocks):
            out[to, index * T : (index + 1) * T, :] = part[:, at * 128 : (at + 1) * 128]
        out[to, len(blocks) * T :, :] = tile
    store.wait()


def search_call(first, last, back, zh, weights, mat, residual, fac, state, full, answer, fix):
    hbm = [residual, fac]
    if not first:
        hbm += [state, full]
    if last:
        hbm += [answer, fix]
    scratch = [
        pltpu.VMEM((T, BLOCK), F32),
        pltpu.VMEM((BLOCK, RANK), BF),
        pltpu.SemaphoreType.DMA((9,)),
        pltpu.VMEM((T, WIDE), F32),
    ]
    if not first:
        scratch.append(pltpu.VMEM((N_MANY, 48, 128), BF))
    if last:
        scratch += [pltpu.VMEM((T, 256), F32), pltpu.VMEM((T, 256), F32), pltpu.VMEM((T, 896), F32)]
    return pl.pallas_call(
        lambda *refs: search_kernel(first, last, *refs),
        out_shape=(
            shape(N_ZH, (2 if last else 8) * T + 8, 128, dtype=BF),
            shape(T, 896 if last else WIDE),
        ),
        in_specs=[IN_VMEM, IN_SMEM, IN_VMEM, IN_VMEM] + [IN_HBM] * len(hbm),
        out_specs=(IN_VMEM, IN_HBM),
        scratch_shapes=scratch,
        compiler_params=PARAMS,
    )(back, zh, weights, mat, *hbm)


def middle_kernel(pieces, me, out):
    total = jnp.zeros(pieces.shape[1:], F32)
    for source in range(N_MANY):
        total = total + pieces[source].astype(F32)
    tile = total[-8:]
    high_a, low_a = split16(tile[0:1] + tile[1:2])
    high_b, low_b = split16(tile[2:3] + tile[3:4])
    line = lax.broadcasted_iota(jnp.int32, (8, 128), 0)
    again = tile
    for index, value in enumerate((high_a, low_a, high_b, low_b)):
        again = jnp.where(line == index, value, again)
    tile = jnp.where(me[0] == SCAL // 8, again, tile)
    if total.shape[0] > 8:
        tile = jnp.concatenate([total[:-8], tile], axis=0)
    tile = tile.astype(BF)
    for target in range(N_MANY):
        out[target] = tile


def middle(pieces, me):
    return pl.pallas_call(
        middle_kernel,
        out_shape=shape(*pieces.shape, dtype=BF),
        in_specs=[IN_VMEM, IN_SMEM],
        out_specs=IN_VMEM,
        compiler_params=PARAMS,
    )(pieces, me)


def final_kernel(arrived, tail, penalty, answer_out, residual_out):
    total = jnp.zeros((2 * T + 8, 128), F32)
    for source in range(N_ZH):
        total = total + arrived[source].astype(F32)
    square = from_tile(total[2 * T :])
    ridge = penalty[:, :1]
    mine = tail[:, :256]
    step = tail[:, 768:769] / (square + ridge * tail[:, 769:770])
    hess = jnp.concatenate([total[:T], total[T : 2 * T]], axis=1) + ridge * mine
    answer_out[...] = tail[:, 256:512] + step * mine
    residual_out[...] = tail[:, 512:768] - step * hess


def program(design, targets, factor, weights, penalty):
    zh = lax.axis_index("zh")
    me = lax.axis_index(MANY).reshape(1)
    w = jnp.broadcast_to(weights[None, :], (8, RANK))
    ridge = jnp.broadcast_to(penalty[:, None], (T, 128))
    owner = lax.axis_index(OWN).reshape(1)
    low_factor, spot, owner, me, w, ridge = lax.optimization_barrier(
        (factor.astype(BF), zh.reshape(1), owner, me, w, ridge)
    )
    slots = jnp.zeros((N_ZH, 256, RANK), BF)
    slots = lax.dynamic_update_slice(slots, low_factor[None], (zh, 0, 0))
    for shift in range(1, N_ZH):
        pairs = [(i, (i + shift) % N_ZH) for i in range(N_ZH)]
        other = lax.ppermute(low_factor, "zh", pairs)
        slots = lax.dynamic_update_slice(slots, other[None], ((zh - shift) % N_ZH, 0, 0))
    fac = slots.reshape(BLOCK, RANK)

    spot = zh.reshape(1)
    goals = [targets.T]
    for shift in range(1, N_OWN):
        pairs = [(i, (i + shift) % N_OWN) for i in range(N_OWN)]
        goals.append(lax.ppermute(goals[0], OWN, pairs))
    mat = exchange(pack(design), OWN)
    arrived = start(mat, owner, goals)
    arrived = exchange(arrived, "zh")
    cross = call(cross_kernel, shape(N_MANY, 40, 128, dtype=BF))(mat, fac)

    packed, residual = first_call(arrived, mat, fac, cross)
    fix = residual
    answer = state = full = None
    for step_index in range(ITERS):
        first, last = step_index == 0, step_index == ITERS - 1
        pieces = exchange(packed.reshape(N_MANY, -1, 128), MANY)
        back = exchange(middle(pieces, me), MANY)
        if first:
            full = back
        else:
            back = back.reshape(HEAD, 128)
        send, state = search_call(
            first, last, back, spot, w, mat, residual, fac, state, full, answer, fix
        )
        arrived = exchange(send, "zh")
        if not last:
            packed, residual, answer = next_call(
                arrived, spot, ridge, mat, state, residual, fac, answer
            )
    answer, residual = call(final_kernel, (shape(T, 256), shape(T, 256)))(arrived, state, ridge)
    return answer.T, residual.T


def solution(mesh):
    finer = Mesh(mesh.devices.reshape(4, 2, 4, 4, 2), ("zh", "zl", "y", "x", "c"))
    spec = P((*FEAT, *ROW), None)
    in_specs = (P(ROW, FEAT), P(ROW, None), spec, P(), P())
    return jax.shard_map(
        program, mesh=finer, in_specs=in_specs, out_specs=(spec, spec), check_vma=False
    )
```

```python
import jax
import jax.numpy as jnp
from jax import lax
from jax.experimental import pallas as pl
from jax.experimental.pallas import tpu as pltpu
from jax.sharding import Mesh
from jax.sharding import PartitionSpec as P


ITERS = 3
ROW = ("zh", "zl", "y")
FEAT = ("x", "c")
OWN = ("zl", "y")
MANY = ("zl", "y", "x", "c")
N_MANY, N_ZH = 64, 4
T, RANK, BLOCK = 48, 256, 1024
SCAL = 480
HEAD = 512
BF = jnp.bfloat16
F32 = jnp.float32


def exchange(pieces, axes):
    return lax.all_to_all(pieces, axes, 0, 0, tiled=True)


def dot(a, b):
    return jnp.dot(a, b, preferred_element_type=F32)


def dot_t(a, b):
    return lax.dot_general(a, b, (((1,), (1,)), ((), ())), preferred_element_type=F32)


PARAMS = pltpu.CompilerParams(vmem_limit_bytes=20 * 1024 * 1024)


IN_HBM = pl.BlockSpec(memory_space=pltpu.HBM)
IN_VMEM = pl.BlockSpec(memory_space=pltpu.VMEM)
IN_SMEM = pl.BlockSpec(memory_space=pltpu.SMEM)


def call(body, out):
    return pl.pallas_call(body, out_shape=out, compiler_params=PARAMS)


def fetch(pairs, sems):
    copies = [pltpu.make_async_copy(a, b, sems.at[i]) for i, (a, b) in enumerate(pairs)]
    for copy in copies:
        copy.start()
    return copies


def shape(*dims, dtype=F32):
    return jax.ShapeDtypeStruct(dims, dtype)


def columns(parts):
    lane = lax.broadcasted_iota(jnp.int32, (T, 128), 1)
    block = jnp.zeros((T, 128), F32)
    for index, part in enumerate(parts):
        block = jnp.where(lane == index, part, block)
    return block


def split16(value):
    high = value.astype(BF).astype(F32)
    return high, value - high


def as_tile(column):
    block = jnp.concatenate([columns(split16(column)), jnp.zeros((80, 128), F32)], axis=0)
    return block.T[:8, :].astype(BF)


def from_tile(tile):
    block = jnp.concatenate([tile, jnp.zeros((120, 128), F32)], axis=0).T
    return block[:T, 0:1] + block[:T, 1:2]


def total_of(array):
    return jnp.sum(array, axis=1, keepdims=True)


CHUNKS, DEEP = 4, 32


def pack_kernel(design, goal_in, out, rows, packed, goals, goal, sems):
    def inward(index):
        at = pl.ds(index * DEEP, DEEP)
        return pltpu.make_async_copy(design.at[at, :], rows.at[at, :], sems.at[index])

    def outward(index):
        at = pl.ds(index * DEEP, DEEP)
        return pltpu.make_async_copy(
            packed.at[:, at, :], out.at[:, at, :], sems.at[CHUNKS + index]
        )

    for index in range(CHUNKS):
        inward(index).start()
    fetched = pltpu.make_async_copy(goal_in, goal, sems.at[2 * CHUNKS + 1])
    fetched.start()
    last = pltpu.make_async_copy(goals, out.at[:, 128:136, :], sems.at[2 * CHUNKS])
    for index in range(CHUNKS):
        inward(index).wait()
        if index == 1:
            fetched.wait()
            for to in range(8):
                for at in range(6):
                    goals[to, :, at * 128 : (at + 1) * 128] = goal[at * 8 : at * 8 + 8, :]
                goals[to, :, 768:] = jnp.zeros((8, 256), BF)
            last.start()
        low, high = index * DEEP, (index + 1) * DEEP
        for to in range(8):
            for part in range(4):
                at = (part * 8 + to) * 256
                packed[to, low:high, part * 256 : (part + 1) * 256] = rows[low:high, at : at + 256]
        outward(index).start()
    for index in range(CHUNKS):
        outward(index).wait()
    last.wait()


def pack(design, goal):
    return pl.pallas_call(
        pack_kernel,
        out_shape=shape(8, 136, BLOCK, dtype=BF),
        in_specs=[IN_HBM, IN_HBM],
        out_specs=IN_HBM,
        scratch_shapes=[
            pltpu.VMEM((128, 8192), BF),
            pltpu.VMEM((8, 128, BLOCK), BF),
            pltpu.VMEM((8, 8, BLOCK), BF),
            pltpu.VMEM((T, 128), BF),
            pltpu.SemaphoreType.DMA((2 * CHUNKS + 2,)),
        ],
    )(design, goal)


def start_kernel(mat, out):
    part = jnp.zeros((T, BLOCK), F32)
    for src in range(8):
        goal = jnp.concatenate(
            [mat[src, 128:136, t * 128 : (t + 1) * 128].astype(F32) for t in range(6)], axis=0
        ).astype(BF)
        part = part + dot(goal, mat[src, :128, :])
    high, low = split16(part)
    high, low = high.astype(BF), low.astype(BF)
    for to in range(N_ZH):
        out[to, :, :BLOCK] = high
        out[to, :, BLOCK:] = low[:, to * 256 : (to + 1) * 256]


def cross_kernel(mat, fac, out):
    factor = fac[...]
    both = jnp.zeros((RANK, RANK), F32)
    for index in range(4):
        rows = fac[index * 256 : (index + 1) * 256, :]
        both = both + lax.dot_general(
            rows, rows, (((0,), (0,)), ((), ())), preferred_element_type=F32
        )
    both = both.astype(BF)
    for src in range(8):
        block = dot(mat[src, :128, :], factor).astype(BF)
        for half in range(2):
            for part in range(4):
                rows = block[part * 32 : (part + 1) * 32, half * 128 : (half + 1) * 128]
                out[src * 8 + half * 4 + part, :32, :] = rows
    for half in range(2):
        for part in range(32):
            rows = both[part * 8 : (part + 1) * 8, half * 128 : (half + 1) * 128]
            out[half * 32 + part, 32:40, :] = rows


def write_head(residual, direction, mat, fac, put):
    low = residual.astype(BF)
    for src in range(8):
        put(src * 6, dot_t(low, mat[src, :128, :]))
    seen = dot(low, fac[...])
    put(48, seen[:, :128])
    put(54, seen[:, 128:])
    rr = split16(total_of(residual * residual))
    rd = split16(total_of(residual * direction))
    block = jnp.concatenate([columns([*rr, *rd]), jnp.zeros((80, 128), F32)], axis=0)
    put(60, block.T[:32, :])


def first_kernel(arrived, mat, fac, cross, out, start_out, held, sem):
    total = jnp.zeros((T, BLOCK + 256), F32)
    for source in range(N_ZH):
        total = total + arrived[source].astype(F32)
    held[...] = total
    store = pltpu.make_async_copy(held, start_out, sem.at[0])
    store.start()
    out[:, :40, :] = cross[...]

    def put(tile, rows):
        for index in range(rows.shape[0] // 8):
            out[tile + index, 40:48, :] = rows[index * 8 : index * 8 + 8, :].astype(BF)

    residual = total[:, :BLOCK]
    write_head(residual, residual, mat, fac, put)
    store.wait()


def first_call(arrived, mat, fac, cross):
    return pl.pallas_call(
        first_kernel,
        out_shape=(shape(N_MANY, 48, 128, dtype=BF), shape(T, BLOCK + 256)),
        in_specs=[IN_VMEM] * 4,
        out_specs=(IN_VMEM, IN_HBM),
        scratch_shapes=[pltpu.VMEM((T, BLOCK + 256), F32), pltpu.SemaphoreType.DMA((1,))],
        compiler_params=PARAMS,
    )(arrived, mat, fac, cross)


def own_part(array, zh):
    mine = array[:, :256]
    for index in range(1, N_ZH):
        mine = jnp.where(zh == index, array[:, index * 256 : (index + 1) * 256], mine)
    return mine


D_AT, R_AT, S_AT, C_AT, WIDE = 0, BLOCK, 2 * BLOCK, 2 * BLOCK + RANK, 2 * BLOCK + RANK + 128


def next_kernel(more, arrived, zh, penalty, mat, state, residual_in, fac_in, *refs):
    refs = list(refs)
    answer_in = refs.pop(0) if more else None
    out, residual_out, answer_out, direction_v, scal_v, residual_v, fac_v, answer_v, sems = refs
    copies = fetch(
        [
            (state.at[:, D_AT:R_AT], direction_v),
            (state.at[:, C_AT:WIDE], scal_v),
            (residual_in.at[:, :BLOCK], residual_v),
            (fac_in, fac_v),
        ]
        + ([(answer_in, answer_v)] if more else []),
        sems,
    )
    total = jnp.zeros((8 * T + 8, 128), F32)
    for source in range(N_ZH):
        total = total + arrived[source].astype(F32)
    square = from_tile(total[8 * T :])
    hess = jnp.concatenate([total[at * T : (at + 1) * T] for at in range(8)], axis=1)
    ridge = penalty[:, :1]
    for copy in copies[:3]:
        copy.wait()
    inner, dd = scal_v[:, :1], scal_v[:, 1:2]
    direction = direction_v[...]
    step = inner / (square + ridge * dd)
    residual = residual_v[...] - step * (hess + ridge * direction)
    residual_v[...] = residual
    answer = step * own_part(direction, zh[0])
    if more:
        copies[4].wait()
        answer = answer_v[...] + answer
    answer_v[...] = answer
    stores = [
        pltpu.make_async_copy(residual_v, residual_out, sems.at[5]),
        pltpu.make_async_copy(answer_v, answer_out, sems.at[6]),
    ]
    for copy in stores:
        copy.start()
    copies[3].wait()

    def put(tile, rows):
        out[tile * 8 : tile * 8 + rows.shape[0], :] = rows.astype(BF)

    write_head(residual, direction, mat, fac_v, put)
    for copy in stores:
        copy.wait()


def next_call(arrived, zh, ridge, mat, state, residual, fac, answer):
    more = answer is not None
    extra = (answer,) if more else ()
    return pl.pallas_call(
        lambda *refs: next_kernel(more, *refs),
        out_shape=(shape(HEAD, 128, dtype=BF), shape(T, BLOCK), shape(T, 256)),
        in_specs=[IN_VMEM, IN_SMEM, IN_VMEM, IN_VMEM] + [IN_HBM] * (3 + len(extra)),
        out_specs=(IN_VMEM, IN_HBM, IN_HBM),
        scratch_shapes=[
            pltpu.VMEM((T, BLOCK), F32),
            pltpu.VMEM((T, 128), F32),
            pltpu.VMEM((T, BLOCK), F32),
            pltpu.VMEM((BLOCK, RANK), BF),
            pltpu.VMEM((T, 256), F32),
            pltpu.SemaphoreType.DMA((7,)),
        ],
        compiler_params=PARAMS,
    )(arrived, zh, ridge, mat, state, residual, fac, *extra)


def search_kernel(first, last, back, zh, weights, mat, residual_in, fac_in, *refs):
    refs = list(refs)
    state_in = None if first else refs.pop(0)
    full = back if first else refs.pop(0)
    answer_in, fix_in = (refs.pop(0), refs.pop(0)) if last else (None, None)
    out, state_out, residual_v, fac_v, sems, state_v = refs[:6]
    refs = refs[6:]

    def lanes(array, low, high):
        return array.at[:, low:high]

    pairs = [(residual_in.at[:, :BLOCK], residual_v), (fac_in, fac_v)]
    if not first:
        full_v = refs.pop(0)
        pairs = [
            (full, full_v),
            (lanes(state_in, S_AT, WIDE), lanes(state_v, S_AT, WIDE)),
            (lanes(state_in, R_AT, S_AT), lanes(state_v, R_AT, S_AT)),
            (lanes(state_in, D_AT, R_AT), lanes(state_v, D_AT, R_AT)),
        ] + pairs
        full = full_v
    late = 0 if first else 3
    if last:
        answer_v, fix_v, tail_v = refs
        pairs += [(answer_in, answer_v), (fix_in.at[:, BLOCK:], fix_v)]
    copies = fetch(pairs, sems)

    def head(tile, count):
        if first:
            return jnp.concatenate(
                [back[t, 40:48, :].astype(F32) for t in range(tile, tile + count)], axis=0
            )
        return back[tile * 8 : (tile + count) * 8, :].astype(F32)

    def crossed(src, half):
        at = src * 8 + half * 4
        return full[at : at + 4, :32, :].reshape(128, 128)

    def grammed(half):
        return full[half * 32 : half * 32 + 32, 32:40, :].astype(F32).reshape(256, 128).astype(BF)

    projected = jnp.concatenate([head(48, 6), head(54, 6)], axis=1)
    tile = jnp.concatenate([head(60, 1), jnp.zeros((120, 128), F32)], axis=0).T
    rr = tile[:T, 0:1] + tile[:T, 1:2]
    rd = tile[:T, 2:3] + tile[:T, 3:4]
    scaled = weights[0:1, :] * projected
    cross_inner = total_of(scaled * projected)
    inner = rr + cross_inner
    low = scaled.astype(BF)
    if not first:
        for copy in copies[:late]:
            copy.wait()
        beta = inner / state_v[:, C_AT : C_AT + 1]
    row_lows = []
    square = jnp.zeros((T, 1), F32)
    for src in range(8):
        row = head(src * 6, 6) + dot_t(low[:, :128], crossed(src, 0))
        row = row + dot_t(low[:, 128:], crossed(src, 1))
        at = R_AT + src * 128
        if not first:
            row = row + beta * state_v[:, at : at + 128]
        state_v[:, at : at + 128] = row
        row_low = row.astype(BF)
        square = square + total_of(row * row_low.astype(F32))
        row_lows.append(row_low)
    through = jnp.concatenate([dot(low, grammed(0)), dot(low, grammed(1))], axis=1)
    dd = rr + 2.0 * cross_inner + total_of(scaled * through)
    seen = projected + through
    if not first:
        sd = rd + total_of(scaled * state_v[:, S_AT:C_AT])
        dd = dd + 2.0 * beta * sd + beta * beta * state_v[:, C_AT + 1 : C_AT + 2]
        seen = seen + beta * state_v[:, S_AT:C_AT]
    for copy in copies[late:]:
        copy.wait()
    direction = residual_v[...] + dot_t(low, fac_v[...])
    if not first:
        direction = direction + beta * state_v[:, D_AT:R_AT]
    if last:
        tail_v[:, :256] = own_part(direction, zh[0])
        tail_v[:, 256:512] = answer_v[...]
        tail_v[:, 512:768] = own_part(residual_v[...], zh[0]) + fix_v[...]
        tail_v[:, 768:] = columns([inner, dd])
        store = pltpu.make_async_copy(tail_v, state_out, sems.at[8])
    else:
        state_v[:, D_AT:R_AT] = direction
        state_v[:, S_AT:C_AT] = seen
        state_v[:, C_AT:WIDE] = columns([inner, dd])
        store = pltpu.make_async_copy(state_v, state_out, sems.at[8])
    store.start()
    part = jnp.zeros((T, BLOCK), F32)
    for src in range(8):
        part = part + dot(row_lows[src], mat[src, :128, :])
    part = part.astype(BF)
    tile = as_tile(square)
    for to in range(N_ZH):
        blocks = range(2 * to, 2 * to + 2) if last else range(8)
        for index, at in enumerate(blocks):
            out[to, index * T : (index + 1) * T, :] = part[:, at * 128 : (at + 1) * 128]
        out[to, len(blocks) * T :, :] = tile
    store.wait()


def search_call(first, last, back, zh, weights, mat, residual, fac, state, full, answer, fix):
    hbm = [residual, fac]
    if not first:
        hbm += [state, full]
    if last:
        hbm += [answer, fix]
    scratch = [
        pltpu.VMEM((T, BLOCK), F32),
        pltpu.VMEM((BLOCK, RANK), BF),
        pltpu.SemaphoreType.DMA((9,)),
        pltpu.VMEM((T, WIDE), F32),
    ]
    if not first:
        scratch.append(pltpu.VMEM((N_MANY, 48, 128), BF))
    if last:
        scratch += [pltpu.VMEM((T, 256), F32), pltpu.VMEM((T, 256), F32), pltpu.VMEM((T, 896), F32)]
    return pl.pallas_call(
        lambda *refs: search_kernel(first, last, *refs),
        out_shape=(
            shape(N_ZH, (2 if last else 8) * T + 8, 128, dtype=BF),
            shape(T, 896 if last else WIDE),
        ),
        in_specs=[IN_VMEM, IN_SMEM, IN_VMEM, IN_VMEM] + [IN_HBM] * len(hbm),
        out_specs=(IN_VMEM, IN_HBM),
        scratch_shapes=scratch,
        compiler_params=PARAMS,
    )(back, zh, weights, mat, *hbm)


def middle_kernel(pieces, me, out):
    total = jnp.zeros(pieces.shape[1:], F32)
    for source in range(N_MANY):
        total = total + pieces[source].astype(F32)
    tile = total[-8:]
    high_a, low_a = split16(tile[0:1] + tile[1:2])
    high_b, low_b = split16(tile[2:3] + tile[3:4])
    line = lax.broadcasted_iota(jnp.int32, (8, 128), 0)
    again = tile
    for index, value in enumerate((high_a, low_a, high_b, low_b)):
        again = jnp.where(line == index, value, again)
    tile = jnp.where(me[0] == SCAL // 8, again, tile)
    if total.shape[0] > 8:
        tile = jnp.concatenate([total[:-8], tile], axis=0)
    tile = tile.astype(BF)
    for target in range(N_MANY):
        out[target] = tile


def middle(pieces, me):
    return pl.pallas_call(
        middle_kernel,
        out_shape=shape(*pieces.shape, dtype=BF),
        in_specs=[IN_VMEM, IN_SMEM],
        out_specs=IN_VMEM,
        compiler_params=PARAMS,
    )(pieces, me)


def final_kernel(arrived, tail, penalty, answer_out, residual_out):
    total = jnp.zeros((2 * T + 8, 128), F32)
    for source in range(N_ZH):
        total = total + arrived[source].astype(F32)
    square = from_tile(total[2 * T :])
    ridge = penalty[:, :1]
    mine = tail[:, :256]
    step = tail[:, 768:769] / (square + ridge * tail[:, 769:770])
    hess = jnp.concatenate([total[:T], total[T : 2 * T]], axis=1) + ridge * mine
    answer_out[...] = tail[:, 256:512] + step * mine
    residual_out[...] = tail[:, 512:768] - step * hess


def program(design, targets, factor, weights, penalty):
    zh = lax.axis_index("zh")
    me = lax.axis_index(MANY).reshape(1)
    w = jnp.broadcast_to(weights[None, :], (8, RANK))
    ridge = jnp.broadcast_to(penalty[:, None], (T, 128))
    low_factor, spot, me, w, ridge = lax.optimization_barrier(
        (factor.astype(BF), zh.reshape(1), me, w, ridge)
    )
    slots = jnp.zeros((N_ZH, 256, RANK), BF)
    slots = lax.dynamic_update_slice(slots, low_factor[None], (zh, 0, 0))
    for shift in range(1, N_ZH):
        pairs = [(i, (i + shift) % N_ZH) for i in range(N_ZH)]
        other = lax.ppermute(low_factor, "zh", pairs)
        slots = lax.dynamic_update_slice(slots, other[None], ((zh - shift) % N_ZH, 0, 0))
    fac = slots.reshape(BLOCK, RANK)

    spot = zh.reshape(1)
    mat = exchange(pack(design, targets.T), OWN)
    arrived = call(start_kernel, shape(N_ZH, T, BLOCK + 256, dtype=BF))(mat)
    arrived = exchange(arrived, "zh")
    cross = call(cross_kernel, shape(N_MANY, 40, 128, dtype=BF))(mat, fac)

    packed, residual = first_call(arrived, mat, fac, cross)
    fix = residual
    answer = state = full = None
    for step_index in range(ITERS):
        first, last = step_index == 0, step_index == ITERS - 1
        pieces = exchange(packed.reshape(N_MANY, -1, 128), MANY)
        back = exchange(middle(pieces, me), MANY)
        if first:
            full = back
        else:
            back = back.reshape(HEAD, 128)
        send, state = search_call(
            first, last, back, spot, w, mat, residual, fac, state, full, answer, fix
        )
        arrived = exchange(send, "zh")
        if not last:
            packed, residual, answer = next_call(
                arrived, spot, ridge, mat, state, residual, fac, answer
            )
    answer, residual = call(final_kernel, (shape(T, 256), shape(T, 256)))(arrived, state, ridge)
    return answer.T, residual.T


def solution(mesh):
    finer = Mesh(mesh.devices.reshape(4, 2, 4, 4, 2), ("zh", "zl", "y", "x", "c"))
    spec = P((*FEAT, *ROW), None)
    in_specs = (P(ROW, FEAT), P(ROW, None), spec, P(), P())
    return jax.shard_map(
        program, mesh=finer, in_specs=in_specs, out_specs=(spec, spec), check_vma=False
    )
```
